256 devices in a mesh: board: 128 (over y, x, z), hand: 2 (over core).
Axes of the slice: x: 4, y: 4, z: 8, core: 2. Of those that a mesh axis runs over, the one named last changes fastest.
Arguments:
- opp_reach: bfloat16 [8192, 1326], P('board', 'hand'), may hold values from 0.019897461 to 1
- hand_rank: int32 [8192, 1326], P('board'), may hold values from 0 to 1325, as said below
- hand_cards: int32 [1326, 2], replicated, may hold values from 0 to 51, as said below
- pot: float32 [8192], P('board'), may hold values from 1 to 12
- bet_frac: float32 [8192], P('board'), may hold values from 0.25 to 1.5
- trav_reach: float32 [1326], P('hand'), may hold values from 0.02 to 1
Outputs:
- board_values: float32 [8192, 1326], P('board', 'hand')
- hand_values: float32 [1326], P('hand')
- exploitability: float32 [], replicated
The draws below stay inside these ranges and needn't reach their ends.
Inputs may be any that keep to these rules, and one draw needn't show every extreme that they name: hand_rank[b, i] is the number of hands strictly weaker than hand i on board b; equal ranks tie. `hand_cards`: the rows are the 1326 distinct pairs of two different cards, smaller card first, in an order drawn from the seed.
All inputs are finite; a program needn't handle non-finite values.
Results may differ from the reference program's by a relative error of at most 0.0003.
Values may be sent and summed in bfloat16 or wider, within the bound.
A program may use at most 64 MiB of HBM per device.

```python
import math
import jax
import jax.numpy as jnp
import numpy as np
from jax import lax

CARDS = 52
H = 1326
BOARDS = 8192


def showdown_order(key):
    seeded = jax.random.fold_in(key, 7)
    hand_key, board_key = jax.random.split(seeded)
    strength = jax.random.randint(hand_key, (1, H), 0, 3 * H // 4)
    noise = jax.random.randint(board_key, (BOARDS, H), 0, H // 2)
    scores = (strength + noise).astype(jnp.int32)
    ordering = jnp.argsort(scores, axis=1, stable=True).astype(jnp.int32)
    ranked = jnp.take_along_axis(scores, ordering, axis=1)
    positions = lax.broadcasted_iota(jnp.int32, (BOARDS, H), 1)
    fresh = jnp.concatenate([jnp.ones((BOARDS, 1), jnp.bool_), ranked[:, 1:] != ranked[:, :-1]], axis=1)
    starts = lax.cummax(jnp.where(fresh, positions, 0), axis=1)
    board_rows = lax.broadcasted_iota(jnp.int32, (BOARDS, H), 0)
    rank_table = jnp.zeros((BOARDS, H), jnp.int32).at[board_rows, ordering].set(starts)
    return rank_table


def draw_hand_rank(key, part):
    return showdown_order(key)


def draw_hand_cards(key, part):
    lower_card, upper_card = np.triu_indices(CARDS, 1)
    pairs = jnp.stack([jnp.asarray(lower_card), jnp.asarray(upper_card)], axis=1).astype(jnp.int32)
    shuffle = jax.random.permutation(jax.random.fold_in(key, 11), H)
    return pairs[shuffle]


def draw_pot(key, part):
    seeded = jax.random.fold_in(key, 13)
    spread = jnp.arange(BOARDS, dtype=jnp.float32) / max(BOARDS - 1, 1)
    level = jnp.exp(jax.random.uniform(seeded, (BOARDS,), jnp.float32, 0.0, math.log(4.0)))
    return ((1.0 + 2.0 * spread) * level).astype(jnp.float32)


def shard_levels(stream_key, extent, pieces, low, top_value):
    level, own = 1.0, jax.random.fold_in(stream_key, 6)
    for position, parts in pieces:
        steps = jnp.exp(jax.random.uniform(jax.random.fold_in(own, position), (parts,), jnp.float32, low / len(pieces), top_value / len(pieces)))
        level = level * jnp.repeat(steps, extent[position] // parts).reshape([-1 if axis == position else 1 for axis in range(len(extent))])
    return level


def setup_inputs(seed: int = 0) -> dict:
    streams_of = jax.random.split(jax.random.key(seed), 7)
    return {
        "opp_reach": jnp.clip(jnp.exp(math.log(1.0) - 3.9171631 * jax.random.uniform(streams_of[0], (BOARDS, H), jnp.float32) ** shard_levels(streams_of[0], (BOARDS, H), ((0, 128), (1, 2)), -0.2, 0.2)), 0.019897461, 1.0).astype(jnp.bfloat16),
        "hand_rank": draw_hand_rank(jax.random.fold_in(streams_of[6], 71), 0),
        "hand_cards": draw_hand_cards(jax.random.fold_in(streams_of[6], 71), 0),
        "pot": draw_pot(jax.random.fold_in(streams_of[6], 71), 0),
        "bet_frac": jnp.clip(0.25 + 1.25 * jax.random.uniform(streams_of[4], (BOARDS,), jnp.float32) ** shard_levels(streams_of[4], (BOARDS,), ((0, 128),), -0.2, 0.2), 0.25, 1.5),
        "trav_reach": jnp.clip(jnp.exp(math.log(1.0) - 3.912023 * jax.random.uniform(streams_of[5], (H,), jnp.float32) ** shard_levels(streams_of[5], (H,), ((0, 2),), -0.2, 0.2)), 0.02, 1.0),
    }


def incidence(hand_cards):
    card_ids = jnp.arange(CARDS, dtype=jnp.int32)
    return ((hand_cards[:, 0:1] == card_ids) | (hand_cards[:, 1:2] == card_ids)).astype(jnp.float32)


def showdown(opp_reach, hand_rank, hand_cards):
    card_hold = incidence(hand_cards)
    first_card = hand_cards[:, 0]
    second_card = hand_cards[:, 1]
    positions = jnp.arange(H, dtype=jnp.int32)

    def one_board(board_data):
        rank_row, reach_row = board_data
        order_row = jnp.argsort(rank_row, stable=True).astype(jnp.int32)
        own_reach = reach_row.astype(jnp.float32)
        weighted = own_reach[:, None] * card_hold
        ordered = weighted[order_row]
        prefix = jnp.concatenate([jnp.zeros((1, CARDS), jnp.float32), jnp.cumsum(ordered, axis=0)], axis=0)
        share = jnp.sum(prefix, axis=1) * 0.5
        sorted_rank = rank_row[order_row]
        group_marks = jnp.where(sorted_rank == positions, positions, H)
        shifted = jnp.concatenate([group_marks[1:], jnp.full((1,), H, jnp.int32)])
        next_start = lax.cummin(shifted, axis=0, reverse=True)
        tie_end = next_start[rank_row]

        def blocked(row_index):
            return share[row_index] - prefix[row_index, first_card] - prefix[row_index, second_card]

        beaten = blocked(rank_row)
        reached = blocked(tie_end) + own_reach
        live_mass = blocked(jnp.full((H,), H, jnp.int32)) + own_reach
        return beaten + reached - live_mass, live_mass

    return lax.map(one_board, (hand_rank, opp_reach))


def reference(opp_reach, hand_rank, hand_cards, pot, bet_frac, trav_reach):
    margin, live_mass = showdown(opp_reach, hand_rank, hand_cards)
    half_pot = (0.5 * pot)[:, None]
    call_value = (half_pot + (bet_frac * pot)[:, None]) * margin / H
    fold_value = -half_pot * live_mass / H
    board_values = jnp.maximum(call_value, fold_value)
    hand_values = jnp.mean(board_values, axis=0)
    opp_mass = jnp.mean(half_pot * live_mass / H, axis=0)
    exploit = jnp.sum(trav_reach * hand_values) / jnp.sum(trav_reach * opp_mass)
    return board_values, hand_values, exploit
```

```python
import functools

import jax
import jax.numpy as jnp
from jax import lax
from jax.experimental import pallas as pl
from jax.experimental.pallas import tpu as pltpu
from jax.sharding import Mesh
from jax.sharding import PartitionSpec as P

CARDS = 52
BOARD = ("board_0", "board_1", "board_2")
BF16 = jnp.bfloat16
F32 = jnp.float32

HALF = CARDS // 2
ROWS = 32
HI, LO = 48, 28
SLOT = 32
GROUP = 8
DBLOCK = 4
NT = (((1,), (1,)), ((), ()))


def iota(shape, axis):
    return lax.broadcasted_iota(jnp.int32, shape, axis)


def split2(x):
    high = x.astype(BF16)
    return high, (x - high.astype(F32)).astype(BF16)


def rank_code(rank):
    return (((rank & 127) | 128) << (rank >> 7)).astype(F32).astype(BF16)


def compute_kernel(
    total_boards, hand_count, own_count, me,
    own_ref, other_ref, rank_ref, cards_ref, pot_ref, bet_ref, trav_ref,
    values_ref, part_ref, sums_ref,
    x_ref, p_ref, o_ref, w_ref, g_ref, q_ref, f_ref, a_ref, b_ref, h_ref, t_ref, s_ref, c_ref,
):
    boards, lanes = own_ref.shape
    width = 2 * lanes
    if me is None:
        me = lax.axis_index("hand")

    for half, (reach, at) in enumerate(((own_ref[...], me), (other_ref[...], 1 - me))):
        cols = slice(half * lanes, (half + 1) * lanes)
        rank = rank_ref[at]
        code = rank_code(rank)
        x_ref[0:boards, cols] = reach
        x_ref[boards : 2 * boards, cols] = reach
        x_ref[2 * boards : 3 * boards, cols] = code
        x_ref[3 * boards : 4 * boards, cols] = code
        hi = (rank * 2341) >> 16
        lo = rank - LO * hi
        f_ref[0, :, cols] = hi.astype(F32)
        f_ref[1, :, cols] = lo.astype(F32)
        f_ref[2, :, cols] = reach.astype(F32)
        c_ref[:, cols] = cards_ref[at]

    row16 = iota((16, width), 0).astype(F32).astype(BF16)

    def hot_rows(d, carry):
        low, high = c_ref[0:1, :], c_ref[1:2, :]
        df = d.astype(F32)
        partner = jnp.where(low == df, high, jnp.where(high == df, low, -1.0))
        for q in range(2):
            rel = partner - float(HALF * q)
            rel = jnp.where(rel < float(HALF), rel, -1.0)
            wide = jnp.broadcast_to(rel, (16, width)).astype(BF16)
            for part in range(2):
                hit = wide == row16 + BF16(16 * part)
                p_ref[q, d, 16 * part : 16 * part + 16, :] = jnp.where(hit, BF16(1), BF16(0))
        return carry

    lax.fori_loop(0, CARDS, hot_rows, 0)

    chunk = CARDS // 2
    for q in range(2):

        def to_cards(i, carry):
            rows = p_ref[q, pl.ds(i * chunk, chunk)].reshape(chunk * ROWS, width)
            got = lax.dot_general(rows, x_ref[...], NT, preferred_element_type=F32)
            o_ref[q, pl.ds(i * chunk, chunk)] = got.reshape(chunk, ROWS, 4 * boards)
            return carry

        lax.fori_loop(0, 2, to_cards, 0)

    first = iota((ROWS, 2 * boards), 1) < boards

    def pack(d, carry):
        w_ref[d] = jnp.where(first, o_ref[0, d, :, 0 : 2 * boards], o_ref[1, d, :, 0 : 2 * boards]).astype(BF16)
        g_ref[d] = jnp.where(first, o_ref[0, d, :, 2 * boards :], o_ref[1, d, :, 2 * boards :]).astype(BF16)
        return carry

    lax.fori_loop(0, CARDS, pack, 0)

    for half in range(2):
        rows = slice(16 * half, 16 * half + 16)

        def pairs(i, carry):
            mine = [g_ref[DBLOCK * i + k, rows, :] for k in range(DBLOCK)]
            sums = [None] * DBLOCK
            for e in range(CARDS):
                ge, we = g_ref[e, rows, :], w_ref[e, rows, :].astype(F32)
                for k in range(DBLOCK):
                    sign = lax.clamp(BF16(-1), mine[k] - ge, BF16(1))
                    term = sign.astype(F32) * we
                    sums[k] = term if sums[k] is None else sums[k] + term
            for k in range(DBLOCK):
                q_ref[DBLOCK * i + k, rows, :] = sums[k]
            return carry

        lax.fori_loop(0, CARDS // DBLOCK, pairs, 0)

    lo_row = iota((16, width), 0).astype(F32).astype(BF16)

    def table(g, carry):
        for b in range(GROUP):
            hi = jnp.broadcast_to(f_ref[0, pl.ds(GROUP * g + b, 1), :], (16, width)).astype(BF16)
            lo = jnp.broadcast_to(f_ref[1, pl.ds(GROUP * g + b, 1), :], (16, width)).astype(BF16)
            reach = jnp.broadcast_to(f_ref[2, pl.ds(GROUP * g + b, 1), :], (16, width)).astype(BF16)
            tile, start = 128 * (b % 2), 128 - SLOT // 2 * b
            for part in range(HI // 16):
                hit = hi == lo_row + BF16(16 * part)
                a_ref[HI * b + 16 * part : HI * b + 16 * part + 16, :] = jnp.where(hit, reach, BF16(0))
            for part in range(SLOT // 16):
                at = tile + (start + 16 * part) % 128
                b_ref[at : at + 16, :] = lax.clamp(
                    BF16(-1), lo_row + BF16(16 * part) - lo, BF16(1)
                )
        got = lax.dot_general(a_ref[...], b_ref[...], NT, preferred_element_type=F32)
        h_ref[0 : GROUP * HI, :] = got[:, 0:128]
        h_ref[GROUP * HI :, :] = got[:, 128:256]
        even = iota((GROUP, 128), 0) % 2 == 0
        block = ((iota((GROUP, 128), 1) + SLOT // 2 * iota((GROUP, 128), 0)) % 128) // SLOT
        for t in range(HI // 4):
            row = None
            for k in range(4):
                at = 4 * t + k
                part = jnp.where(
                    even,
                    h_ref[pl.ds(at, GROUP, stride=HI), :],
                    h_ref[pl.ds(at + GROUP * HI, GROUP, stride=HI), :],
                )
                part = pltpu.roll(part, SLOT * k, 1) if k else part
                row = part if row is None else jnp.where(block == k, part, row)
            t_ref[t, pl.ds(GROUP * g, GROUP), :] = pltpu.roll(row, 0, 1, stride=SLOT // 2, stride_axis=0)
        return carry

    lax.fori_loop(0, boards // GROUP, table, 0)

    tiles = HI // 4
    spot = iota((boards, 128), 1) % SLOT == LO
    below = []
    run = jnp.zeros((boards, 128), F32)
    whole = []
    for t in range(tiles):
        mark = jnp.where(spot, t_ref[t], 0.0)
        whole.append(mark)
        below.append(run)
        run = run + mark
    src, dst = iota((256, 128), 0), iota((256, 128), 1)
    at_spot = src % SLOT == LO
    within = (dst // SLOT > (src - 128) // SLOT).astype(F32) - (dst // SLOT < (src - 128) // SLOT).astype(F32)
    spread = jnp.where(at_spot, jnp.where(src < 128, 1.0, within), 0.0).astype(BF16)
    for t in range(tiles):
        outer = below[t] - (run - below[t] - whole[t])
        both = jnp.concatenate([outer, whole[t]], axis=1)
        high, low = split2(both)
        got = jnp.dot(jnp.concatenate([high, low], axis=0), spread, preferred_element_type=F32)
        t_ref[t] = t_ref[t] + got[:boards] + got[boards:]

    def look_up(g, carry):
        rows = pl.ds(pl.multiple_of(GROUP * g, GROUP), GROUP)
        for k in range(lanes // 128):
            cols = slice(128 * k, 128 * k + 128)
            hi = f_ref[0, rows, cols].astype(jnp.int32)
            lo = f_ref[1, rows, cols].astype(jnp.int32)
            tile = hi >> 2
            at = ((hi & 3) << 5) + lo
            found = jnp.zeros((GROUP, 128), F32)
            for t in range(tiles):
                got = jnp.take_along_axis(t_ref[t, rows, :], at, axis=1, mode="promise_in_bounds")
                found = jnp.where(tile == t, got, found)
            s_ref[rows, cols] = found
        return carry

    lax.fori_loop(0, boards // GROUP, look_up, 0)

    shared = jnp.zeros((2 * boards, lanes), F32)
    turned = jnp.transpose(q_ref[...].reshape(CARDS * ROWS, 2 * boards))
    for q in range(2):
        high, low = split2(turned[boards * q : boards * (q + 1)])
        shared = shared + jnp.dot(
            jnp.concatenate([high, low], axis=0),
            p_ref[q, :, :, 0:lanes].reshape(CARDS * ROWS, lanes),
            preferred_element_type=F32,
        )

    card = iota((64, width), 0).astype(F32)
    hold = ((card == c_ref[0:1, :]) | (card == c_ref[1:2, :])).astype(F32).astype(BF16)
    card_totals = lax.dot_general(x_ref[0:boards, :], hold, NT, preferred_element_type=F32)
    high, low = split2(card_totals)
    held = jnp.dot(jnp.concatenate([high, low], axis=0), hold[:, 0:lanes], preferred_element_type=F32)
    live = (
        0.5 * jnp.sum(card_totals, axis=1, keepdims=True)
        - (held[:boards] + held[boards:])
        + own_ref[...].astype(F32)
    )
    margin = s_ref[...] - (shared[:boards] + shared[boards:])
    half_pot = 0.5 * pot_ref[...]
    call_value = ((half_pot + bet_ref[...] * pot_ref[...]) / hand_count) * margin
    stake = (half_pot / hand_count) * live
    values = jnp.maximum(call_value, -stake)
    values_ref[...] = values[:, 0:own_count]
    part = jnp.sum(values, axis=0, keepdims=True) / total_boards
    mass = jnp.sum(stake, axis=0, keepdims=True) / total_boards
    part = jnp.where(iota((1, lanes), 1) < own_count, part, 0.0)
    part_ref[...] = part
    numerator = jnp.sum(part * trav_ref[...], axis=1, keepdims=True)
    denominator = jnp.sum(mass * trav_ref[...], axis=1, keepdims=True)
    sums_ref[...] = jnp.where(iota((1, 128), 1) == 0, numerator, denominator)


def compute(own, other, rank, cards, pot, bet, trav, total_boards, hand_count, own_count, me=None):
    boards, lanes = own.shape
    width = 2 * lanes
    whole = pl.BlockSpec(memory_space=pltpu.VMEM)
    return pl.pallas_call(
        functools.partial(compute_kernel, total_boards, hand_count, own_count, me),
        out_shape=(
            jax.ShapeDtypeStruct((boards, own_count), F32),
            jax.ShapeDtypeStruct((1, lanes), F32),
            jax.ShapeDtypeStruct((1, 128), F32),
        ),
        in_specs=[whole] * 7,
        out_specs=(whole,) * 3,
        scratch_shapes=[
            pltpu.VMEM((4 * boards, width), BF16),
            pltpu.VMEM((2, CARDS, ROWS, width), BF16),
            pltpu.VMEM((2, CARDS, ROWS, 4 * boards), F32),
            pltpu.VMEM((CARDS, ROWS, 2 * boards), BF16),
            pltpu.VMEM((CARDS, ROWS, 2 * boards), BF16),
            pltpu.VMEM((CARDS, ROWS, 2 * boards), F32),
            pltpu.VMEM((3, boards, width), F32),
            pltpu.VMEM((GROUP * HI, width), BF16),
            pltpu.VMEM((GROUP * SLOT, width), BF16),
            pltpu.VMEM((2 * GROUP * HI, 128), F32),
            pltpu.VMEM((HI // 4, boards, 128), F32),
            pltpu.VMEM((boards, lanes), F32),
            pltpu.VMEM((2, width), F32),
        ],
        compiler_params=pltpu.CompilerParams(vmem_limit_bytes=56 * 1024 * 1024),
        cost_estimate=pl.CostEstimate(flops=10**9, bytes_accessed=10**6, transcendentals=0),
    )(own, other, rank, cards, pot, bet, trav)


def local(opp_reach, hand_rank, hand_cards, pot, bet_frac, trav_reach):
    boards, hand_count = hand_rank.shape
    own_count = opp_reach.shape[1]
    lanes = -(-own_count // 128) * 128
    gap = lanes - own_count
    total_boards = boards * lax.axis_size(BOARD)
    own = jnp.pad(opp_reach, ((0, 0), (0, gap)))
    other = lax.ppermute(own, "hand", [(0, 1), (1, 0)])
    rank = jnp.pad(hand_rank.reshape(boards, 2, own_count).transpose(1, 0, 2), ((0, 0), (0, 0), (0, gap)))
    cards = jnp.pad(
        hand_cards.reshape(2, own_count, 2).transpose(0, 2, 1).astype(F32),
        ((0, 0), (0, 0), (0, gap)),
        constant_values=-1.0,
    )
    trav = jnp.pad(trav_reach, (0, gap))[None, :]
    board_values, part, sums = compute(
        own, other, rank, cards, pot[:, None], bet_frac[:, None], trav, total_boards, hand_count, own_count
    )
    packed = jnp.concatenate([part, sums], axis=1)
    packed = functools.reduce(lax.psum, BOARD, packed)
    hand_values = packed[0, :own_count]
    ends = lax.psum(packed[0, lanes : lanes + 2], "hand")
    return board_values, hand_values, ends[0] / ends[1]


def solution(mesh):
    torus = Mesh(
        mesh.devices.reshape(4, 4, 8, mesh.shape["hand"]), ("board_0", "board_1", "board_2", "hand")
    )
    placed = (P(BOARD, "hand"), P(BOARD, None), P(), P(BOARD), P(BOARD), P("hand"))
    return jax.shard_map(
        local,
        mesh=torus,
        in_specs=placed,
        out_specs=(P(BOARD, "hand"), P("hand"), P()),
        check_vma=False,
    )
```

```python
import functools

import jax
import jax.numpy as jnp
from jax import lax
from jax.experimental import pallas as pl
from jax.experimental.pallas import tpu as pltpu
from jax.sharding import Mesh
from jax.sharding import PartitionSpec as P

CARDS = 52
BOARD = ("board_0", "board_1", "board_2")
BF16 = jnp.bfloat16
F32 = jnp.float32

HALF = CARDS // 2
ROWS = 32
HI, LO = 48, 28
SLOT = 32
GROUP = 8
DBLOCK = 4
YS, XS, ZS = 4, 4, 8
MESH = pl.DeviceIdType.MESH
NT = (((1,), (1,)), ((), ()))


def iota(shape, axis):
    return lax.broadcasted_iota(jnp.int32, shape, axis)


def split2(x):
    high = x.astype(BF16)
    return high, (x - high.astype(F32)).astype(BF16)


def rank_code(rank):
    return (((rank & 127) | 128) << (rank >> 7)).astype(F32).astype(BF16)


def every_peer(places):
    y, x, z, h = places
    plane = [
        {"board_0": lax.rem(y + i, YS), "board_1": lax.rem(x + j, XS)}
        for i in range(YS)
        for j in range(XS)
        if i or j
    ]
    line = [{"board_2": lax.rem(z + i, ZS)} for i in range(1, ZS)]
    cross = [{"board_2": lax.rem(z + i, ZS), "hand": 1 - h} for i in range(ZS)]
    return plane, line, cross


def column(row):
    n = row.shape[1]
    return jnp.sum(jnp.where(iota((n, n), 0) == iota((n, n), 1), row, 0.0), axis=1, keepdims=True)


def fused_kernel(
    total_boards, hand_count,
    reach_ref, rank_ref, cards_ref, pot_ref, bet_ref, trav_ref,
    values_ref, hand_ref, ratio_ref,
    x_ref, p_ref, o_ref, w_ref, g_ref, q_ref, f_ref, a_ref, b_ref, h_ref, t_ref, s_ref, c_ref,
    swap_ref, mine_ref, plane_ref, line_ref, cross_ref, swap_sem, plane_sem, line_sem, cross_sem,
):
    boards, own_count = reach_ref.shape
    lanes = x_ref.shape[1] // 2
    width = 2 * lanes
    places = tuple(lax.axis_index(name) for name in BOARD) + (lax.axis_index("hand"),)
    y, x, z, me = places
    plane, line, cross = every_peer(places)
    barrier = pltpu.get_barrier_semaphore()
    for peer in plane + line + cross:
        pl.semaphore_signal(barrier, inc=1, device_id=peer, device_id_type=MESH)

    def cols_of(half, start=0, size=lanes):
        return pl.ds(pl.multiple_of(half * lanes + start, 128), size)

    x_ref[0:boards, cols_of(me, lanes - 128, 128)] = jnp.zeros((boards, 128), BF16)
    x_ref[0:boards, cols_of(1 - me, lanes - 128, 128)] = jnp.zeros((boards, 128), BF16)
    for half in range(2):
        start = half * lanes
        f_ref[0:2, :, start + lanes - 128 : start + lanes] = jnp.zeros((2, boards, 128), F32)
        x_ref[2 * boards : 3 * boards, start + lanes - 128 : start + lanes] = jnp.zeros((boards, 128), BF16)
        c_ref[:, start + lanes - 128 : start + lanes] = jnp.full((2, 128), -1.0, F32)
        c_ref[:, start : start + own_count] = cards_ref[:, half * own_count : (half + 1) * own_count].astype(F32)
        rank = rank_ref[:, half * own_count : (half + 1) * own_count]
        x_ref[2 * boards : 3 * boards, start : start + own_count] = rank_code(rank)
        hi = (rank * 2341) >> 16
        f_ref[0, :, start : start + own_count] = hi.astype(F32)
        f_ref[1, :, start : start + own_count] = (rank - LO * hi).astype(F32)
    x_ref[3 * boards : 4 * boards, :] = x_ref[2 * boards : 3 * boards, :]

    def place(half, ref):
        x_ref[0:boards, pl.ds(pl.multiple_of(half * lanes, 128), own_count)] = ref[...]
        x_ref[boards : 2 * boards, cols_of(half)] = x_ref[0:boards, cols_of(half)]

    row16 = iota((16, lanes), 0).astype(F32).astype(BF16)

    def hot_rows(half):
        def one(d, carry):
            low, high = c_ref[0:1, cols_of(half)], c_ref[1:2, cols_of(half)]
            df = d.astype(F32)
            partner = jnp.where(low == df, high, jnp.where(high == df, low, -1.0))
            for q in range(2):
                rel = partner - float(HALF * q)
                rel = jnp.where(rel < float(HALF), rel, -1.0)
                wide = jnp.broadcast_to(rel, (16, lanes)).astype(BF16)
                for part in range(2):
                    hit = wide == row16 + BF16(16 * part)
                    p_ref[q, d, 16 * part : 16 * part + 16, cols_of(half)] = jnp.where(hit, BF16(1), BF16(0))
            return carry

        lax.fori_loop(0, CARDS, one, 0)

    chunk = CARDS // 2

    def to_cards(half, more):
        for q in range(2):

            def one(i, carry):
                rows = p_ref[q, pl.ds(i * chunk, chunk), :, cols_of(half)].reshape(chunk * ROWS, lanes)
                got = lax.dot_general(rows, x_ref[:, cols_of(half)], NT, preferred_element_type=F32)
                got = got.reshape(chunk, ROWS, 4 * boards)
                if more:
                    got = got + o_ref[q, pl.ds(i * chunk, chunk)]
                o_ref[q, pl.ds(i * chunk, chunk)] = got
                return carry

            lax.fori_loop(0, 2, one, 0)

    place(me, reach_ref)
    hot_rows(me)
    to_cards(me, False)
    pl.semaphore_wait(barrier, len(plane + line + cross))
    swap = pltpu.make_async_remote_copy(
        reach_ref, swap_ref, swap_sem.at[0], swap_sem.at[1], device_id={"hand": 1 - me}, device_id_type=MESH
    )
    swap.start()
    hot_rows(1 - me)
    swap.wait()
    place(1 - me, swap_ref)
    to_cards(1 - me, True)
    f_ref[2] = x_ref[0:boards, :].astype(F32)

    first = iota((ROWS, 2 * boards), 1) < boards

    def pack(d, carry):
        w_ref[d] = jnp.where(first, o_ref[0, d, :, 0 : 2 * boards], o_ref[1, d, :, 0 : 2 * boards]).astype(BF16)
        g_ref[d] = jnp.where(first, o_ref[0, d, :, 2 * boards :], o_ref[1, d, :, 2 * boards :]).astype(BF16)
        return carry

    lax.fori_loop(0, CARDS, pack, 0)

    for half in range(2):
        rows = slice(16 * half, 16 * half + 16)

        def pairs(i, carry):
            mine = [g_ref[DBLOCK * i + k, rows, :] for k in range(DBLOCK)]
            sums = [None] * DBLOCK
            for e in range(CARDS):
                ge, we = g_ref[e, rows, :], w_ref[e, rows, :].astype(F32)
                for k in range(DBLOCK):
                    sign = lax.clamp(BF16(-1), mine[k] - ge, BF16(1))
                    term = sign.astype(F32) * we
                    sums[k] = term if sums[k] is None else sums[k] + term
            for k in range(DBLOCK):
                q_ref[DBLOCK * i + k, rows, :] = sums[k]
            return carry

        lax.fori_loop(0, CARDS // DBLOCK, pairs, 0)

    lo_row = iota((16, width), 0).astype(F32).astype(BF16)

    def table(g, carry):
        for b in range(GROUP):
            hi = jnp.broadcast_to(f_ref[0, pl.ds(GROUP * g + b, 1), :], (16, width)).astype(BF16)
            lo = jnp.broadcast_to(f_ref[1, pl.ds(GROUP * g + b, 1), :], (16, width)).astype(BF16)
            reach = jnp.broadcast_to(f_ref[2, pl.ds(GROUP * g + b, 1), :], (16, width)).astype(BF16)
            tile, start = 128 * (b % 2), 128 - SLOT // 2 * b
            for part in range(HI // 16):
                hit = hi == lo_row + BF16(16 * part)
                a_ref[HI * b + 16 * part : HI * b + 16 * part + 16, :] = jnp.where(hit, reach, BF16(0))
            for part in range(SLOT // 16):
                at = tile + (start + 16 * part) % 128
                b_ref[at : at + 16, :] = lax.clamp(
                    BF16(-1), lo_row + BF16(16 * part) - lo, BF16(1)
                )
        got = lax.dot_general(a_ref[...], b_ref[...], NT, preferred_element_type=F32)
        h_ref[0 : GROUP * HI, :] = got[:, 0:128]
        h_ref[GROUP * HI :, :] = got[:, 128:256]
        even = iota((GROUP, 128), 0) % 2 == 0
        block = ((iota((GROUP, 128), 1) + SLOT // 2 * iota((GROUP, 128), 0)) % 128) // SLOT
        for t in range(HI // 4):
            row = None
            for k in range(4):
                at = 4 * t + k
                part = jnp.where(
                    even,
                    h_ref[pl.ds(at, GROUP, stride=HI), :],
                    h_ref[pl.ds(at + GROUP * HI, GROUP, stride=HI), :],
                )
                part = pltpu.roll(part, SLOT * k, 1) if k else part
                row = part if row is None else jnp.where(block == k, part, row)
            t_ref[t, pl.ds(GROUP * g, GROUP), :] = pltpu.roll(row, 0, 1, stride=SLOT // 2, stride_axis=0)
        return carry

    lax.fori_loop(0, boards // GROUP, table, 0)

    tiles = HI // 4
    spot = iota((boards, 128), 1) % SLOT == LO
    below = []
    run = jnp.zeros((boards, 128), F32)
    whole = []
    for t in range(tiles):
        mark = jnp.where(spot, t_ref[t], 0.0)
        whole.append(mark)
        below.append(run)
        run = run + mark
    src, dst = iota((256, 128), 0), iota((256, 128), 1)
    at_spot = src % SLOT == LO
    within = (dst // SLOT > (src - 128) // SLOT).astype(F32) - (dst // SLOT < (src - 128) // SLOT).astype(F32)
    spread = jnp.where(at_spot, jnp.where(src < 128, 1.0, within), 0.0).astype(BF16)
    for t in range(tiles):
        outer = below[t] - (run - below[t] - whole[t])
        both = jnp.concatenate([outer, whole[t]], axis=1)
        high, low = split2(both)
        got = jnp.dot(jnp.concatenate([high, low], axis=0), spread, preferred_element_type=F32)
        t_ref[t] = t_ref[t] + got[:boards] + got[boards:]

    def look_up(g, carry):
        rows = pl.ds(pl.multiple_of(GROUP * g, GROUP), GROUP)
        for k in range(lanes // 128):
            cols = slice(128 * k, 128 * k + 128)
            hi = f_ref[0, rows, cols_of(me, 128 * k, 128)].astype(jnp.int32)
            lo = f_ref[1, rows, cols_of(me, 128 * k, 128)].astype(jnp.int32)
            tile = hi >> 2
            at = ((hi & 3) << 5) + lo
            found = jnp.zeros((GROUP, 128), F32)
            for t in range(tiles):
                got = jnp.take_along_axis(t_ref[t, rows, :], at, axis=1, mode="promise_in_bounds")
                found = jnp.where(tile == t, got, found)
            s_ref[rows, cols] = found
        return carry

    lax.fori_loop(0, boards // GROUP, look_up, 0)

    shared = jnp.zeros((2 * boards, lanes), F32)
    turned = jnp.transpose(q_ref[...].reshape(CARDS * ROWS, 2 * boards))
    for q in range(2):
        high, low = split2(turned[boards * q : boards * (q + 1)])
        shared = shared + jnp.dot(
            jnp.concatenate([high, low], axis=0),
            p_ref[q, :, :, cols_of(me)].reshape(CARDS * ROWS, lanes),
            preferred_element_type=F32,
        )

    card = iota((64, lanes), 0).astype(F32)
    card_totals = jnp.zeros((boards, 64), F32)
    for half in (1 - me, me):
        hold = ((card == c_ref[0:1, cols_of(half)]) | (card == c_ref[1:2, cols_of(half)])).astype(F32).astype(BF16)
        card_totals = card_totals + lax.dot_general(
            x_ref[0:boards, cols_of(half)], hold, NT, preferred_element_type=F32
        )
    high, low = split2(card_totals)
    held = jnp.dot(jnp.concatenate([high, low], axis=0), hold, preferred_element_type=F32)
    live = (
        0.5 * jnp.sum(card_totals, axis=1, keepdims=True)
        - (held[:boards] + held[boards:])
        + f_ref[2, :, cols_of(me)]
    )
    margin = s_ref[...] - (shared[:boards] + shared[boards:])
    pot, bet = column(pot_ref[...]), column(bet_ref[...])
    half_pot = 0.5 * pot
    call_value = ((half_pot + bet * pot) / hand_count) * margin
    stake = (half_pot / hand_count) * live
    values = jnp.maximum(call_value, -stake)
    values_ref[...] = values[:, 0:own_count]
    part = jnp.sum(values, axis=0, keepdims=True)[:, 0:own_count] / total_boards
    mass = jnp.sum(stake, axis=0, keepdims=True)[:, 0:own_count] / total_boards
    trav = trav_ref[...]
    numerator = jnp.sum(part * trav, axis=1, keepdims=True)
    denominator = jnp.sum(mass * trav, axis=1, keepdims=True)

    spot = XS * y + x
    mine_ref[0] = jnp.zeros((8, 128), F32)
    for k in range(lanes // 128):
        size = min(128, own_count - 128 * k)
        mine_ref[0, k : k + 1, 0:size] = part[:, 128 * k : 128 * k + size]
    mine_ref[0, 6:7, :] = jnp.where(iota((1, 128), 1) == 0, numerator, denominator)

    def exchange(source, groups):
        sent = []
        for peers, here, slots, sems in groups:
            for k, peer in enumerate(peers):
                copy = pltpu.make_async_remote_copy(
                    source, slots.at[here], sems.at[0, k], sems.at[1, here], device_id=peer, device_id_type=MESH
                )
                copy.start()
                sent.append(copy)
        return sent

    def arrived(source, where, slots, sems):
        pltpu.make_async_remote_copy(
            source, slots.at[where], sems.at[0, 0], sems.at[1, where], device_id=plane[0], device_id_type=MESH
        ).wait_recv()

    sent = exchange(mine_ref.at[0], [(plane, spot, plane_ref, plane_sem)])
    plane_ref[spot] = mine_ref[0]
    for peer in plane:
        arrived(mine_ref.at[0], XS * peer["board_0"] + peer["board_1"], plane_ref, plane_sem)
    mine_ref[1] = functools.reduce(jnp.add, [plane_ref[k] for k in range(YS * XS)])
    sent += exchange(mine_ref.at[1], [(line, z, line_ref, line_sem), (cross, z, cross_ref, cross_sem)])
    line_ref[z] = mine_ref[1]
    for peer in line:
        arrived(mine_ref.at[1], peer["board_2"], line_ref, line_sem)
    for peer in cross:
        arrived(mine_ref.at[1], peer["board_2"], cross_ref, cross_sem)
    total = functools.reduce(jnp.add, [line_ref[k] for k in range(ZS)])
    rest = functools.reduce(jnp.add, [cross_ref[k] for k in range(ZS)])
    hand_ref[...] = total
    ends = total[6:7] + rest[6:7]
    ratio_ref[...] = ends[:, 0:1] / ends[:, 1:2]
    for copy in sent:
        copy.wait_send()


def local(opp_reach, hand_rank, hand_cards, pot, bet_frac, trav_reach):
    boards, hand_count = hand_rank.shape
    own_count = opp_reach.shape[1]
    lanes = -(-own_count // 128) * 128
    width = 2 * lanes
    total_boards = boards * lax.axis_size(BOARD)
    whole = pl.BlockSpec(memory_space=pltpu.VMEM)
    board_values, hand_rows, ratio = pl.pallas_call(
        functools.partial(fused_kernel, total_boards, hand_count),
        out_shape=(
            jax.ShapeDtypeStruct((boards, own_count), F32),
            jax.ShapeDtypeStruct((8, 128), F32),
            jax.ShapeDtypeStruct((1, 1), F32),
        ),
        in_specs=[whole] * 6,
        out_specs=(whole,) * 3,
        scratch_shapes=[
            pltpu.VMEM((4 * boards, width), BF16),
            pltpu.VMEM((2, CARDS, ROWS, width), BF16),
            pltpu.VMEM((2, CARDS, ROWS, 4 * boards), F32),
            pltpu.VMEM((CARDS, ROWS, 2 * boards), BF16),
            pltpu.VMEM((CARDS, ROWS, 2 * boards), BF16),
            pltpu.VMEM((CARDS, ROWS, 2 * boards), F32),
            pltpu.VMEM((3, boards, width), F32),
            pltpu.VMEM((GROUP * HI, width), BF16),
            pltpu.VMEM((GROUP * SLOT, width), BF16),
            pltpu.VMEM((2 * GROUP * HI, 128), F32),
            pltpu.VMEM((HI // 4, boards, 128), F32),
            pltpu.VMEM((boards, lanes), F32),
            pltpu.VMEM((2, width), F32),
            pltpu.VMEM((boards, own_count), BF16),
            pltpu.VMEM((2, 8, 128), F32),
            pltpu.VMEM((YS * XS, 8, 128), F32),
            pltpu.VMEM((ZS, 8, 128), F32),
            pltpu.VMEM((ZS, 8, 128), F32),
            pltpu.SemaphoreType.DMA((2,)),
            pltpu.SemaphoreType.DMA((2, YS * XS)),
            pltpu.SemaphoreType.DMA((2, ZS)),
            pltpu.SemaphoreType.DMA((2, ZS)),
        ],
        compiler_params=pltpu.CompilerParams(
            vmem_limit_bytes=56 * 1024 * 1024, collective_id=0, has_side_effects=True
        ),
        cost_estimate=pl.CostEstimate(flops=10**9, bytes_accessed=10**6, transcendentals=0),
    )(opp_reach, hand_rank, hand_cards.T, pot[None, :], bet_frac[None, :], trav_reach[None, :])
    return board_values, hand_rows.reshape(-1)[:own_count], ratio[0, 0]


def solution(mesh):
    torus = Mesh(
        mesh.devices.reshape(YS, XS, ZS, mesh.shape["hand"]), ("board_0", "board_1", "board_2", "hand")
    )
    placed = (P(BOARD, "hand"), P(BOARD, None), P(), P(BOARD), P(BOARD), P("hand"))
    return jax.shard_map(
        local,
        mesh=torus,
        in_specs=placed,
        out_specs=(P(BOARD, "hand"), P("hand"), P()),
        check_vma=False,
    )
```

```python
import functools

import jax
import jax.numpy as jnp
from jax import lax
from jax.experimental import pallas as pl
from jax.experimental.pallas import tpu as pltpu
from jax.sharding import Mesh
from jax.sharding import PartitionSpec as P

CARDS = 52
BOARD = ("board_0", "board_1", "board_2")
BF16 = jnp.bfloat16
F32 = jnp.float32

PARTS = 4
SHARE = CARDS // PARTS
ROWS = 16
HI, LO = 48, 28
SLOT = 32
GROUP = 8
DBLOCK = 4
YS, XS, ZS = 4, 4, 8
MESH = pl.DeviceIdType.MESH
NT = (((1,), (1,)), ((), ()))


def iota(shape, axis):
    return lax.broadcasted_iota(jnp.int32, shape, axis)


def split2(x):
    high = x.astype(BF16)
    return high, (x - high.astype(F32)).astype(BF16)


def rank_code(rank):
    return (((rank & 127) | 128) << (rank >> 7)).astype(F32).astype(BF16)


def every_peer(places):
    y, x, z, h = places
    plane = [
        {"board_0": lax.rem(y + i, YS), "board_1": lax.rem(x + j, XS)}
        for i in range(YS)
        for j in range(XS)
        if i or j
    ]
    line = [{"board_2": lax.rem(z + i, ZS)} for i in range(1, ZS)]
    cross = [{"board_2": lax.rem(z + i, ZS), "hand": 1 - h} for i in range(ZS)]
    return plane, line, cross


def column(row, start, size):
    n = row.shape[1]
    hit = iota((size, n), 1) == iota((size, n), 0) + start
    return jnp.sum(jnp.where(hit, row, 0.0), axis=1, keepdims=True)


def fused_kernel(
    total_boards, hand_count,
    reach_ref, rank_ref, cards_ref, pot_ref, bet_ref, trav_ref,
    values_ref, hand_ref, ratio_ref,
    x_ref, p_ref, o_ref, w_ref, g_ref, q_ref, f_ref, a_ref, b_ref, h_ref, t_ref, s_ref, c_ref, k_ref,
    swap_ref, mine_ref, plane_ref, line_ref, cross_ref,
    swap_sem, pair_sem, total_sem, sum_sem, plane_sem, line_sem, cross_sem,
):
    all_boards, own_count = reach_ref.shape
    boards = all_boards // 2
    block = 4 * boards
    lanes = x_ref.shape[1] // 2
    width = 2 * lanes
    places = tuple(lax.axis_index(name) for name in BOARD) + (lax.axis_index("hand"),)
    y, x, z, me = places
    plane, line, cross = every_peer(places)
    barrier = pltpu.get_barrier_semaphore()
    for peer in plane + line + cross:
        pl.semaphore_signal(barrier, inc=1, device_id=peer, device_id_type=MESH)

    def cols_of(half, start=0, size=lanes):
        return pl.ds(pl.multiple_of(half * lanes + start, 128), size)

    def rows_of(core):
        return pl.ds(pl.multiple_of(core * boards, boards), boards)

    def to_partner(source, target, sems):
        copy = pltpu.make_async_remote_copy(
            source, target, sems.at[0], sems.at[1], device_id={"hand": 1 - me}, device_id_type=MESH
        )
        copy.start()
        return copy

    for half in range(2):
        start = half * lanes
        c_ref[:, start + lanes - 128 : start + lanes] = jnp.full((2, 128), -1.0, F32)
        c_ref[:, start : start + own_count] = cards_ref[:, half * own_count : (half + 1) * own_count].astype(F32)

    row16 = iota((16, width), 0)
    own_row = [
        jnp.where(row16 < SHARE, row16 + SHARE * q, -5).astype(F32).astype(BF16) for q in range(PARTS)
    ]

    def hot_rows(d, carry):
        low, high = c_ref[0:1, :], c_ref[1:2, :]
        df = d.astype(F32)
        partner = jnp.where(low == df, high, jnp.where(high == df, low, -1.0))
        wide = jnp.broadcast_to(partner, (16, width)).astype(BF16)
        for q in range(PARTS):
            p_ref[q, d] = jnp.where(wide == own_row[q], BF16(1), BF16(0))
        return carry

    lax.fori_loop(0, CARDS, hot_rows, 0)

    for half in range(2):
        start = half * lanes
        f_ref[0:2, :, start + lanes - 128 : start + lanes] = jnp.zeros((2, boards, 128), F32)
        x_ref[:, start + lanes - 128 : start + lanes] = jnp.zeros((8 * boards, 128), BF16)
        rank = rank_ref[rows_of(me), half * own_count : (half + 1) * own_count]
        x_ref[block : block + boards, start : start + own_count] = rank_code(rank)
        hi = (rank * 2341) >> 16
        f_ref[0, :, start : start + own_count] = hi.astype(F32)
        f_ref[1, :, start : start + own_count] = (rank - LO * hi).astype(F32)
    for k in range(1, PARTS):
        x_ref[block + k * boards : block + (k + 1) * boards, :] = x_ref[block : block + boards, :]

    def place(half, reach):
        x_ref[0:boards, pl.ds(pl.multiple_of(half * lanes, 128), own_count)] = reach
        for k in range(1, PARTS):
            x_ref[k * boards : (k + 1) * boards, cols_of(half)] = x_ref[0:boards, cols_of(half)]

    def to_cards(half, more):
        def one(q, carry):
            rows = p_ref[q, :, :, cols_of(half)].reshape(CARDS * ROWS, lanes)
            got = lax.dot_general(rows, x_ref[:, cols_of(half)], NT, preferred_element_type=F32)
            got = got.reshape(CARDS, ROWS, 2 * block)
            if more:
                got = got + o_ref[q]
            o_ref[q] = got
            return carry

        lax.fori_loop(0, PARTS, one, 0)

    place(me, reach_ref[rows_of(me), :])
    pl.semaphore_wait(barrier, len(plane + line + cross))
    swap = to_partner(reach_ref.at[rows_of(1 - me), :], swap_ref, swap_sem)
    to_cards(me, False)
    swap.wait()
    place(1 - me, swap_ref[...])
    to_cards(1 - me, True)
    f_ref[2] = x_ref[0:boards, :].astype(F32)

    part_of = iota((ROWS, block), 1) // boards

    def pack(d, carry):
        for ref, at in ((w_ref, 0), (g_ref, block)):
            got = o_ref[0, d, :, at : at + block]
            for q in range(1, PARTS):
                got = jnp.where(part_of == q, o_ref[q, d, :, at : at + block], got)
            ref[d] = got
        return carry

    lax.fori_loop(0, CARDS, pack, 0)

    def pairs(i, carry):
        mine = [g_ref[DBLOCK * i + k].astype(BF16) for k in range(DBLOCK)]
        sums = [None] * DBLOCK
        for e in range(CARDS):
            ge, we = g_ref[e].astype(BF16), w_ref[e].astype(BF16)
            for k in range(DBLOCK):
                sign = lax.clamp(BF16(-1), mine[k] - ge, BF16(1))
                term = sign.astype(F32) * we.astype(F32)
                sums[k] = term if sums[k] is None else sums[k] + term
        for k in range(DBLOCK):
            q_ref[0, DBLOCK * i + k] = sums[k]
        return carry

    lax.fori_loop(0, CARDS // DBLOCK, pairs, 0)
    pair_copy = to_partner(q_ref.at[0], q_ref.at[1], pair_sem)

    card = iota((64, lanes), 0).astype(F32)
    card_totals = jnp.zeros((boards, 64), F32)
    for half in (1 - me, me):
        hold = ((card == c_ref[0:1, cols_of(half)]) | (card == c_ref[1:2, cols_of(half)])).astype(F32).astype(BF16)
        card_totals = card_totals + lax.dot_general(
            x_ref[0:boards, cols_of(half)], hold, NT, preferred_element_type=F32
        )
    k_ref[0] = jnp.concatenate([card_totals, jnp.zeros((boards, 64), F32)], axis=1)
    total_copy = to_partner(k_ref.at[0], k_ref.at[1], total_sem)

    lo_row = row16.astype(F32).astype(BF16)
    even = iota((GROUP, 128), 0) % 2 == 0
    slot = ((iota((GROUP, 128), 1) + SLOT // 2 * iota((GROUP, 128), 0)) % 128) // SLOT
    tiles = HI // 4
    for g in range(boards // GROUP):
        now = g % 2
        for b in range(GROUP):
            at = GROUP * g + b
            hi = jnp.broadcast_to(f_ref[0, at : at + 1, :], (16, width)).astype(BF16)
            lo = jnp.broadcast_to(f_ref[1, at : at + 1, :], (16, width)).astype(BF16)
            reach = jnp.broadcast_to(f_ref[2, at : at + 1, :], (16, width)).astype(BF16)
            tile, start = 128 * (b % 2), 128 - SLOT // 2 * b
            for part in range(HI // 16):
                hit = hi == lo_row + BF16(16 * part)
                a_ref[now, HI * b + 16 * part : HI * b + 16 * part + 16, :] = jnp.where(hit, reach, BF16(0))
            for part in range(SLOT // 16):
                at = tile + (start + 16 * part) % 128
                b_ref[now, at : at + 16, :] = lax.clamp(BF16(-1), lo_row + BF16(16 * part) - lo, BF16(1))
        got = lax.dot_general(a_ref[now], b_ref[now], NT, preferred_element_type=F32)
        h_ref[now, 0 : GROUP * HI, :] = got[:, 0:128]
        h_ref[now, GROUP * HI :, :] = got[:, 128:256]
        for t in range(tiles):
            row = None
            for k in range(4):
                at = 4 * t + k
                part = jnp.where(
                    even,
                    h_ref[now, pl.ds(at, GROUP, stride=HI), :],
                    h_ref[now, pl.ds(at + GROUP * HI, GROUP, stride=HI), :],
                )
                part = pltpu.roll(part, SLOT * k, 1) if k else part
                row = part if row is None else jnp.where(slot == k, part, row)
            t_ref[t, GROUP * g : GROUP * (g + 1), :] = pltpu.roll(row, 0, 1, stride=SLOT // 2, stride_axis=0)

    spot = iota((boards, 128), 1) % SLOT == LO
    below = []
    run = jnp.zeros((boards, 128), F32)
    whole = []
    for t in range(tiles):
        mark = jnp.where(spot, t_ref[t], 0.0)
        whole.append(mark)
        below.append(run)
        run = run + mark
    src, dst = iota((256, 128), 0), iota((256, 128), 1)
    within = (dst // SLOT > (src - 128) // SLOT).astype(F32) - (dst // SLOT < (src - 128) // SLOT).astype(F32)
    spread = jnp.where(src % SLOT == LO, jnp.where(src < 128, 1.0, within), 0.0).astype(BF16)
    both = jnp.concatenate(
        [jnp.concatenate([below[t] - (run - below[t] - whole[t]), whole[t]], axis=1) for t in range(tiles)], axis=0
    )
    high, low = split2(both)
    got = jnp.dot(high, spread, preferred_element_type=F32) + jnp.dot(low, spread, preferred_element_type=F32)
    for t in range(tiles):
        t_ref[t] = t_ref[t] + got[boards * t : boards * (t + 1)]

    for half in (1 - me, me):

        def look_up(g, carry):
            rows = pl.ds(pl.multiple_of(GROUP * g, GROUP), GROUP)
            for k in range(lanes // 128):
                hi = f_ref[0, rows, cols_of(half, 128 * k, 128)].astype(jnp.int32)
                lo = f_ref[1, rows, cols_of(half, 128 * k, 128)].astype(jnp.int32)
                tile = hi >> 2
                at = ((hi & 3) << 5) + lo
                found = jnp.zeros((GROUP, 128), F32)
                for t in range(tiles):
                    got = jnp.take_along_axis(t_ref[t, rows, :], at, axis=1, mode="promise_in_bounds")
                    found = jnp.where(tile == t, got, found)
                s_ref[half, rows, 128 * k : 128 * k + 128] = found
            return carry

        lax.fori_loop(0, boards // GROUP, look_up, 0)
        if half is not me:
            sum_copy = to_partner(s_ref.at[1 - me], s_ref.at[2], sum_sem)

    pair_copy.wait()
    total_copy.wait()
    turned = [jnp.transpose(q_ref[k].reshape(CARDS * ROWS, block)) for k in range(2)]
    shared = jnp.zeros((4 * boards, lanes), F32)
    for q in range(PARTS):
        pieces = [split2(t[boards * q : boards * (q + 1)]) for t in turned]
        shared = shared + jnp.dot(
            jnp.concatenate([piece for pair in pieces for piece in pair], axis=0),
            p_ref[q, :, :, cols_of(me)].reshape(CARDS * ROWS, lanes),
            preferred_element_type=F32,
        )
    pieces = [split2(k_ref[k][:, 0:64]) for k in range(2)]
    held = jnp.dot(
        jnp.concatenate([piece for pair in pieces for piece in pair], axis=0), hold, preferred_element_type=F32
    )
    sum_copy.wait()
    part = mass = None
    for k, core in ((0, me), (1, 1 - me)):
        at = 2 * boards * k
        live = (
            0.5 * jnp.sum(k_ref[k][:, 0:64], axis=1, keepdims=True)
            - (held[at : at + boards] + held[at + boards : at + 2 * boards])
        )[:, 0:own_count] + reach_ref[rows_of(core), :].astype(F32)
        sums = s_ref[me] if k == 0 else s_ref[2]
        margin = (sums - (shared[at : at + boards] + shared[at + boards : at + 2 * boards]))[:, 0:own_count]
        pot = column(pot_ref[...], core * boards, boards)
        bet = column(bet_ref[...], core * boards, boards)
        half_pot = 0.5 * pot
        stake = (half_pot / hand_count) * live
        values = jnp.maximum(((half_pot + bet * pot) / hand_count) * margin, -stake)
        values_ref[rows_of(core), :] = values
        values, stake = (jnp.sum(v, axis=0, keepdims=True) for v in (values, stake))
        part = values if part is None else part + values
        mass = stake if mass is None else mass + stake
    part, mass = part / total_boards, mass / total_boards
    trav = trav_ref[...]
    numerator = jnp.sum(part * trav, axis=1, keepdims=True)
    denominator = jnp.sum(mass * trav, axis=1, keepdims=True)

    spot = XS * y + x
    mine_ref[0] = jnp.zeros((8, 128), F32)
    for k in range(lanes // 128):
        size = min(128, own_count - 128 * k)
        mine_ref[0, k : k + 1, 0:size] = part[:, 128 * k : 128 * k + size]
    mine_ref[0, 6:7, :] = jnp.where(iota((1, 128), 1) == 0, numerator, denominator)

    def exchange(source, groups):
        sent = []
        for peers, here, slots, sems in groups:
            for k, peer in enumerate(peers):
                copy = pltpu.make_async_remote_copy(
                    source, slots.at[here], sems.at[0, k], sems.at[1, here], device_id=peer, device_id_type=MESH
                )
                copy.start()
                sent.append(copy)
        return sent

    def arrived(source, where, slots, sems):
        pltpu.make_async_remote_copy(
            source, slots.at[where], sems.at[0, 0], sems.at[1, where], device_id=plane[0], device_id_type=MESH
        ).wait_recv()

    sent = exchange(mine_ref.at[0], [(plane, spot, plane_ref, plane_sem)])
    plane_ref[spot] = mine_ref[0]
    for peer in plane:
        arrived(mine_ref.at[0], XS * peer["board_0"] + peer["board_1"], plane_ref, plane_sem)
    mine_ref[1] = functools.reduce(jnp.add, [plane_ref[k] for k in range(YS * XS)])
    sent += exchange(mine_ref.at[1], [(line, z, line_ref, line_sem), (cross, z, cross_ref, cross_sem)])
    line_ref[z] = mine_ref[1]
    for peer in line:
        arrived(mine_ref.at[1], peer["board_2"], line_ref, line_sem)
    for peer in cross:
        arrived(mine_ref.at[1], peer["board_2"], cross_ref, cross_sem)
    total = functools.reduce(jnp.add, [line_ref[k] for k in range(ZS)])
    rest = functools.reduce(jnp.add, [cross_ref[k] for k in range(ZS)])
    hand_ref[...] = total
    ends = total[6:7] + rest[6:7]
    ratio_ref[...] = ends[:, 0:1] / ends[:, 1:2]
    for copy in sent:
        copy.wait_send()


def local(opp_reach, hand_rank, hand_cards, pot, bet_frac, trav_reach):
    boards, hand_count = hand_rank.shape
    own_count = opp_reach.shape[1]
    lanes = -(-own_count // 128) * 128
    width = 2 * lanes
    half = boards // 2
    total_boards = boards * lax.axis_size(BOARD)
    whole = pl.BlockSpec(memory_space=pltpu.VMEM)
    board_values, hand_rows, ratio = pl.pallas_call(
        functools.partial(fused_kernel, total_boards, hand_count),
        out_shape=(
            jax.ShapeDtypeStruct((boards, own_count), F32),
            jax.ShapeDtypeStruct((8, 128), F32),
            jax.ShapeDtypeStruct((1, 1), F32),
        ),
        in_specs=[whole] * 6,
        out_specs=(whole,) * 3,
        scratch_shapes=[
            pltpu.VMEM((8 * half, width), BF16),
            pltpu.VMEM((PARTS, CARDS, ROWS, width), BF16),
            pltpu.VMEM((PARTS, CARDS, ROWS, 8 * half), F32),
            pltpu.VMEM((CARDS, ROWS, 4 * half), F32),
            pltpu.VMEM((CARDS, ROWS, 4 * half), F32),
            pltpu.VMEM((2, CARDS, ROWS, 4 * half), F32),
            pltpu.VMEM((3, half, width), F32),
            pltpu.VMEM((2, GROUP * HI, width), BF16),
            pltpu.VMEM((2, GROUP * SLOT, width), BF16),
            pltpu.VMEM((2, 2 * GROUP * HI, 128), F32),
            pltpu.VMEM((HI // 4, half, 128), F32),
            pltpu.VMEM((3, half, lanes), F32),
            pltpu.VMEM((2, width), F32),
            pltpu.VMEM((2, half, 128), F32),
            pltpu.VMEM((half, own_count), BF16),
            pltpu.VMEM((2, 8, 128), F32),
            pltpu.VMEM((YS * XS, 8, 128), F32),
            pltpu.VMEM((ZS, 8, 128), F32),
            pltpu.VMEM((ZS, 8, 128), F32),
            pltpu.SemaphoreType.DMA((2,)),
            pltpu.SemaphoreType.DMA((2,)),
            pltpu.SemaphoreType.DMA((2,)),
            pltpu.SemaphoreType.DMA((2,)),
            pltpu.SemaphoreType.DMA((2, YS * XS)),
            pltpu.SemaphoreType.DMA((2, ZS)),
            pltpu.SemaphoreType.DMA((2, ZS)),
        ],
        compiler_params=pltpu.CompilerParams(
            vmem_limit_bytes=56 * 1024 * 1024, collective_id=0, has_side_effects=True
        ),
        cost_estimate=pl.CostEstimate(flops=10**9, bytes_accessed=10**6, transcendentals=0),
    )(opp_reach, hand_rank, hand_cards.T, pot[None, :], bet_frac[None, :], trav_reach[None, :])
    return board_values, hand_rows.reshape(-1)[:own_count], ratio[0, 0]


def solution(mesh):
    torus = Mesh(
        mesh.devices.reshape(YS, XS, ZS, mesh.shape["hand"]), ("board_0", "board_1", "board_2", "hand")
    )
    placed = (P(BOARD, "hand"), P(BOARD, None), P(), P(BOARD), P(BOARD), P("hand"))
    return jax.shard_map(
        local,
        mesh=torus,
        in_specs=placed,
        out_specs=(P(BOARD, "hand"), P("hand"), P()),
        check_vma=False,
    )
```

```python
import functools

import jax
import jax.numpy as jnp
from jax import lax
from jax.experimental import pallas as pl
from jax.experimental.pallas import tpu as pltpu
from jax.sharding import Mesh
from jax.sharding import PartitionSpec as P

CARDS = 52
BOARD = ("board_0", "board_1", "board_2")
BF16 = jnp.bfloat16
F32 = jnp.float32

PARTS = 4
SHARE = CARDS // PARTS
ROWS = 16
HI, LO = 48, 28
SLOT = 32
GROUP = 8
DBLOCK = 4
YS, XS, ZS = 4, 4, 8
MESH = pl.DeviceIdType.MESH
NT = (((1,), (1,)), ((), ()))


def iota(shape, axis):
    return lax.broadcasted_iota(jnp.int32, shape, axis)


def split2(x):
    high = x.astype(BF16)
    return high, (x - high.astype(F32)).astype(BF16)


def rank_code(rank):
    return (((rank & 127) | 128) << (rank >> 7)).astype(F32).astype(BF16)


def every_peer(places):
    y, x, z, h = places
    plane = [
        {"board_0": lax.rem(y + i, YS), "board_1": lax.rem(x + j, XS)}
        for i in range(YS)
        for j in range(XS)
        if i or j
    ]
    line = [{"board_2": lax.rem(z + i, ZS)} for i in range(1, ZS)]
    cross = [{"board_2": lax.rem(z + i, ZS), "hand": 1 - h} for i in range(ZS)]
    return plane, line, cross


def column(row, start, size):
    n = row.shape[1]
    hit = iota((size, n), 1) == iota((size, n), 0) + start
    return jnp.sum(jnp.where(hit, row, 0.0), axis=1, keepdims=True)


def fused_kernel(
    total_boards, hand_count,
    reach_hbm, rank_hbm, cards_hbm, pot_hbm, bet_hbm, trav_hbm,
    values_hbm, hand_ref, ratio_ref,
    reach_ref, rank_ref, cards_ref, pot_ref, bet_ref, trav_ref, values_ref, io_sem,
    x_ref, p_ref, o_ref, w_ref, g_ref, q_ref, f_ref, a_ref, b_ref, h_ref, t_ref, s_ref, c_ref, k_ref,
    swap_ref, mine_ref, plane_ref, line_ref, cross_ref,
    swap_sem, pair_sem, total_sem, sum_sem, plane_sem, line_sem, cross_sem,
):
    all_boards, own_count = reach_ref.shape
    boards = all_boards // 2
    block = 4 * boards
    lanes = x_ref.shape[1] // 2
    width = 2 * lanes
    places = tuple(lax.axis_index(name) for name in BOARD) + (lax.axis_index("hand"),)
    y, x, z, me = places
    plane, line, cross = every_peer(places)
    barrier = pltpu.get_barrier_semaphore()

    def cols_of(half, start=0, size=lanes):
        return pl.ds(pl.multiple_of(half * lanes + start, 128), size)

    def rows_of(core):
        return pl.ds(pl.multiple_of(core * boards, boards), boards)

    def to_partner(source, target, sems):
        copy = pltpu.make_async_remote_copy(
            source, target, sems.at[0], sems.at[1], device_id={"hand": 1 - me}, device_id_type=MESH
        )
        copy.start()
        return copy

    loads = [
        pltpu.make_async_copy(source, target, io_sem.at[k])
        for k, (source, target) in enumerate(
            (
                (cards_hbm, cards_ref),
                (rank_hbm.at[rows_of(me), :], rank_ref),
                (reach_hbm, reach_ref),
                (pot_hbm, pot_ref),
                (bet_hbm, bet_ref),
                (trav_hbm, trav_ref),
            )
        )
    ]
    for load in loads:
        load.start()
    for peer in plane + line + cross:
        pl.semaphore_signal(barrier, inc=1, device_id=peer, device_id_type=MESH)

    loads[0].wait()
    for half in range(2):
        start = half * lanes
        c_ref[:, start + lanes - 128 : start + lanes] = jnp.full((2, 128), -1.0, F32)
        c_ref[:, start : start + own_count] = cards_ref[:, half * own_count : (half + 1) * own_count].astype(F32)

    row16 = iota((16, width), 0)
    own_row = [
        jnp.where(row16 < SHARE, row16 + SHARE * q, -5).astype(F32).astype(BF16) for q in range(PARTS)
    ]

    def hot_rows(d, carry):
        low, high = c_ref[0:1, :], c_ref[1:2, :]
        df = d.astype(F32)
        partner = jnp.where(low == df, high, jnp.where(high == df, low, -1.0))
        wide = jnp.broadcast_to(partner, (16, width)).astype(BF16)
        for q in range(PARTS):
            p_ref[q, d] = jnp.where(wide == own_row[q], BF16(1), BF16(0))
        return carry

    lax.fori_loop(0, CARDS, hot_rows, 0)

    loads[1].wait()
    loads[2].wait()
    for half in range(2):
        start = half * lanes
        f_ref[0:2, :, start + lanes - 128 : start + lanes] = jnp.zeros((2, boards, 128), F32)
        x_ref[:, start + lanes - 128 : start + lanes] = jnp.zeros((8 * boards, 128), BF16)
        rank = rank_ref[:, half * own_count : (half + 1) * own_count]
        x_ref[block : block + boards, start : start + own_count] = rank_code(rank)
        hi = (rank * 2341) >> 16
        f_ref[0, :, start : start + own_count] = hi.astype(F32)
        f_ref[1, :, start : start + own_count] = (rank - LO * hi).astype(F32)
    for k in range(1, PARTS):
        x_ref[block + k * boards : block + (k + 1) * boards, :] = x_ref[block : block + boards, :]

    def place(half, reach):
        x_ref[0:boards, pl.ds(pl.multiple_of(half * lanes, 128), own_count)] = reach
        f_ref[2, :, cols_of(half)] = x_ref[0:boards, cols_of(half)].astype(F32)
        for k in range(1, PARTS):
            x_ref[k * boards : (k + 1) * boards, cols_of(half)] = x_ref[0:boards, cols_of(half)]

    def to_cards(half, more):
        for q in range(PARTS):
            rows = p_ref[q, :, :, cols_of(half)].reshape(CARDS * ROWS, lanes)
            got = lax.dot_general(rows, x_ref[:, cols_of(half)], NT, preferred_element_type=F32)
            got = got.reshape(CARDS, ROWS, 2 * block)
            o_ref[q] = got + o_ref[q] if more else got

    digit = iota((16, lanes), 0).astype(F32).astype(BF16)

    def high_factor(half):
        for b in range(boards):
            hi = jnp.broadcast_to(f_ref[0, b : b + 1, cols_of(half)], (16, lanes)).astype(BF16)
            reach = jnp.broadcast_to(f_ref[2, b : b + 1, cols_of(half)], (16, lanes)).astype(BF16)
            for part in range(HI // 16):
                at = HI * (b % GROUP) + 16 * part
                hit = hi == digit + BF16(16 * part)
                a_ref[b // GROUP, at : at + 16, cols_of(half)] = jnp.where(hit, reach, BF16(0))

    def low_factor(half):
        for b in range(boards):
            lo = jnp.broadcast_to(f_ref[1, b : b + 1, cols_of(half)], (16, lanes)).astype(BF16)
            for part in range(SLOT // 16):
                at = 128 * (b % 2) + (128 - SLOT // 2 * (b % GROUP) + 16 * part) % 128
                b_ref[b // GROUP, at : at + 16, cols_of(half)] = lax.clamp(
                    BF16(-1), digit + BF16(16 * part) - lo, BF16(1)
                )

    place(me, reach_ref[rows_of(me), :])
    to_cards(me, False)
    pl.semaphore_wait(barrier, len(plane + line + cross))
    swap = to_partner(reach_ref.at[rows_of(1 - me), :], swap_ref, swap_sem)
    low_factor(0)
    low_factor(1)
    high_factor(me)
    swap.wait()
    place(1 - me, swap_ref[...])
    high_factor(1 - me)
    to_cards(1 - me, True)

    part_of = iota((ROWS, block), 1) // boards

    def pack(d, carry):
        for ref, at in ((w_ref, 0), (g_ref, block)):
            got = o_ref[0, d, :, at : at + block]
            for q in range(1, PARTS):
                got = jnp.where(part_of == q, o_ref[q, d, :, at : at + block], got)
            ref[d] = got
        return carry

    lax.fori_loop(0, CARDS, pack, 0)

    def pairs(i, carry):
        mine = [g_ref[DBLOCK * i + k].astype(BF16) for k in range(DBLOCK)]
        sums = [None] * DBLOCK
        for e in range(CARDS):
            ge, we = g_ref[e].astype(BF16), w_ref[e].astype(BF16)
            for k in range(DBLOCK):
                sign = lax.clamp(BF16(-1), mine[k] - ge, BF16(1))
                term = sign.astype(F32) * we.astype(F32)
                sums[k] = term if sums[k] is None else sums[k] + term
        for k in range(DBLOCK):
            q_ref[0, DBLOCK * i + k] = sums[k]
        return carry

    lax.fori_loop(0, CARDS // DBLOCK, pairs, 0)
    pair_copy = to_partner(q_ref.at[0], q_ref.at[1], pair_sem)

    card = iota((64, lanes), 0).astype(F32)
    card_totals = jnp.zeros((boards, 64), F32)
    for half in (1 - me, me):
        hold = ((card == c_ref[0:1, cols_of(half)]) | (card == c_ref[1:2, cols_of(half)])).astype(F32).astype(BF16)
        card_totals = card_totals + lax.dot_general(
            x_ref[0:boards, cols_of(half)], hold, NT, preferred_element_type=F32
        )
    k_ref[0] = jnp.concatenate([card_totals, jnp.zeros((boards, 64), F32)], axis=1)
    total_copy = to_partner(k_ref.at[0], k_ref.at[1], total_sem)

    even = iota((GROUP, 128), 0) % 2 == 0
    slot = ((iota((GROUP, 128), 1) + SLOT // 2 * iota((GROUP, 128), 0)) % 128) // SLOT
    tiles = HI // 4
    for g in range(boards // GROUP):
        now = g % 2
        got = lax.dot_general(a_ref[g], b_ref[g], NT, preferred_element_type=F32)
        h_ref[now, 0 : GROUP * HI, :] = got[:, 0:128]
        h_ref[now, GROUP * HI :, :] = got[:, 128:256]
        for t in range(tiles):
            row = None
            for k in range(4):
                at = 4 * t + k
                part = jnp.where(
                    even,
                    h_ref[now, pl.ds(at, GROUP, stride=HI), :],
                    h_ref[now, pl.ds(at + GROUP * HI, GROUP, stride=HI), :],
                )
                part = pltpu.roll(part, SLOT * k, 1) if k else part
                row = part if row is None else jnp.where(slot == k, part, row)
            t_ref[t, GROUP * g : GROUP * (g + 1), :] = pltpu.roll(row, 0, 1, stride=SLOT // 2, stride_axis=0)

    spot = iota((boards, 128), 1) % SLOT == LO
    below = []
    run = jnp.zeros((boards, 128), F32)
    whole = []
    for t in range(tiles):
        mark = jnp.where(spot, t_ref[t], 0.0)
        whole.append(mark)
        below.append(run)
        run = run + mark
    src, dst = iota((256, 128), 0), iota((256, 128), 1)
    within = (dst // SLOT > (src - 128) // SLOT).astype(F32) - (dst // SLOT < (src - 128) // SLOT).astype(F32)
    spread = jnp.where(src % SLOT == LO, jnp.where(src < 128, 1.0, within), 0.0).astype(BF16)
    both = jnp.concatenate(
        [jnp.concatenate([below[t] - (run - below[t] - whole[t]), whole[t]], axis=1) for t in range(tiles)], axis=0
    )
    high, low = split2(both)
    got = jnp.dot(high, spread, preferred_element_type=F32) + jnp.dot(low, spread, preferred_element_type=F32)
    for t in range(tiles):
        t_ref[t] = t_ref[t] + got[boards * t : boards * (t + 1)]

    for half in (1 - me, me):
        for g in range(boards // GROUP):
            rows = slice(GROUP * g, GROUP * (g + 1))
            for k in range(lanes // 128):
                hi = f_ref[0, rows, cols_of(half, 128 * k, 128)].astype(jnp.int32)
                lo = f_ref[1, rows, cols_of(half, 128 * k, 128)].astype(jnp.int32)
                tile = hi >> 2
                at = ((hi & 3) << 5) + lo
                found = jnp.zeros((GROUP, 128), F32)
                for t in range(tiles):
                    got = jnp.take_along_axis(t_ref[t, rows, :], at, axis=1, mode="promise_in_bounds")
                    found = jnp.where(tile == t, got, found)
                s_ref[half, rows, 128 * k : 128 * k + 128] = found
        if half is not me:
            sum_copy = to_partner(s_ref.at[1 - me], s_ref.at[2], sum_sem)

    pair_copy.wait()
    total_copy.wait()
    turned = [jnp.transpose(q_ref[k].reshape(CARDS * ROWS, block)) for k in range(2)]
    shared = jnp.zeros((4 * boards, lanes), F32)
    for q in range(PARTS):
        pieces = [split2(t[boards * q : boards * (q + 1)]) for t in turned]
        shared = shared + jnp.dot(
            jnp.concatenate([piece for pair in pieces for piece in pair], axis=0),
            p_ref[q, :, :, cols_of(me)].reshape(CARDS * ROWS, lanes),
            preferred_element_type=F32,
        )
    pieces = [split2(k_ref[k][:, 0:64]) for k in range(2)]
    held = jnp.dot(
        jnp.concatenate([piece for pair in pieces for piece in pair], axis=0), hold, preferred_element_type=F32
    )
    sum_copy.wait()
    for load in loads[3:]:
        load.wait()
    part = mass = None
    for k, core in ((0, me), (1, 1 - me)):
        at = 2 * boards * k
        live = (
            0.5 * jnp.sum(k_ref[k][:, 0:64], axis=1, keepdims=True)
            - (held[at : at + boards] + held[at + boards : at + 2 * boards])
        )[:, 0:own_count] + reach_ref[rows_of(core), :].astype(F32)
        sums = s_ref[me] if k == 0 else s_ref[2]
        margin = (sums - (shared[at : at + boards] + shared[at + boards : at + 2 * boards]))[:, 0:own_count]
        pot = column(pot_ref[...], core * boards, boards)
        bet = column(bet_ref[...], core * boards, boards)
        half_pot = 0.5 * pot
        stake = half_pot * live
        values = jnp.maximum((half_pot + bet * pot) * margin, -stake)
        values_ref[rows_of(core), :] = values
        values, stake = (jnp.sum(v, axis=0, keepdims=True) for v in (values, stake))
        part = values if part is None else part + values
        mass = stake if mass is None else mass + stake
    save = pltpu.make_async_copy(values_ref, values_hbm, io_sem.at[6])
    save.start()
    scale = 1.0 / (hand_count * total_boards)
    part, mass = part * scale, mass * scale
    trav = trav_ref[...].reshape(1, own_count)
    numerator = jnp.sum(part * trav, axis=1, keepdims=True)
    denominator = jnp.sum(mass * trav, axis=1, keepdims=True)

    spot = XS * y + x
    mine_ref[0] = jnp.zeros((8, 128), F32)
    for k in range(lanes // 128):
        size = min(128, own_count - 128 * k)
        mine_ref[0, k : k + 1, 0:size] = part[:, 128 * k : 128 * k + size]
    mine_ref[0, 6:7, :] = jnp.where(iota((1, 128), 1) == 0, numerator, denominator)

    def exchange(source, groups):
        sent = []
        for peers, here, slots, sems in groups:
            for k, peer in enumerate(peers):
                copy = pltpu.make_async_remote_copy(
                    source, slots.at[here], sems.at[0, k], sems.at[1, here], device_id=peer, device_id_type=MESH
                )
                copy.start()
                sent.append(copy)
        return sent

    def arrived(source, where, slots, sems):
        pltpu.make_async_remote_copy(
            source, slots.at[where], sems.at[0, 0], sems.at[1, where], device_id=plane[0], device_id_type=MESH
        ).wait_recv()

    sent = exchange(mine_ref.at[0], [(plane, spot, plane_ref, plane_sem)])
    plane_ref[spot] = mine_ref[0]
    for peer in plane:
        arrived(mine_ref.at[0], XS * peer["board_0"] + peer["board_1"], plane_ref, plane_sem)
    mine_ref[1] = functools.reduce(jnp.add, [plane_ref[k] for k in range(YS * XS)])
    sent += exchange(mine_ref.at[1], [(line, z, line_ref, line_sem), (cross, z, cross_ref, cross_sem)])
    line_ref[z] = mine_ref[1]
    for peer in line:
        arrived(mine_ref.at[1], peer["board_2"], line_ref, line_sem)
    for peer in cross:
        arrived(mine_ref.at[1], peer["board_2"], cross_ref, cross_sem)
    total = functools.reduce(jnp.add, [line_ref[k] for k in range(ZS)])
    rest = functools.reduce(jnp.add, [cross_ref[k] for k in range(ZS)])
    hand_ref[...] = total
    ends = total[6:7] + rest[6:7]
    ratio_ref[...] = ends[:, 0:1] / ends[:, 1:2]
    save.wait()
    for copy in sent:
        copy.wait_send()


def local(opp_reach, hand_rank, hand_cards, pot, bet_frac, trav_reach):
    boards, hand_count = hand_rank.shape
    own_count = opp_reach.shape[1]
    lanes = -(-own_count // 128) * 128
    width = 2 * lanes
    half = boards // 2
    total_boards = boards * lax.axis_size(BOARD)
    whole = pl.BlockSpec(memory_space=pltpu.VMEM)
    board_values, hand_rows, ratio = pl.pallas_call(
        functools.partial(fused_kernel, total_boards, hand_count),
        out_shape=(
            jax.ShapeDtypeStruct((boards, own_count), F32),
            jax.ShapeDtypeStruct((8, 128), F32),
            jax.ShapeDtypeStruct((1, 1), F32),
        ),
        in_specs=[pl.BlockSpec(memory_space=pl.ANY)] * 6,
        out_specs=(pl.BlockSpec(memory_space=pl.ANY), whole, whole),
        scratch_shapes=[
            pltpu.VMEM((boards, own_count), BF16),
            pltpu.VMEM((half, hand_count), jnp.int32),
            pltpu.VMEM((2, hand_count), jnp.int32),
            pltpu.VMEM((1, boards), F32),
            pltpu.VMEM((1, boards), F32),
            pltpu.VMEM((own_count,), F32),
            pltpu.VMEM((boards, own_count), F32),
            pltpu.SemaphoreType.DMA((7,)),
            pltpu.VMEM((8 * half, width), BF16),
            pltpu.VMEM((PARTS, CARDS, ROWS, width), BF16),
            pltpu.VMEM((PARTS, CARDS, ROWS, 8 * half), F32),
            pltpu.VMEM((CARDS, ROWS, 4 * half), F32),
            pltpu.VMEM((CARDS, ROWS, 4 * half), F32),
            pltpu.VMEM((2, CARDS, ROWS, 4 * half), F32),
            pltpu.VMEM((3, half, width), F32),
            pltpu.VMEM((half // GROUP, GROUP * HI, width), BF16),
            pltpu.VMEM((half // GROUP, GROUP * SLOT, width), BF16),
            pltpu.VMEM((2, 2 * GROUP * HI, 128), F32),
            pltpu.VMEM((HI // 4, half, 128), F32),
            pltpu.VMEM((3, half, lanes), F32),
            pltpu.VMEM((2, width), F32),
            pltpu.VMEM((2, half, 128), F32),
            pltpu.VMEM((half, own_count), BF16),
            pltpu.VMEM((2, 8, 128), F32),
            pltpu.VMEM((YS * XS, 8, 128), F32),
            pltpu.VMEM((ZS, 8, 128), F32),
            pltpu.VMEM((ZS, 8, 128), F32),
            pltpu.SemaphoreType.DMA((2,)),
            pltpu.SemaphoreType.DMA((2,)),
            pltpu.SemaphoreType.DMA((2,)),
            pltpu.SemaphoreType.DMA((2,)),
            pltpu.SemaphoreType.DMA((2, YS * XS)),
            pltpu.SemaphoreType.DMA((2, ZS)),
            pltpu.SemaphoreType.DMA((2, ZS)),
        ],
        compiler_params=pltpu.CompilerParams(
            vmem_limit_bytes=56 * 1024 * 1024, collective_id=0, has_side_effects=True
        ),
        cost_estimate=pl.CostEstimate(flops=10**9, bytes_accessed=10**6, transcendentals=0),
    )(opp_reach, hand_rank, hand_cards.T, pot[None, :], bet_frac[None, :], trav_reach)
    return board_values * (1.0 / hand_count), hand_rows.reshape(-1)[:own_count], ratio[0, 0]


def solution(mesh):
    torus = Mesh(
        mesh.devices.reshape(YS, XS, ZS, mesh.shape["hand"]), ("board_0", "board_1", "board_2", "hand")
    )
    placed = (P(BOARD, "hand"), P(BOARD, None), P(), P(BOARD), P(BOARD), P("hand"))
    return jax.shard_map(
        local,
        mesh=torus,
        in_specs=placed,
        out_specs=(P(BOARD, "hand"), P("hand"), P()),
        check_vma=False,
    )
```

```python
import functools

import jax
import jax.numpy as jnp
from jax import lax
from jax.experimental import pallas as pl
from jax.experimental.pallas import tpu as pltpu
from jax.sharding import Mesh
from jax.sharding import PartitionSpec as P

CARDS = 52
BOARD = ("board_0", "board_1", "board_2")
BF16 = jnp.bfloat16
F32 = jnp.float32

PARTS = 4
SHARE = CARDS // PARTS
ROWS = 16
HI, LO = 48, 28
SLOT = 32
GROUP = 8
DBLOCK = 4
YS, XS, ZS = 4, 4, 8
MESH = pl.DeviceIdType.MESH
NT = (((1,), (1,)), ((), ()))


def iota(shape, axis):
    return lax.broadcasted_iota(jnp.int32, shape, axis)


def split2(x):
    high = x.astype(BF16)
    return high, (x - high.astype(F32)).astype(BF16)


def rank_code(rank):
    return (((rank & 127) | 128) << (rank >> 7)).astype(F32).astype(BF16)


def every_peer(places):
    y, x, z, h = places
    plane = [
        {"board_0": lax.rem(y + i, YS), "board_1": lax.rem(x + j, XS)}
        for i in (2, 1, 3, 0)
        for j in (2, 1, 3, 0)
        if i or j
    ]
    line = [{"board_2": lax.rem(z + i, ZS)} for i in (4, 3, 5, 2, 6, 1, 7)]
    cross = [{"board_2": lax.rem(z + i, ZS), "hand": 1 - h} for i in (4, 3, 5, 2, 6, 1, 7, 0)]
    return plane, line, cross


def column(row, start, size):
    n = row.shape[1]
    hit = iota((size, n), 1) == iota((size, n), 0) + start
    return jnp.sum(jnp.where(hit, row, 0.0), axis=1, keepdims=True)


def fused_kernel(
    total_boards, hand_count,
    reach_hbm, rank_hbm, cards_hbm, pot_hbm, bet_hbm, trav_hbm,
    values_ref, hand_ref, ratio_ref,
    reach_ref, rank_ref, cards_ref, pot_ref, bet_ref, trav_ref, io_sem,
    x_ref, p_ref, o_ref, w_ref, g_ref, q_ref, l_ref, f_ref, a_ref, b_ref, h0_ref, h1_ref, h2_ref, h3_ref, t0_ref, t1_ref, t2_ref, t3_ref, s_ref, c_ref,
    swap_ref, mine_ref, plane_ref, line_ref, cross_ref,
    swap_sem, pair_sem, sum_sem, plane_sem, line_sem, cross_sem,
):
    all_boards, own_count = reach_ref.shape
    boards = all_boards // 2
    block = 4 * boards
    lanes = x_ref.shape[1] // 2
    width = 2 * lanes
    places = tuple(lax.axis_index(name) for name in BOARD) + (lax.axis_index("hand"),)
    y, x, z, me = places
    plane, line, cross = every_peer(places)
    barrier = pltpu.get_barrier_semaphore()

    def cols_of(half, start=0, size=lanes):
        return pl.ds(pl.multiple_of(half * lanes + start, 128), size)

    def rows_of(core):
        return pl.ds(pl.multiple_of(core * boards, boards), boards)

    def to_partner(source, target, sems):
        copy = pltpu.make_async_remote_copy(
            source, target, sems.at[0], sems.at[1], device_id={"hand": 1 - me}, device_id_type=MESH
        )
        copy.start()
        return copy

    loads = [
        pltpu.make_async_copy(source, target, io_sem.at[k])
        for k, (source, target) in enumerate(
            (
                (cards_hbm, cards_ref),
                (rank_hbm.at[rows_of(me), :], rank_ref),
                (reach_hbm, reach_ref),
                (pot_hbm, pot_ref),
                (bet_hbm, bet_ref),
                (trav_hbm, trav_ref),
            )
        )
    ]
    for load in loads:
        load.start()
    for peer in plane + line + cross:
        pl.semaphore_signal(barrier, inc=1, device_id=peer, device_id_type=MESH)

    loads[0].wait()
    for half in range(2):
        start = half * lanes
        c_ref[:, start + lanes - 128 : start + lanes] = jnp.full((2, 128), -1.0, F32)
        c_ref[:, start : start + own_count] = cards_ref[:, half * own_count : (half + 1) * own_count].astype(F32)

    row16 = iota((16, lanes), 0)
    own_row = [
        jnp.where(row16 < SHARE, row16 + SHARE * q, -5).astype(F32).astype(BF16) for q in range(PARTS)
    ]

    def hot_rows(half, d):
        low, high = c_ref[0:1, cols_of(half)], c_ref[1:2, cols_of(half)]
        partner = jnp.where(low == float(d), high, jnp.where(high == float(d), low, -1.0))
        wide = jnp.broadcast_to(partner, (16, lanes)).astype(BF16)
        for q in range(PARTS):
            p_ref[d, q, :, cols_of(half)] = jnp.where(wide == own_row[q], BF16(1), BF16(0))

    loads[1].wait()
    loads[2].wait()
    for half in range(2):
        start = half * lanes
        f_ref[0:2, :, start + lanes - 128 : start + lanes] = jnp.zeros((2, boards, 128), F32)
        x_ref[:, start + lanes - 128 : start + lanes] = jnp.zeros((8 * boards, 128), BF16)
        rank = rank_ref[:, half * own_count : (half + 1) * own_count]
        x_ref[block : block + boards, start : start + own_count] = rank_code(rank)
        hi = (rank * 2341) >> 16
        f_ref[0, :, start : start + own_count] = hi.astype(F32)
        f_ref[1, :, start : start + own_count] = (rank - LO * hi).astype(F32)
    for k in range(1, PARTS):
        x_ref[block + k * boards : block + (k + 1) * boards, :] = x_ref[block : block + boards, :]

    def place(half, reach):
        x_ref[0:boards, pl.ds(pl.multiple_of(half * lanes, 128), own_count)] = reach
        f_ref[2, :, cols_of(half)] = x_ref[0:boards, cols_of(half)].astype(F32)
        for k in range(1, PARTS):
            x_ref[k * boards : (k + 1) * boards, cols_of(half)] = x_ref[0:boards, cols_of(half)]

    chunk = CARDS // PARTS

    def to_cards(half, more):
        for i in range(PARTS):
            these = slice(chunk * i, chunk * (i + 1))
            if not more:
                for d in range(chunk * i, chunk * (i + 1)):
                    hot_rows(half, d)
            if more:
                low_factor(half, i)
                high_factor(half, i)
            rows = p_ref[these, :, :, cols_of(half)].reshape(chunk * PARTS * ROWS, lanes)
            got = lax.dot_general(rows, x_ref[:, cols_of(half)], NT, preferred_element_type=F32)
            got = got.reshape(chunk, PARTS, ROWS, 2 * block)
            o_ref[these] = got + o_ref[these] if more else got

    digit = iota((16, lanes), 0).astype(F32).astype(BF16)

    def high_factor(half, g):
        for b in range(GROUP):
            at = GROUP * g + b
            hi = jnp.broadcast_to(f_ref[0, at : at + 1, cols_of(half)], (16, lanes)).astype(BF16)
            reach = jnp.broadcast_to(f_ref[2, at : at + 1, cols_of(half)], (16, lanes)).astype(BF16)
            for part in range(HI // 16):
                rows = slice(HI * b + 16 * part, HI * b + 16 * part + 16)
                hit = hi == digit + BF16(16 * part)
                a_ref[g, rows, cols_of(half)] = jnp.where(hit, reach, BF16(0))

    def low_factor(half, g):
        for b in range(GROUP):
            at = GROUP * g + b
            lo = jnp.broadcast_to(f_ref[1, at : at + 1, cols_of(half)], (16, lanes)).astype(BF16)
            for part in range(SLOT // 16):
                at = 128 * (b % 2) + (128 - SLOT // 2 * b + 16 * part) % 128
                b_ref[g, at : at + 16, cols_of(half)] = lax.clamp(
                    BF16(-1), digit + BF16(16 * part) - lo, BF16(1)
                )

    place(me, reach_ref[rows_of(me), :])
    to_cards(me, False)
    loads[3].wait()
    for d in range(CARDS):
        hot_rows(1 - me, d)
    pl.semaphore_wait(barrier, len(plane + line + cross))
    swap = to_partner(reach_ref.at[rows_of(1 - me), :], swap_ref, swap_sem)
    groups = boards // GROUP
    for g in range(groups):
        low_factor(me, g)
        high_factor(me, g)
    swap.wait()
    place(1 - me, swap_ref[...])
    to_cards(1 - me, True)

    part_of = iota((ROWS, block), 1) // boards

    def pack(d, carry):
        for ref, at in ((w_ref, 0), (g_ref, block)):
            got = o_ref[d, 0, :, at : at + block]
            for q in range(1, PARTS):
                got = jnp.where(part_of == q, o_ref[d, q, :, at : at + block], got)
            ref[d] = got
        return carry

    lax.fori_loop(0, CARDS, pack, 0)

    def pairs(i, carry):
        mine = [g_ref[DBLOCK * i + k].astype(BF16) for k in range(DBLOCK)]
        sums = [None] * DBLOCK
        for e in range(CARDS):
            ge, we = g_ref[e].astype(BF16), w_ref[e].astype(BF16)
            for k in range(DBLOCK):
                sign = lax.clamp(BF16(-1), mine[k] - ge, BF16(1))
                term = sign.astype(F32) * we.astype(F32)
                sums[k] = term if sums[k] is None else sums[k] + term
        for k in range(DBLOCK):
            q_ref[DBLOCK * i + k] = sums[k]
        return carry

    lax.fori_loop(0, CARDS // DBLOCK, pairs, 0)
    card = iota((64, lanes), 0).astype(F32)
    card_totals = jnp.zeros((boards, 64), F32)
    for half in (1 - me, me):
        hold = ((card == c_ref[0:1, cols_of(half)]) | (card == c_ref[1:2, cols_of(half)])).astype(F32).astype(BF16)
        card_totals = card_totals + lax.dot_general(
            x_ref[0:boards, cols_of(half)], hold, NT, preferred_element_type=F32
        )
    wide = jnp.concatenate([card_totals, jnp.zeros((boards, 64), F32)], axis=1)
    pair_lanes = PARTS * CARDS * ROWS
    turned = jnp.transpose(q_ref[...].reshape(CARDS * ROWS, block))
    for k, piece in enumerate(split2(turned)):
        for q in range(PARTS):
            l_ref[0, boards * k : boards * (k + 1), CARDS * ROWS * q : CARDS * ROWS * (q + 1)] = piece[
                boards * q : boards * (q + 1)
            ]
    for k, piece in enumerate(split2(wide)):
        l_ref[0, boards * k : boards * (k + 1), pair_lanes:] = piece
    pair_copy = to_partner(l_ref.at[0], l_ref.at[1], pair_sem)

    even = iota((GROUP, 128), 0) % 2 == 0
    slot = ((iota((GROUP, 128), 1) + SLOT // 2 * iota((GROUP, 128), 0)) % 128) // SLOT
    tiles = HI // 4
    h_refs = (h0_ref, h1_ref, h2_ref, h3_ref)
    t_refs = (t0_ref, t1_ref, t2_ref, t3_ref)

    def tabulate(g):
        got = lax.dot_general(a_ref[g], b_ref[g], NT, preferred_element_type=F32)
        h_refs[g][0 : GROUP * HI, :] = got[:, 0:128]
        h_refs[g][GROUP * HI :, :] = got[:, 128:256]

    def lay_out(g):
        for t in range(tiles):
            row = None
            for k in range(4):
                at = 4 * t + k
                part = jnp.where(
                    even,
                    h_refs[g][pl.ds(at, GROUP, stride=HI), :],
                    h_refs[g][pl.ds(at + GROUP * HI, GROUP, stride=HI), :],
                )
                part = pltpu.roll(part, SLOT * k, 1) if k else part
                row = part if row is None else jnp.where(slot == k, part, row)
            t_refs[g][t] = pltpu.roll(row, 0, 1, stride=SLOT // 2, stride_axis=0)

    src, dst = iota((256, 128), 0), iota((256, 128), 1)
    within = (dst // SLOT > (src - 128) // SLOT).astype(F32) - (dst // SLOT < (src - 128) // SLOT).astype(F32)
    spread = jnp.where(src % SLOT == LO, jnp.where(src < 128, 1.0, within), 0.0).astype(BF16)
    spot = iota((GROUP, 128), 1) % SLOT == LO

    def add_rows(g):
        run = jnp.zeros((GROUP, 128), F32)
        below, whole = [], []
        for t in range(tiles):
            mark = jnp.where(spot, t_refs[g][t], 0.0)
            whole.append(mark)
            below.append(run)
            run = run + mark
        both = jnp.concatenate(
            [jnp.concatenate([below[t] - (run - below[t] - whole[t]), whole[t]], axis=1) for t in range(tiles)],
            axis=0,
        )
        got = jnp.dot(jnp.concatenate(split2(both), axis=0), spread, preferred_element_type=F32)
        got = got[: GROUP * tiles] + got[GROUP * tiles :]
        for t in range(tiles):
            t_refs[g][t] = t_refs[g][t] + got[GROUP * t : GROUP * (t + 1)]

    def look_up(g):
        rows = slice(GROUP * g, GROUP * (g + 1))
        for half in (1 - me, me):
            for k in range(lanes // 128):
                hi = f_ref[0, rows, cols_of(half, 128 * k, 128)].astype(jnp.int32)
                lo = f_ref[1, rows, cols_of(half, 128 * k, 128)].astype(jnp.int32)
                tile = hi >> 2
                at = ((hi & 3) << 5) + lo
                found = jnp.zeros((GROUP, 128), F32)
                for t in range(tiles):
                    got = jnp.take_along_axis(t_refs[g][t], at, axis=1, mode="promise_in_bounds")
                    found = jnp.where(tile == t, got, found)
                s_ref[half, rows, 128 * k : 128 * k + 128] = found

    stages = (tabulate, lay_out, add_rows, look_up)
    for step in range(groups + len(stages) - 1):
        for k, stage in enumerate(stages):
            if 0 <= step - k < groups:
                stage(step - k)
    sum_copy = to_partner(s_ref.at[1 - me], s_ref.at[2], sum_sem)

    pair_copy.wait()
    back = [p_ref[:, q, :, cols_of(me)].reshape(CARDS * ROWS, lanes) for q in range(PARTS)]
    shared = jnp.dot(
        l_ref[:, :, 0:pair_lanes].reshape(4 * boards, pair_lanes),
        jnp.concatenate(back, axis=0),
        preferred_element_type=F32,
    )
    held = jnp.dot(
        l_ref[:, :, pair_lanes:].reshape(4 * boards, 128)[:, 0:64], hold, preferred_element_type=F32
    )
    sum_copy.wait()
    for load in loads[4:]:
        load.wait()
    part = mass = None
    for k, core in ((0, me), (1, 1 - me)):
        at = 2 * boards * k
        live = (
            0.5 * jnp.sum(l_ref[k, :, pair_lanes:].astype(F32).reshape(2, boards, 128).sum(0), axis=1, keepdims=True)
            - (held[at : at + boards] + held[at + boards : at + 2 * boards])
        )[:, 0:own_count] + reach_ref[rows_of(core), :].astype(F32)
        sums = s_ref[me] if k == 0 else s_ref[2]
        margin = (sums - (shared[at : at + boards] + shared[at + boards : at + 2 * boards]))[:, 0:own_count]
        pot = column(pot_ref[...], core * boards, boards)
        bet = column(bet_ref[...], core * boards, boards)
        half_pot = 0.5 * pot
        half_pot, bet = half_pot / hand_count, bet / hand_count
        stake = half_pot * live
        values = jnp.maximum((half_pot + bet * pot) * margin, -stake)
        values_ref[rows_of(core), :] = values
        values, stake = (jnp.sum(v, axis=0, keepdims=True) for v in (values, stake))
        part = values if part is None else part + values
        mass = stake if mass is None else mass + stake
    part, mass = part / total_boards, mass / total_boards
    trav = trav_ref[...].reshape(1, own_count)
    numerator = jnp.sum(part * trav, axis=1, keepdims=True)
    denominator = jnp.sum(mass * trav, axis=1, keepdims=True)

    spot = XS * y + x
    mine_ref[0] = jnp.zeros((8, 128), F32)
    for k in range(lanes // 128):
        size = min(128, own_count - 128 * k)
        mine_ref[0, k : k + 1, 0:size] = part[:, 128 * k : 128 * k + size]
    mine_ref[0, 6:7, :] = jnp.where(iota((1, 128), 1) == 0, numerator, denominator)

    def exchange(source, groups):
        sent = []
        for peers, here, slots, sems in groups:
            for k, peer in enumerate(peers):
                copy = pltpu.make_async_remote_copy(
                    source, slots.at[here], sems.at[0, k], sems.at[1, here], device_id=peer, device_id_type=MESH
                )
                copy.start()
                sent.append(copy)
        return sent

    def arrived(source, where, slots, sems):
        pltpu.make_async_remote_copy(
            source, slots.at[where], sems.at[0, 0], sems.at[1, where], device_id=plane[0], device_id_type=MESH
        ).wait_recv()

    sent = exchange(mine_ref.at[0], [(plane, spot, plane_ref, plane_sem)])
    plane_ref[spot] = mine_ref[0]
    for peer in plane:
        arrived(mine_ref.at[0], XS * peer["board_0"] + peer["board_1"], plane_ref, plane_sem)
    mine_ref[1] = functools.reduce(jnp.add, [plane_ref[k] for k in range(YS * XS)])
    sent += exchange(mine_ref.at[1], [(line, z, line_ref, line_sem), (cross, z, cross_ref, cross_sem)])
    line_ref[z] = mine_ref[1]
    for peer in line:
        arrived(mine_ref.at[1], peer["board_2"], line_ref, line_sem)
    for peer in cross:
        arrived(mine_ref.at[1], peer["board_2"], cross_ref, cross_sem)
    total = functools.reduce(jnp.add, [line_ref[k] for k in range(ZS)])
    rest = functools.reduce(jnp.add, [cross_ref[k] for k in range(ZS)])
    hand_ref[...] = total
    ends = total[6:7] + rest[6:7]
    ratio_ref[...] = ends[:, 0:1] / ends[:, 1:2]
    for copy in sent:
        copy.wait_send()


def write_kernel(*refs):
    count = (len(refs) - 1) // 2
    copies = [pltpu.make_async_copy(refs[k], refs[count + k], refs[-1].at[k]) for k in range(count)]
    for copy in copies:
        copy.start()
    for copy in copies:
        copy.wait()


def write_out(*arrays):
    return pl.pallas_call(
        write_kernel,
        out_shape=tuple(jax.ShapeDtypeStruct(a.shape, a.dtype) for a in arrays),
        in_specs=[pl.BlockSpec(memory_space=pltpu.VMEM)] * len(arrays),
        out_specs=(pl.BlockSpec(memory_space=pl.ANY),) * len(arrays),
        scratch_shapes=[pltpu.SemaphoreType.DMA((len(arrays),))],
        cost_estimate=pl.CostEstimate(flops=10**6, bytes_accessed=10**6, transcendentals=0),
    )(*(pltpu.with_memory_space_constraint(a, pltpu.VMEM) for a in arrays))


def local(opp_reach, hand_rank, hand_cards, pot, bet_frac, trav_reach):
    boards, hand_count = hand_rank.shape
    own_count = opp_reach.shape[1]
    lanes = -(-own_count // 128) * 128
    width = 2 * lanes
    half = boards // 2
    total_boards = boards * lax.axis_size(BOARD)
    whole = pl.BlockSpec(memory_space=pltpu.VMEM)
    board_values, hand_rows, ratio = pl.pallas_call(
        functools.partial(fused_kernel, total_boards, hand_count),
        out_shape=(
            pltpu.VMEM((boards, own_count), F32),
            pltpu.VMEM((8, 128), F32),
            pltpu.VMEM((1, 1), F32),
        ),
        in_specs=[pl.BlockSpec(memory_space=pl.ANY)] * 6,
        out_specs=(whole, whole, whole),
        scratch_shapes=[
            pltpu.VMEM((boards, own_count), BF16),
            pltpu.VMEM((half, hand_count), jnp.int32),
            pltpu.VMEM((2, hand_count), jnp.int32),
            pltpu.VMEM((1, boards), F32),
            pltpu.VMEM((1, boards), F32),
            pltpu.VMEM((own_count,), F32),
            pltpu.SemaphoreType.DMA((6,)),
            pltpu.VMEM((8 * half, width), BF16),
            pltpu.VMEM((CARDS, PARTS, ROWS, width), BF16),
            pltpu.VMEM((CARDS, PARTS, ROWS, 8 * half), F32),
            pltpu.VMEM((CARDS, ROWS, 4 * half), F32),
            pltpu.VMEM((CARDS, ROWS, 4 * half), F32),
            pltpu.VMEM((CARDS, ROWS, 4 * half), F32),
            pltpu.VMEM((2, 2 * half, PARTS * CARDS * ROWS + 128), BF16),
            pltpu.VMEM((3, half, width), F32),
            pltpu.VMEM((half // GROUP, GROUP * HI, width), BF16),
            pltpu.VMEM((half // GROUP, GROUP * SLOT, width), BF16),
            *[pltpu.VMEM((2 * GROUP * HI, 128), F32)] * 4,
            *[pltpu.VMEM((HI // 4, GROUP, 128), F32)] * 4,
            pltpu.VMEM((3, half, lanes), F32),
            pltpu.VMEM((2, width), F32),
            pltpu.VMEM((half, own_count), BF16),
            pltpu.VMEM((2, 8, 128), F32),
            pltpu.VMEM((YS * XS, 8, 128), F32),
            pltpu.VMEM((ZS, 8, 128), F32),
            pltpu.VMEM((ZS, 8, 128), F32),
            pltpu.SemaphoreType.DMA((2,)),
            pltpu.SemaphoreType.DMA((2,)),
            pltpu.SemaphoreType.DMA((2,)),
            pltpu.SemaphoreType.DMA((2, YS * XS)),
            pltpu.SemaphoreType.DMA((2, ZS)),
            pltpu.SemaphoreType.DMA((2, ZS)),
        ],
        compiler_params=pltpu.CompilerParams(
            vmem_limit_bytes=56 * 1024 * 1024, collective_id=0, has_side_effects=True
        ),
        cost_estimate=pl.CostEstimate(flops=10**9, bytes_accessed=10**6, transcendentals=0),
    )(opp_reach, hand_rank, hand_cards.T, pot[None, :], bet_frac[None, :], trav_reach)
    board_values, hand_rows, ratio = write_out(board_values, hand_rows, ratio)
    return board_values, hand_rows.reshape(-1)[:own_count], ratio[0, 0]


def solution(mesh):
    torus = Mesh(
        mesh.devices.reshape(YS, XS, ZS, mesh.shape["hand"]), ("board_0", "board_1", "board_2", "hand")
    )
    placed = (P(BOARD, "hand"), P(BOARD, None), P(), P(BOARD), P(BOARD), P("hand"))
    return jax.shard_map(
        local,
        mesh=torus,
        in_specs=placed,
        out_specs=(P(BOARD, "hand"), P("hand"), P()),
        check_vma=False,
    )
```

```python
import functools

import jax
import jax.numpy as jnp
from jax import lax
from jax.experimental import pallas as pl
from jax.experimental.pallas import tpu as pltpu
from jax.sharding import Mesh
from jax.sharding import PartitionSpec as P

CARDS = 52
BOARD = ("board_0", "board_1", "board_2")
BF16 = jnp.bfloat16
F32 = jnp.float32

PARTS = 4
SHARE = CARDS // PARTS
ROWS = 16
HI, LO = 48, 28
SLOT = 32
GROUP = 8
DBLOCK = 4
YS, XS, ZS = 4, 4, 8
MESH = pl.DeviceIdType.MESH
NT = (((1,), (1,)), ((), ()))


def iota(shape, axis):
    return lax.broadcasted_iota(jnp.int32, shape, axis)


def split2(x):
    high = x.astype(BF16)
    return high, (x - high.astype(F32)).astype(BF16)


def rank_code(rank):
    return (((rank & 127) | 128) << (rank >> 7)).astype(F32).astype(BF16)


def every_peer(places):
    y, x, z, h = places
    plane = [
        {"board_0": lax.rem(y + i, YS), "board_1": lax.rem(x + j, XS)}
        for i in (2, 1, 3, 0)
        for j in (2, 1, 3, 0)
        if i or j
    ]
    line = [{"board_2": lax.rem(z + i, ZS)} for i in (4, 3, 5, 2, 6, 1, 7)]
    cross = [{"board_2": lax.rem(z + i, ZS), "hand": 1 - h} for i in (4, 3, 5, 2, 6, 1, 7, 0)]
    return plane, line, cross


def column(row, start, size):
    n = row.shape[1]
    hit = iota((size, n), 1) == iota((size, n), 0) + start
    return jnp.sum(jnp.where(hit, row, 0.0), axis=1, keepdims=True)


def fused_kernel(
    total_boards, hand_count,
    reach_hbm, rank_hbm, cards_hbm, pot_hbm, bet_hbm, trav_hbm,
    values_ref, hand_ref, ratio_ref,
    reach_ref, rank_ref, cards_ref, pot_ref, bet_ref, trav_ref, io_sem,
    x_ref, p_ref, o_ref, w_ref, g_ref, q_ref, l_ref, f_ref, a_ref, b_ref, h0_ref, h1_ref, h2_ref, h3_ref, t0_ref, t1_ref, t2_ref, t3_ref, s_ref, c_ref,
    swap_ref, mine_ref, plane_ref, line_ref, cross_ref,
    swap_sem, pair_sem, sum_sem, plane_sem, line_sem, cross_sem,
):
    all_boards, own_count = reach_ref.shape
    boards = all_boards // 2
    block = 4 * boards
    lanes = x_ref.shape[1] // 2
    width = 2 * lanes
    places = tuple(lax.axis_index(name) for name in BOARD) + (lax.axis_index("hand"),)
    y, x, z, me = places
    plane, line, cross = every_peer(places)
    barrier = pltpu.get_barrier_semaphore()

    def cols_of(half, start=0, size=lanes):
        return pl.ds(pl.multiple_of(half * lanes + start, 128), size)

    def rows_of(core):
        return pl.ds(pl.multiple_of(core * boards, boards), boards)

    def to_partner(source, target, sems):
        copy = pltpu.make_async_remote_copy(
            source, target, sems.at[0], sems.at[1], device_id={"hand": 1 - me}, device_id_type=MESH
        )
        copy.start()
        return copy

    loads = [
        pltpu.make_async_copy(source, target, io_sem.at[k])
        for k, (source, target) in enumerate(
            (
                (cards_hbm, cards_ref),
                (rank_hbm.at[rows_of(me), :], rank_ref),
                (reach_hbm, reach_ref),
                (pot_hbm, pot_ref),
                (bet_hbm, bet_ref),
                (trav_hbm, trav_ref),
            )
        )
    ]
    for load in loads:
        load.start()
    for peer in plane + line + cross:
        pl.semaphore_signal(barrier, inc=1, device_id=peer, device_id_type=MESH)

    loads[0].wait()
    for half in range(2):
        start = half * lanes
        c_ref[:, start + lanes - 128 : start + lanes] = jnp.full((2, 128), -1.0, F32)
        c_ref[:, start : start + own_count] = cards_ref[:, half * own_count : (half + 1) * own_count].astype(F32)

    row16 = iota((16, lanes), 0)
    own_row = [
        jnp.where(row16 < SHARE, row16 + SHARE * q, -5).astype(F32).astype(BF16) for q in range(PARTS)
    ]

    def hot_rows(half, d):
        low, high = c_ref[0:1, cols_of(half)], c_ref[1:2, cols_of(half)]
        partner = jnp.where(low == float(d), high, jnp.where(high == float(d), low, -1.0))
        wide = jnp.broadcast_to(partner, (16, lanes)).astype(BF16)
        for q in range(PARTS):
            p_ref[d, q, :, cols_of(half)] = jnp.where(wide == own_row[q], BF16(1), BF16(0))

    loads[1].wait()
    loads[2].wait()
    for half in range(2):
        start = half * lanes
        f_ref[0:2, :, start + lanes - 128 : start + lanes] = jnp.zeros((2, boards, 128), F32)
        x_ref[:, start + lanes - 128 : start + lanes] = jnp.zeros((8 * boards, 128), BF16)
        rank = rank_ref[:, half * own_count : (half + 1) * own_count]
        x_ref[block : block + boards, start : start + own_count] = rank_code(rank)
        hi = (rank * 2341) >> 16
        f_ref[0, :, start : start + own_count] = hi.astype(F32)
        f_ref[1, :, start : start + own_count] = (rank - LO * hi).astype(F32)
    for k in range(1, PARTS):
        x_ref[block + k * boards : block + (k + 1) * boards, :] = x_ref[block : block + boards, :]

    def place(half, reach):
        x_ref[0:boards, pl.ds(pl.multiple_of(half * lanes, 128), own_count)] = reach
        f_ref[2, :, cols_of(half)] = x_ref[0:boards, cols_of(half)].astype(F32)
        for k in range(1, PARTS):
            x_ref[k * boards : (k + 1) * boards, cols_of(half)] = x_ref[0:boards, cols_of(half)]

    chunk = CARDS // PARTS

    def to_cards(half, more):
        for i in range(PARTS):
            these = slice(chunk * i, chunk * (i + 1))
            if not more:
                for d in range(chunk * i, chunk * (i + 1)):
                    hot_rows(half, d)
            if more:
                high_factor(half, i)
            rows = p_ref[these, :, :, cols_of(half)].reshape(chunk * PARTS * ROWS, lanes)
            got = lax.dot_general(rows, x_ref[:, cols_of(half)], NT, preferred_element_type=F32)
            got = got.reshape(chunk, PARTS, ROWS, 2 * block)
            o_ref[these] = got + o_ref[these] if more else got

    digit = iota((16, lanes), 0).astype(F32).astype(BF16)

    def high_factor(half, g):
        for b in range(GROUP):
            at = GROUP * g + b
            hi = jnp.broadcast_to(f_ref[0, at : at + 1, cols_of(half)], (16, lanes)).astype(BF16)
            reach = jnp.broadcast_to(f_ref[2, at : at + 1, cols_of(half)], (16, lanes)).astype(BF16)
            for part in range(HI // 16):
                rows = slice(HI * b + 16 * part, HI * b + 16 * part + 16)
                hit = hi == digit + BF16(16 * part)
                a_ref[g, rows, cols_of(half)] = jnp.where(hit, reach, BF16(0))

    def low_factor(half, g):
        for b in range(GROUP):
            at = GROUP * g + b
            lo = jnp.broadcast_to(f_ref[1, at : at + 1, cols_of(half)], (16, lanes)).astype(BF16)
            for part in range(SLOT // 16):
                at = SLOT * b + 16 * part
                b_ref[g, at : at + 16, cols_of(half)] = lax.clamp(
                    BF16(-1), digit + BF16(16 * part) - lo, BF16(1)
                )

    place(me, reach_ref[rows_of(me), :])
    to_cards(me, False)
    loads[3].wait()
    for d in range(CARDS):
        hot_rows(1 - me, d)
    pl.semaphore_wait(barrier, len(plane + line + cross))
    swap = to_partner(reach_ref.at[rows_of(1 - me), :], swap_ref, swap_sem)
    groups = boards // GROUP
    for g in range(groups):
        low_factor(me, g)
        high_factor(me, g)
        low_factor(1 - me, g)
    swap.wait()
    place(1 - me, swap_ref[...])
    to_cards(1 - me, True)

    part_of = iota((ROWS, block), 1) // boards

    def pack(d, carry):
        for ref, at in ((w_ref, 0), (g_ref, block)):
            got = o_ref[d, 0, :, at : at + block]
            for q in range(1, PARTS):
                got = jnp.where(part_of == q, o_ref[d, q, :, at : at + block], got)
            ref[d] = got
        return carry

    lax.fori_loop(0, CARDS, pack, 0, unroll=4)

    def pairs(i, carry):
        mine = [g_ref[DBLOCK * i + k].astype(BF16) for k in range(DBLOCK)]
        sums = [None] * DBLOCK
        for e in range(CARDS):
            ge, we = g_ref[e].astype(BF16), w_ref[e].astype(BF16)
            for k in range(DBLOCK):
                sign = lax.clamp(BF16(-1), mine[k] - ge, BF16(1))
                term = sign.astype(F32) * we.astype(F32)
                sums[k] = term if sums[k] is None else sums[k] + term
        for k in range(DBLOCK):
            q_ref[DBLOCK * i + k] = sums[k]
        return carry

    lax.fori_loop(0, CARDS // DBLOCK, pairs, 0)
    card = iota((64, lanes), 0).astype(F32)
    card_totals = jnp.zeros((boards, 64), F32)
    for half in (1 - me, me):
        hold = ((card == c_ref[0:1, cols_of(half)]) | (card == c_ref[1:2, cols_of(half)])).astype(F32).astype(BF16)
        card_totals = card_totals + lax.dot_general(
            x_ref[0:boards, cols_of(half)], hold, NT, preferred_element_type=F32
        )
    wide = jnp.concatenate([card_totals, jnp.zeros((boards, 64), F32)], axis=1)
    pair_lanes = PARTS * CARDS * ROWS
    turned = jnp.transpose(q_ref[...].reshape(CARDS * ROWS, block))
    for k, piece in enumerate(split2(turned)):
        for q in range(PARTS):
            l_ref[0, boards * k : boards * (k + 1), CARDS * ROWS * q : CARDS * ROWS * (q + 1)] = piece[
                boards * q : boards * (q + 1)
            ]
    for k, piece in enumerate(split2(wide)):
        l_ref[0, boards * k : boards * (k + 1), pair_lanes:] = piece
    pair_copy = to_partner(l_ref.at[0], l_ref.at[1], pair_sem)

    row_slot = iota((GROUP, 128), 0) % 4
    upper = iota((GROUP, 128), 0) < 4
    shift = (iota((GROUP, 128), 1) // SLOT - row_slot) % 4
    tiles = HI // 4
    h_refs = (h0_ref, h1_ref, h2_ref, h3_ref)
    t_refs = (t0_ref, t1_ref, t2_ref, t3_ref)

    def tabulate(g):
        got = lax.dot_general(a_ref[g], b_ref[g], NT, preferred_element_type=F32)
        h_refs[g][0 : GROUP * HI, :] = got[:, 0:128]
        h_refs[g][GROUP * HI :, :] = got[:, 128:256]

    def lay_out(g):
        for t in range(tiles):
            parts = [
                jnp.where(
                    upper,
                    h_refs[g][pl.ds(4 * t + k, GROUP, stride=HI), :],
                    h_refs[g][pl.ds(4 * t + k + GROUP * HI, GROUP, stride=HI), :],
                )
                for k in range(4)
            ]
            row = None
            for k in range(4):
                moved = parts[(3 + k) % 4]
                for p in range(3):
                    moved = jnp.where(row_slot == p, parts[(p + k) % 4], moved)
                row = moved if row is None else jnp.where(shift == k, pltpu.roll(moved, SLOT * k, 1), row)
            t_refs[g][t] = row

    src, dst = iota((256, 128), 0), iota((256, 128), 1)
    within = (dst // SLOT > (src - 128) // SLOT).astype(F32) - (dst // SLOT < (src - 128) // SLOT).astype(F32)
    spread = jnp.where(src % SLOT == LO, jnp.where(src < 128, 1.0, within), 0.0).astype(BF16)
    spot = iota((GROUP, 128), 1) % SLOT == LO

    def add_rows(g):
        run = jnp.zeros((GROUP, 128), F32)
        below, whole = [], []
        for t in range(tiles):
            mark = jnp.where(spot, t_refs[g][t], 0.0)
            whole.append(mark)
            below.append(run)
            run = run + mark
        both = jnp.concatenate(
            [jnp.concatenate([below[t] - (run - below[t] - whole[t]), whole[t]], axis=1) for t in range(tiles)],
            axis=0,
        )
        got = jnp.dot(jnp.concatenate(split2(both), axis=0), spread, preferred_element_type=F32)
        got = got[: GROUP * tiles] + got[GROUP * tiles :]
        for t in range(tiles):
            t_refs[g][t] = t_refs[g][t] + got[GROUP * t : GROUP * (t + 1)]

    def look_up(g, half=1 - me):
        rows = slice(GROUP * g, GROUP * (g + 1))
        for k in range(lanes // 128):
            hi = f_ref[0, rows, cols_of(half, 128 * k, 128)].astype(jnp.int32)
            lo = f_ref[1, rows, cols_of(half, 128 * k, 128)].astype(jnp.int32)
            tile = hi >> 2
            at = ((hi & 3) << 5) + lo
            found = jnp.zeros((GROUP, 128), F32)
            for t in range(tiles):
                got = jnp.take_along_axis(t_refs[g][t], at, axis=1, mode="promise_in_bounds")
                found = jnp.where(tile == t, got, found)
            s_ref[half, rows, 128 * k : 128 * k + 128] = found

    stages = (tabulate, lay_out, add_rows, look_up)
    for step in range(groups + len(stages) - 1):
        for k, stage in enumerate(stages):
            if 0 <= step - k < groups:
                stage(step - k)
    sum_copy = to_partner(s_ref.at[1 - me], s_ref.at[2], sum_sem)

    pair_copy.wait()
    for g in range(groups):
        look_up(g, me)
    back = [p_ref[:, q, :, cols_of(me)].reshape(CARDS * ROWS, lanes) for q in range(PARTS)]
    shared = jnp.dot(
        l_ref[:, :, 0:pair_lanes].reshape(4 * boards, pair_lanes),
        jnp.concatenate(back, axis=0),
        preferred_element_type=F32,
    )
    held = jnp.dot(
        l_ref[:, :, pair_lanes:].reshape(4 * boards, 128)[:, 0:64], hold, preferred_element_type=F32
    )
    sum_copy.wait()
    for load in loads[4:]:
        load.wait()
    part = mass = None
    for k, core in ((0, me), (1, 1 - me)):
        at = 2 * boards * k
        live = (
            0.5 * jnp.sum(l_ref[k, :, pair_lanes:].astype(F32).reshape(2, boards, 128).sum(0), axis=1, keepdims=True)
            - (held[at : at + boards] + held[at + boards : at + 2 * boards])
        )[:, 0:own_count] + reach_ref[rows_of(core), :].astype(F32)
        sums = s_ref[me] if k == 0 else s_ref[2]
        margin = (sums - (shared[at : at + boards] + shared[at + boards : at + 2 * boards]))[:, 0:own_count]
        pot = column(pot_ref[...], core * boards, boards)
        bet = column(bet_ref[...], core * boards, boards)
        half_pot = 0.5 * pot
        half_pot, bet = half_pot / hand_count, bet / hand_count
        stake = half_pot * live
        values = jnp.maximum((half_pot + bet * pot) * margin, -stake)
        values_ref[rows_of(core), :] = values
        values, stake = (jnp.sum(v, axis=0, keepdims=True) for v in (values, stake))
        part = values if part is None else part + values
        mass = stake if mass is None else mass + stake
    part, mass = part / total_boards, mass / total_boards
    trav = trav_ref[...].reshape(1, own_count)
    numerator = jnp.sum(part * trav, axis=1, keepdims=True)
    denominator = jnp.sum(mass * trav, axis=1, keepdims=True)

    spot = XS * y + x
    mine_ref[0] = jnp.zeros((8, 128), F32)
    for k in range(lanes // 128):
        size = min(128, own_count - 128 * k)
        mine_ref[0, k : k + 1, 0:size] = part[:, 128 * k : 128 * k + size]
    mine_ref[0, 6:7, :] = jnp.where(iota((1, 128), 1) == 0, numerator, denominator)

    def exchange(source, groups):
        sent = []
        for peers, here, slots, sems in groups:
            for k, peer in enumerate(peers):
                copy = pltpu.make_async_remote_copy(
                    source, slots.at[here], sems.at[0, k], sems.at[1, here], device_id=peer, device_id_type=MESH
                )
                copy.start()
                sent.append(copy)
        return sent

    def arrived(source, where, slots, sems):
        pltpu.make_async_remote_copy(
            source, slots.at[where], sems.at[0, 0], sems.at[1, where], device_id=plane[0], device_id_type=MESH
        ).wait_recv()

    sent = exchange(mine_ref.at[0], [(plane, spot, plane_ref, plane_sem)])
    plane_ref[spot] = mine_ref[0]
    for peer in plane:
        arrived(mine_ref.at[0], XS * peer["board_0"] + peer["board_1"], plane_ref, plane_sem)
    mine_ref[1] = functools.reduce(jnp.add, [plane_ref[k] for k in range(YS * XS)])
    sent += exchange(mine_ref.at[1], [(line, z, line_ref, line_sem), (cross, z, cross_ref, cross_sem)])
    line_ref[z] = mine_ref[1]
    for peer in line:
        arrived(mine_ref.at[1], peer["board_2"], line_ref, line_sem)
    for peer in cross:
        arrived(mine_ref.at[1], peer["board_2"], cross_ref, cross_sem)
    total = functools.reduce(jnp.add, [line_ref[k] for k in range(ZS)])
    rest = functools.reduce(jnp.add, [cross_ref[k] for k in range(ZS)])
    hand_ref[...] = total
    ends = total[6:7] + rest[6:7]
    ratio_ref[...] = ends[:, 0:1] / ends[:, 1:2]
    for copy in sent:
        copy.wait_send()


def write_kernel(*refs):
    count = (len(refs) - 1) // 2
    copies = [pltpu.make_async_copy(refs[k], refs[count + k], refs[-1].at[k]) for k in range(count)]
    for copy in copies:
        copy.start()
    for copy in copies:
        copy.wait()


def write_out(*arrays):
    return pl.pallas_call(
        write_kernel,
        out_shape=tuple(jax.ShapeDtypeStruct(a.shape, a.dtype) for a in arrays),
        in_specs=[pl.BlockSpec(memory_space=pltpu.VMEM)] * len(arrays),
        out_specs=(pl.BlockSpec(memory_space=pl.ANY),) * len(arrays),
        scratch_shapes=[pltpu.SemaphoreType.DMA((len(arrays),))],
        cost_estimate=pl.CostEstimate(flops=10**6, bytes_accessed=10**6, transcendentals=0),
    )(*(pltpu.with_memory_space_constraint(a, pltpu.VMEM) for a in arrays))


def local(opp_reach, hand_rank, hand_cards, pot, bet_frac, trav_reach):
    boards, hand_count = hand_rank.shape
    own_count = opp_reach.shape[1]
    lanes = -(-own_count // 128) * 128
    width = 2 * lanes
    half = boards // 2
    total_boards = boards * lax.axis_size(BOARD)
    whole = pl.BlockSpec(memory_space=pltpu.VMEM)
    board_values, hand_rows, ratio = pl.pallas_call(
        functools.partial(fused_kernel, total_boards, hand_count),
        out_shape=(
            pltpu.VMEM((boards, own_count), F32),
            pltpu.VMEM((8, 128), F32),
            pltpu.VMEM((1, 1), F32),
        ),
        in_specs=[pl.BlockSpec(memory_space=pl.ANY)] * 6,
        out_specs=(whole, whole, whole),
        scratch_shapes=[
            pltpu.VMEM((boards, own_count), BF16),
            pltpu.VMEM((half, hand_count), jnp.int32),
            pltpu.VMEM((2, hand_count), jnp.int32),
            pltpu.VMEM((1, boards), F32),
            pltpu.VMEM((1, boards), F32),
            pltpu.VMEM((own_count,), F32),
            pltpu.SemaphoreType.DMA((6,)),
            pltpu.VMEM((8 * half, width), BF16),
            pltpu.VMEM((CARDS, PARTS, ROWS, width), BF16),
            pltpu.VMEM((CARDS, PARTS, ROWS, 8 * half), F32),
            pltpu.VMEM((CARDS, ROWS, 4 * half), F32),
            pltpu.VMEM((CARDS, ROWS, 4 * half), F32),
            pltpu.VMEM((CARDS, ROWS, 4 * half), F32),
            pltpu.VMEM((2, 2 * half, PARTS * CARDS * ROWS + 128), BF16),
            pltpu.VMEM((3, half, width), F32),
            pltpu.VMEM((half // GROUP, GROUP * HI, width), BF16),
            pltpu.VMEM((half // GROUP, GROUP * SLOT, width), BF16),
            *[pltpu.VMEM((2 * GROUP * HI, 128), F32)] * 4,
            *[pltpu.VMEM((HI // 4, GROUP, 128), F32)] * 4,
            pltpu.VMEM((3, half, lanes), F32),
            pltpu.VMEM((2, width), F32),
            pltpu.VMEM((half, own_count), BF16),
            pltpu.VMEM((2, 8, 128), F32),
            pltpu.VMEM((YS * XS, 8, 128), F32),
            pltpu.VMEM((ZS, 8, 128), F32),
            pltpu.VMEM((ZS, 8, 128), F32),
            pltpu.SemaphoreType.DMA((2,)),
            pltpu.SemaphoreType.DMA((2,)),
            pltpu.SemaphoreType.DMA((2,)),
            pltpu.SemaphoreType.DMA((2, YS * XS)),
            pltpu.SemaphoreType.DMA((2, ZS)),
            pltpu.SemaphoreType.DMA((2, ZS)),
        ],
        compiler_params=pltpu.CompilerParams(
            vmem_limit_bytes=56 * 1024 * 1024, collective_id=0, has_side_effects=True
        ),
        cost_estimate=pl.CostEstimate(flops=10**9, bytes_accessed=10**6, transcendentals=0),
    )(opp_reach, hand_rank, hand_cards.T, pot[None, :], bet_frac[None, :], trav_reach)
    board_values, hand_rows, ratio = write_out(board_values, hand_rows, ratio)
    return board_values, hand_rows.reshape(-1)[:own_count], ratio[0, 0]


def solution(mesh):
    torus = Mesh(
        mesh.devices.reshape(YS, XS, ZS, mesh.shape["hand"]), ("board_0", "board_1", "board_2", "hand")
    )
    placed = (P(BOARD, "hand"), P(BOARD, None), P(), P(BOARD), P(BOARD), P("hand"))
    return jax.shard_map(
        local,
        mesh=torus,
        in_specs=placed,
        out_specs=(P(BOARD, "hand"), P("hand"), P()),
        check_vma=False,
    )
```

```python
import functools

import jax
import jax.numpy as jnp
from jax import lax
from jax.experimental import pallas as pl
from jax.experimental.pallas import tpu as pltpu
from jax.sharding import Mesh
from jax.sharding import PartitionSpec as P

CARDS = 52
BOARD = ("board_0", "board_1", "board_2")
BF16 = jnp.bfloat16
F32 = jnp.float32

PARTS = 4
SHARE = CARDS // PARTS
ROWS = 16
HI, LO = 48, 28
SLOT = 32
GROUP = 8
DBLOCK = 4
WRITES = 4
YS, XS, ZS = 4, 4, 8
MESH = pl.DeviceIdType.MESH
NT = (((1,), (1,)), ((), ()))


def iota(shape, axis):
    return lax.broadcasted_iota(jnp.int32, shape, axis)


def split2(x):
    high = x.astype(BF16)
    return high, (x - high.astype(F32)).astype(BF16)


def rank_code(rank):
    return (((rank & 127) | 128) << (rank >> 7)).astype(F32).astype(BF16)


def every_peer(places):
    y, x, z, h = places
    plane = [
        {"board_0": lax.rem(y + i, YS), "board_1": lax.rem(x + j, XS)}
        for i in (2, 1, 3, 0)
        for j in (2, 1, 3, 0)
        if i or j
    ]
    line = [{"board_2": lax.rem(z + i, ZS)} for i in (4, 3, 5, 2, 6, 1, 7)]
    cross = [{"board_2": lax.rem(z + i, ZS), "hand": 1 - h} for i in (4, 3, 5, 2, 6, 1, 7, 0)]
    return plane, line, cross


def column(row, start, size):
    n = row.shape[1]
    hit = iota((size, n), 1) == iota((size, n), 0) + start
    return jnp.sum(jnp.where(hit, row, 0.0), axis=1, keepdims=True)


def fused_kernel(
    total_boards, hand_count,
    reach_hbm, rank_hbm, cards_hbm, pot_hbm, bet_hbm, trav_hbm,
    values_ref, hand_ref, ratio_ref,
    reach_ref, rank_ref, cards_ref, pot_ref, bet_ref, trav_ref, io_sem,
    x_ref, p_ref, o_ref, w_ref, g_ref, q_ref, l_ref, f_ref, a_ref, b_ref, h0_ref, h1_ref, h2_ref, h3_ref, t0_ref, t1_ref, t2_ref, t3_ref, s_ref, c_ref,
    swap_ref, mine_ref, plane_ref, line_ref, cross_ref,
    swap_sem, pair_sem, sum_sem, plane_sem, line_sem, cross_sem,
):
    all_boards, own_count = reach_ref.shape
    boards = all_boards // 2
    block = 4 * boards
    lanes = x_ref.shape[1] // 2
    width = 2 * lanes
    places = tuple(lax.axis_index(name) for name in BOARD) + (lax.axis_index("hand"),)
    y, x, z, me = places
    plane, line, cross = every_peer(places)
    barrier = pltpu.get_barrier_semaphore()

    def cols_of(half, start=0, size=lanes):
        return pl.ds(pl.multiple_of(half * lanes + start, 128), size)

    def rows_of(core):
        return pl.ds(pl.multiple_of(core * boards, boards), boards)

    def to_partner(source, target, sems):
        copy = pltpu.make_async_remote_copy(
            source, target, sems.at[0], sems.at[1], device_id={"hand": 1 - me}, device_id_type=MESH
        )
        copy.start()
        return copy

    loads = [
        pltpu.make_async_copy(source, target, io_sem.at[k])
        for k, (source, target) in enumerate(
            (
                (cards_hbm, cards_ref),
                (rank_hbm.at[rows_of(me), :], rank_ref),
                (reach_hbm, reach_ref),
                (pot_hbm, pot_ref),
                (bet_hbm, bet_ref),
                (trav_hbm, trav_ref),
            )
        )
    ]
    for load in loads:
        load.start()
    for peer in plane + line + cross:
        pl.semaphore_signal(barrier, inc=1, device_id=peer, device_id_type=MESH)

    loads[0].wait()
    for half in range(2):
        start = half * lanes
        c_ref[:, start + lanes - 128 : start + lanes] = jnp.full((2, 128), -1.0, F32)
        c_ref[:, start : start + own_count] = cards_ref[:, half * own_count : (half + 1) * own_count].astype(F32)

    row16 = iota((16, lanes), 0)
    own_row = [
        jnp.where(row16 < SHARE, row16 + SHARE * q, -5).astype(F32).astype(BF16) for q in range(PARTS)
    ]

    def hot_rows(half, d):
        low, high = c_ref[0:1, cols_of(half)], c_ref[1:2, cols_of(half)]
        partner = jnp.where(low == float(d), high, jnp.where(high == float(d), low, -1.0))
        wide = jnp.broadcast_to(partner, (16, lanes)).astype(BF16)
        for q in range(PARTS):
            p_ref[d, q, :, cols_of(half)] = jnp.where(wide == own_row[q], BF16(1), BF16(0))

    loads[1].wait()
    loads[2].wait()
    for half in range(2):
        start = half * lanes
        f_ref[0:2, :, start + lanes - 128 : start + lanes] = jnp.zeros((2, boards, 128), F32)
        x_ref[:, start + lanes - 128 : start + lanes] = jnp.zeros((8 * boards, 128), BF16)
        rank = rank_ref[:, half * own_count : (half + 1) * own_count]
        x_ref[block : block + boards, start : start + own_count] = rank_code(rank)
        hi = (rank * 2341) >> 16
        f_ref[0, :, start : start + own_count] = hi.astype(F32)
        f_ref[1, :, start : start + own_count] = (rank - LO * hi).astype(F32)
    for k in range(1, PARTS):
        x_ref[block + k * boards : block + (k + 1) * boards, :] = x_ref[block : block + boards, :]

    def place(half, reach):
        x_ref[0:boards, pl.ds(pl.multiple_of(half * lanes, 128), own_count)] = reach
        f_ref[2, :, cols_of(half)] = x_ref[0:boards, cols_of(half)].astype(F32)
        for k in range(1, PARTS):
            x_ref[k * boards : (k + 1) * boards, cols_of(half)] = x_ref[0:boards, cols_of(half)]

    chunk = CARDS // PARTS

    def to_cards(half, more):
        for i in range(PARTS):
            these = slice(chunk * i, chunk * (i + 1))
            if not more:
                for d in range(chunk * i, chunk * (i + 1)):
                    hot_rows(half, d)
            if more:
                high_factor(half, i)
            rows = p_ref[these, :, :, cols_of(half)].reshape(chunk * PARTS * ROWS, lanes)
            got = lax.dot_general(rows, x_ref[:, cols_of(half)], NT, preferred_element_type=F32)
            got = got.reshape(chunk, PARTS, ROWS, 2 * block)
            o_ref[these] = got + o_ref[these] if more else got

    digit = iota((16, lanes), 0).astype(F32).astype(BF16)

    def high_factor(half, g):
        for b in range(GROUP):
            at = GROUP * g + b
            hi = jnp.broadcast_to(f_ref[0, at : at + 1, cols_of(half)], (16, lanes)).astype(BF16)
            reach = jnp.broadcast_to(f_ref[2, at : at + 1, cols_of(half)], (16, lanes)).astype(BF16)
            for part in range(HI // 16):
                rows = slice(HI * b + 16 * part, HI * b + 16 * part + 16)
                hit = hi == digit + BF16(16 * part)
                a_ref[g, rows, cols_of(half)] = jnp.where(hit, reach, BF16(0))

    def low_factor(half, g):
        for b in range(GROUP):
            at = GROUP * g + b
            lo = jnp.broadcast_to(f_ref[1, at : at + 1, cols_of(half)], (16, lanes)).astype(BF16)
            for part in range(SLOT // 16):
                at = SLOT * b + 16 * part
                b_ref[g, at : at + 16, cols_of(half)] = lax.clamp(
                    BF16(-1), digit + BF16(16 * part) - lo, BF16(1)
                )

    h_refs = (h0_ref, h1_ref, h2_ref, h3_ref)

    def tabulate(g, half=1 - me):
        got = lax.dot_general(
            a_ref[g, :, cols_of(half)], b_ref[g, :, cols_of(half)], NT, preferred_element_type=F32
        )
        for k in range(2):
            rows, piece = slice(GROUP * HI * k, GROUP * HI * (k + 1)), got[:, 128 * k : 128 * (k + 1)]
            h_refs[g][rows, :] = piece if half is me else piece + h_refs[g][rows, :]

    place(me, reach_ref[rows_of(me), :])
    to_cards(me, False)
    loads[3].wait()
    groups = boards // GROUP
    for d in range(CARDS):
        hot_rows(1 - me, d)
    for g in range(groups):
        low_factor(me, g)
        low_factor(1 - me, g)
    pl.semaphore_wait(barrier, len(plane + line + cross))
    swap = to_partner(reach_ref.at[rows_of(1 - me), :], swap_ref, swap_sem)
    for g in range(groups):
        high_factor(me, g)
        tabulate(g, me)
    swap.wait()
    place(1 - me, swap_ref[...])
    to_cards(1 - me, True)

    part_of = iota((ROWS, block), 1) // boards

    def pack(d, carry):
        for ref, at in ((w_ref, 0), (g_ref, block)):
            got = o_ref[d, 0, :, at : at + block]
            for q in range(1, PARTS):
                got = jnp.where(part_of == q, o_ref[d, q, :, at : at + block], got)
            ref[d] = got
        return carry

    lax.fori_loop(0, CARDS, pack, 0, unroll=4)

    def pairs(i, carry):
        mine = [g_ref[DBLOCK * i + k].astype(BF16) for k in range(DBLOCK)]
        sums = [None] * DBLOCK
        for e in range(CARDS):
            ge, we = g_ref[e].astype(BF16), w_ref[e].astype(BF16)
            for k in range(DBLOCK):
                sign = lax.clamp(BF16(-1), mine[k] - ge, BF16(1))
                term = sign.astype(F32) * we.astype(F32)
                sums[k] = term if sums[k] is None else sums[k] + term
        for k in range(DBLOCK):
            q_ref[DBLOCK * i + k] = sums[k]
        return carry

    lax.fori_loop(0, CARDS // DBLOCK, pairs, 0)
    card = iota((64, lanes), 0).astype(F32)
    card_totals = jnp.zeros((boards, 64), F32)
    for half in (1 - me, me):
        hold = ((card == c_ref[0:1, cols_of(half)]) | (card == c_ref[1:2, cols_of(half)])).astype(F32).astype(BF16)
        card_totals = card_totals + lax.dot_general(
            x_ref[0:boards, cols_of(half)], hold, NT, preferred_element_type=F32
        )
    wide = jnp.concatenate([card_totals, jnp.zeros((boards, 64), F32)], axis=1)
    pair_lanes = PARTS * CARDS * ROWS
    turned = jnp.transpose(q_ref[...].reshape(CARDS * ROWS, block))
    for k, piece in enumerate(split2(turned)):
        for q in range(PARTS):
            l_ref[0, boards * k : boards * (k + 1), CARDS * ROWS * q : CARDS * ROWS * (q + 1)] = piece[
                boards * q : boards * (q + 1)
            ]
    for k, piece in enumerate(split2(wide)):
        l_ref[0, boards * k : boards * (k + 1), pair_lanes:] = piece
    pair_copy = to_partner(l_ref.at[0], l_ref.at[1], pair_sem)

    row_slot = iota((GROUP, 128), 0) % 4
    upper = iota((GROUP, 128), 0) < 4
    shift = (iota((GROUP, 128), 1) // SLOT - row_slot) % 4
    tiles = HI // 4
    t_refs = (t0_ref, t1_ref, t2_ref, t3_ref)

    def lay_out(g):
        for t in range(tiles):
            parts = [
                jnp.where(
                    upper,
                    h_refs[g][pl.ds(4 * t + k, GROUP, stride=HI), :],
                    h_refs[g][pl.ds(4 * t + k + GROUP * HI, GROUP, stride=HI), :],
                )
                for k in range(4)
            ]
            row = None
            for k in range(4):
                moved = parts[(3 + k) % 4]
                for p in range(3):
                    moved = jnp.where(row_slot == p, parts[(p + k) % 4], moved)
                row = moved if row is None else jnp.where(shift == k, pltpu.roll(moved, SLOT * k, 1), row)
            t_refs[g][t] = row

    src, dst = iota((256, 128), 0), iota((256, 128), 1)
    within = (dst // SLOT > (src - 128) // SLOT).astype(F32) - (dst // SLOT < (src - 128) // SLOT).astype(F32)
    spread = jnp.where(src % SLOT == LO, jnp.where(src < 128, 1.0, within), 0.0).astype(BF16)
    spot = iota((GROUP, 128), 1) % SLOT == LO

    def add_rows(g):
        run = jnp.zeros((GROUP, 128), F32)
        below, whole = [], []
        for t in range(tiles):
            mark = jnp.where(spot, t_refs[g][t], 0.0)
            whole.append(mark)
            below.append(run)
            run = run + mark
        both = jnp.concatenate(
            [jnp.concatenate([below[t] - (run - below[t] - whole[t]), whole[t]], axis=1) for t in range(tiles)],
            axis=0,
        )
        got = jnp.dot(jnp.concatenate(split2(both), axis=0), spread, preferred_element_type=F32)
        got = got[: GROUP * tiles] + got[GROUP * tiles :]
        for t in range(tiles):
            t_refs[g][t] = t_refs[g][t] + got[GROUP * t : GROUP * (t + 1)]

    def look_up(g, half=1 - me):
        rows = slice(GROUP * g, GROUP * (g + 1))
        for k in range(lanes // 128):
            hi = f_ref[0, rows, cols_of(half, 128 * k, 128)].astype(jnp.int32)
            lo = f_ref[1, rows, cols_of(half, 128 * k, 128)].astype(jnp.int32)
            tile = hi >> 2
            at = ((hi & 3) << 5) + lo
            found = jnp.zeros((GROUP, 128), F32)
            for t in range(tiles):
                got = jnp.take_along_axis(t_refs[g][t], at, axis=1, mode="promise_in_bounds")
                found = jnp.where(tile == t, got, found)
            s_ref[half, rows, 128 * k : 128 * k + 128] = found

    stages = (tabulate, lay_out, add_rows, look_up)
    for step in range(groups + len(stages) - 1):
        for k, stage in enumerate(stages):
            if 0 <= step - k < groups:
                stage(step - k)
    sum_copy = to_partner(s_ref.at[1 - me], s_ref.at[2], sum_sem)

    pair_copy.wait()
    for g in range(groups):
        look_up(g, me)
    back = [p_ref[:, q, :, cols_of(me)].reshape(CARDS * ROWS, lanes) for q in range(PARTS)]
    shared = jnp.dot(
        l_ref[:, :, 0:pair_lanes].reshape(4 * boards, pair_lanes),
        jnp.concatenate(back, axis=0),
        preferred_element_type=F32,
    )
    held = jnp.dot(
        l_ref[:, :, pair_lanes:].reshape(4 * boards, 128)[:, 0:64], hold, preferred_element_type=F32
    )
    sum_copy.wait()
    for load in loads[4:]:
        load.wait()
    part = mass = None
    for k, core in ((0, me), (1, 1 - me)):
        at = 2 * boards * k
        live = (
            0.5 * jnp.sum(l_ref[k, :, pair_lanes:].astype(F32).reshape(2, boards, 128).sum(0), axis=1, keepdims=True)
            - (held[at : at + boards] + held[at + boards : at + 2 * boards])
        )[:, 0:own_count] + reach_ref[rows_of(core), :].astype(F32)
        sums = s_ref[me] if k == 0 else s_ref[2]
        margin = (sums - (shared[at : at + boards] + shared[at + boards : at + 2 * boards]))[:, 0:own_count]
        pot = column(pot_ref[...], core * boards, boards)
        bet = column(bet_ref[...], core * boards, boards)
        half_pot = 0.5 * pot
        half_pot, bet = half_pot / hand_count, bet / hand_count
        stake = half_pot * live
        values = jnp.maximum((half_pot + bet * pot) * margin, -stake)
        values_ref[rows_of(core), :] = values
        values, stake = (jnp.sum(v, axis=0, keepdims=True) for v in (values, stake))
        part = values if part is None else part + values
        mass = stake if mass is None else mass + stake
    part, mass = part / total_boards, mass / total_boards
    trav = trav_ref[...].reshape(1, own_count)
    numerator = jnp.sum(part * trav, axis=1, keepdims=True)
    denominator = jnp.sum(mass * trav, axis=1, keepdims=True)

    spot = XS * y + x
    mine_ref[0] = jnp.zeros((8, 128), F32)
    for k in range(lanes // 128):
        size = min(128, own_count - 128 * k)
        mine_ref[0, k : k + 1, 0:size] = part[:, 128 * k : 128 * k + size]
    mine_ref[0, 6:7, :] = jnp.where(iota((1, 128), 1) == 0, numerator, denominator)

    def exchange(source, groups):
        sent = []
        for peers, here, slots, sems in groups:
            for k, peer in enumerate(peers):
                copy = pltpu.make_async_remote_copy(
                    source, slots.at[here], sems.at[0, k], sems.at[1, here], device_id=peer, device_id_type=MESH
                )
                copy.start()
                sent.append(copy)
        return sent

    def arrived(source, where, slots, sems):
        pltpu.make_async_remote_copy(
            source, slots.at[where], sems.at[0, 0], sems.at[1, where], device_id=plane[0], device_id_type=MESH
        ).wait_recv()

    sent = exchange(mine_ref.at[0], [(plane, spot, plane_ref, plane_sem)])
    plane_ref[spot] = mine_ref[0]
    for peer in plane:
        arrived(mine_ref.at[0], XS * peer["board_0"] + peer["board_1"], plane_ref, plane_sem)
    mine_ref[1] = functools.reduce(jnp.add, [plane_ref[k] for k in range(YS * XS)])
    sent += exchange(mine_ref.at[1], [(line, z, line_ref, line_sem), (cross, z, cross_ref, cross_sem)])
    line_ref[z] = mine_ref[1]
    for peer in line:
        arrived(mine_ref.at[1], peer["board_2"], line_ref, line_sem)
    for peer in cross:
        arrived(mine_ref.at[1], peer["board_2"], cross_ref, cross_sem)
    total = functools.reduce(jnp.add, [line_ref[k] for k in range(ZS)])
    rest = functools.reduce(jnp.add, [cross_ref[k] for k in range(ZS)])
    hand_ref[...] = total
    ends = total[6:7] + rest[6:7]
    ratio_ref[...] = ends[:, 0:1] / ends[:, 1:2]
    for copy in sent:
        copy.wait_send()


def write_kernel(*refs):
    count = (len(refs) - 1) // 2
    pieces = []
    for source, target in zip(refs[:count], refs[count:-1]):
        step = max(source.shape[0] // WRITES // 8 * 8, min(source.shape[0], 8))
        for start in range(0, source.shape[0], step):
            pieces.append((source.at[start : start + step, :], target.at[start : start + step, :]))
    copies = [pltpu.make_async_copy(*piece, refs[-1].at[k]) for k, piece in enumerate(pieces)]
    for copy in copies:
        copy.start()
    for copy in copies:
        copy.wait()


def write_out(*arrays):
    return pl.pallas_call(
        write_kernel,
        out_shape=tuple(jax.ShapeDtypeStruct(a.shape, a.dtype) for a in arrays),
        in_specs=[pl.BlockSpec(memory_space=pltpu.VMEM)] * len(arrays),
        out_specs=(pl.BlockSpec(memory_space=pl.ANY),) * len(arrays),
        scratch_shapes=[pltpu.SemaphoreType.DMA((WRITES + len(arrays),))],
        cost_estimate=pl.CostEstimate(flops=10**6, bytes_accessed=10**6, transcendentals=0),
    )(*(pltpu.with_memory_space_constraint(a, pltpu.VMEM) for a in arrays))


def local(opp_reach, hand_rank, hand_cards, pot, bet_frac, trav_reach):
    boards, hand_count = hand_rank.shape
    own_count = opp_reach.shape[1]
    lanes = -(-own_count // 128) * 128
    width = 2 * lanes
    half = boards // 2
    total_boards = boards * lax.axis_size(BOARD)
    whole = pl.BlockSpec(memory_space=pltpu.VMEM)
    board_values, hand_rows, ratio = pl.pallas_call(
        functools.partial(fused_kernel, total_boards, hand_count),
        out_shape=(
            pltpu.VMEM((boards, own_count), F32),
            pltpu.VMEM((8, 128), F32),
            pltpu.VMEM((1, 1), F32),
        ),
        in_specs=[pl.BlockSpec(memory_space=pl.ANY)] * 6,
        out_specs=(whole, whole, whole),
        scratch_shapes=[
            pltpu.VMEM((boards, own_count), BF16),
            pltpu.VMEM((half, hand_count), jnp.int32),
            pltpu.VMEM((2, hand_count), jnp.int32),
            pltpu.VMEM((1, boards), F32),
            pltpu.VMEM((1, boards), F32),
            pltpu.VMEM((own_count,), F32),
            pltpu.SemaphoreType.DMA((6,)),
            pltpu.VMEM((8 * half, width), BF16),
            pltpu.VMEM((CARDS, PARTS, ROWS, width), BF16),
            pltpu.VMEM((CARDS, PARTS, ROWS, 8 * half), F32),
            pltpu.VMEM((CARDS, ROWS, 4 * half), F32),
            pltpu.VMEM((CARDS, ROWS, 4 * half), F32),
            pltpu.VMEM((CARDS, ROWS, 4 * half), F32),
            pltpu.VMEM((2, 2 * half, PARTS * CARDS * ROWS + 128), BF16),
            pltpu.VMEM((3, half, width), F32),
            pltpu.VMEM((half // GROUP, GROUP * HI, width), BF16),
            pltpu.VMEM((half // GROUP, GROUP * SLOT, width), BF16),
            *[pltpu.VMEM((2 * GROUP * HI, 128), F32)] * 4,
            *[pltpu.VMEM((HI // 4, GROUP, 128), F32)] * 4,
            pltpu.VMEM((3, half, lanes), F32),
            pltpu.VMEM((2, width), F32),
            pltpu.VMEM((half, own_count), BF16),
            pltpu.VMEM((2, 8, 128), F32),
            pltpu.VMEM((YS * XS, 8, 128), F32),
            pltpu.VMEM((ZS, 8, 128), F32),
            pltpu.VMEM((ZS, 8, 128), F32),
            pltpu.SemaphoreType.DMA((2,)),
            pltpu.SemaphoreType.DMA((2,)),
            pltpu.SemaphoreType.DMA((2,)),
            pltpu.SemaphoreType.DMA((2, YS * XS)),
            pltpu.SemaphoreType.DMA((2, ZS)),
            pltpu.SemaphoreType.DMA((2, ZS)),
        ],
        compiler_params=pltpu.CompilerParams(
            vmem_limit_bytes=56 * 1024 * 1024, collective_id=0, has_side_effects=True
        ),
        cost_estimate=pl.CostEstimate(flops=10**9, bytes_accessed=10**6, transcendentals=0),
    )(opp_reach, hand_rank, hand_cards.T, pot[None, :], bet_frac[None, :], trav_reach)
    board_values, hand_rows, ratio = write_out(board_values, hand_rows, ratio)
    return board_values, hand_rows.reshape(-1)[:own_count], ratio[0, 0]


def solution(mesh):
    torus = Mesh(
        mesh.devices.reshape(YS, XS, ZS, mesh.shape["hand"]), ("board_0", "board_1", "board_2", "hand")
    )
    placed = (P(BOARD, "hand"), P(BOARD, None), P(), P(BOARD), P(BOARD), P("hand"))
    return jax.shard_map(
        local,
        mesh=torus,
        in_specs=placed,
        out_specs=(P(BOARD, "hand"), P("hand"), P()),
        check_vma=False,
    )
```

```python
import functools

import jax
import jax.numpy as jnp
from jax import lax
from jax.experimental import pallas as pl
from jax.experimental.pallas import tpu as pltpu
from jax.sharding import Mesh
from jax.sharding import PartitionSpec as P

CARDS = 52
BOARD = ("board_0", "board_1", "board_2")
BF16 = jnp.bfloat16
F32 = jnp.float32

PARTS = 4
SHARE = CARDS // PARTS
ROWS = 16
HI, LO = 48, 28
SLOT = 32
GROUP = 8
DBLOCK = 4
WRITES = 4
YS, XS, ZS = 4, 4, 8
MESH = pl.DeviceIdType.MESH
NT = (((1,), (1,)), ((), ()))


def iota(shape, axis):
    return lax.broadcasted_iota(jnp.int32, shape, axis)


def split2(x):
    high = x.astype(BF16)
    return high, (x - high.astype(F32)).astype(BF16)


def rank_code(rank):
    return (((rank & 127) | 128) << (rank >> 7)).astype(F32).astype(BF16)


def every_peer(places):
    y, x, z, h = places
    plane = [
        {"board_0": lax.rem(y + i, YS), "board_1": lax.rem(x + j, XS)}
        for i in (2, 1, 3, 0)
        for j in (2, 1, 3, 0)
        if i or j
    ]
    line = [{"board_2": lax.rem(z + i, ZS)} for i in (4, 3, 5, 2, 6, 1, 7)]
    cross = [{"board_2": lax.rem(z + i, ZS), "hand": 1 - h} for i in (4, 3, 5, 2, 6, 1, 7, 0)]
    return plane, line, cross


def column(row, start, size):
    n = row.shape[1]
    hit = iota((size, n), 1) == iota((size, n), 0) + start
    return jnp.sum(jnp.where(hit, row, 0.0), axis=1, keepdims=True)


def fused_kernel(
    total_boards, hand_count,
    reach_hbm, rank_hbm, cards_hbm, pot_hbm, bet_hbm, trav_hbm,
    values_ref, hand_ref, ratio_ref,
    reach_ref, rank_ref, cards_ref, pot_ref, bet_ref, trav_ref, io_sem,
    x_ref, p_ref, o_ref, w_ref, g_ref, q_ref, l_ref, f_ref, a_ref, b_ref, h0_ref, h1_ref, h2_ref, h3_ref, t0_ref, t1_ref, t2_ref, t3_ref, s_ref, c_ref,
    swap_ref, mine_ref, plane_ref, line_ref, cross_ref,
    swap_sem, pair_sem, sum_sem, plane_sem, line_sem, cross_sem,
):
    all_boards, own_count = reach_ref.shape
    boards = all_boards // 2
    block = 4 * boards
    lanes = x_ref.shape[1] // 2
    width = 2 * lanes
    places = tuple(lax.axis_index(name) for name in BOARD) + (lax.axis_index("hand"),)
    y, x, z, me = places
    plane, line, cross = every_peer(places)
    barrier = pltpu.get_barrier_semaphore()

    def cols_of(half, start=0, size=lanes):
        return pl.ds(pl.multiple_of(half * lanes + start, 128), size)

    def rows_of(core):
        return pl.ds(pl.multiple_of(core * boards, boards), boards)

    def to_partner(source, target, sems):
        copy = pltpu.make_async_remote_copy(
            source, target, sems.at[0], sems.at[1], device_id={"hand": 1 - me}, device_id_type=MESH
        )
        copy.start()
        return copy

    loads = [
        pltpu.make_async_copy(source, target, io_sem.at[k])
        for k, (source, target) in enumerate(
            (
                (cards_hbm, cards_ref),
                (rank_hbm.at[rows_of(me), :], rank_ref),
                (reach_hbm, reach_ref),
                (pot_hbm, pot_ref),
                (bet_hbm, bet_ref),
                (trav_hbm, trav_ref),
            )
        )
    ]
    for load in loads:
        load.start()
    for peer in plane + line + cross:
        pl.semaphore_signal(barrier, inc=1, device_id=peer, device_id_type=MESH)

    loads[0].wait()
    for half in range(2):
        start = half * lanes
        c_ref[:, start + lanes - 128 : start + lanes] = jnp.full((2, 128), -1.0, F32)
        c_ref[:, start : start + own_count] = cards_ref[:, half * own_count : (half + 1) * own_count].astype(F32)

    row16 = iota((16, lanes), 0)
    own_row = [
        jnp.where(row16 < SHARE, row16 + SHARE * q, -5).astype(F32).astype(BF16) for q in range(PARTS)
    ]

    def hot_rows(half, d):
        low, high = c_ref[0:1, cols_of(half)], c_ref[1:2, cols_of(half)]
        partner = jnp.where(low == float(d), high, jnp.where(high == float(d), low, -1.0))
        wide = jnp.broadcast_to(partner, (16, lanes)).astype(BF16)
        for q in range(PARTS):
            p_ref[d, q, :, cols_of(half)] = jnp.where(wide == own_row[q], BF16(1), BF16(0))

    loads[1].wait()
    loads[2].wait()
    for half in range(2):
        start = half * lanes
        f_ref[0:2, :, start + lanes - 128 : start + lanes] = jnp.zeros((2, boards, 128), F32)
        x_ref[:, start + lanes - 128 : start + lanes] = jnp.zeros((8 * boards, 128), BF16)
        rank = rank_ref[:, half * own_count : (half + 1) * own_count]
        x_ref[block : block + boards, start : start + own_count] = rank_code(rank)
        hi = (rank * 2341) >> 16
        f_ref[0, :, start : start + own_count] = hi.astype(F32)
        f_ref[1, :, start : start + own_count] = (rank - LO * hi).astype(F32)
    for k in range(1, PARTS):
        x_ref[block + k * boards : block + (k + 1) * boards, :] = x_ref[block : block + boards, :]

    def place(half, reach):
        x_ref[0:boards, pl.ds(pl.multiple_of(half * lanes, 128), own_count)] = reach
        f_ref[2, :, cols_of(half)] = x_ref[0:boards, cols_of(half)].astype(F32)
        for k in range(1, PARTS):
            x_ref[k * boards : (k + 1) * boards, cols_of(half)] = x_ref[0:boards, cols_of(half)]

    chunk = CARDS // PARTS

    def to_cards(half, more):
        for i in range(PARTS):
            these = slice(chunk * i, chunk * (i + 1))
            if not more:
                for d in range(chunk * i, chunk * (i + 1)):
                    hot_rows(half, d)
            if more:
                high_factor(half, i)
            rows = p_ref[these, :, :, cols_of(half)].reshape(chunk * PARTS * ROWS, lanes)
            got = lax.dot_general(rows, x_ref[:, cols_of(half)], NT, preferred_element_type=F32)
            got = got.reshape(chunk, PARTS, ROWS, 2 * block)
            o_ref[these] = got + o_ref[these] if more else got

    digit = iota((16, lanes), 0).astype(F32).astype(BF16)

    def high_factor(half, g):
        for b in range(GROUP):
            at = GROUP * g + b
            hi = jnp.broadcast_to(f_ref[0, at : at + 1, cols_of(half)], (16, lanes)).astype(BF16)
            reach = jnp.broadcast_to(f_ref[2, at : at + 1, cols_of(half)], (16, lanes)).astype(BF16)
            for part in range(HI // 16):
                rows = slice(HI * b + 16 * part, HI * b + 16 * part + 16)
                hit = hi == digit + BF16(16 * part)
                a_ref[g, rows, cols_of(half)] = jnp.where(hit, reach, BF16(0))

    def low_factor(half, g):
        for b in range(GROUP):
            at = GROUP * g + b
            lo = jnp.broadcast_to(f_ref[1, at : at + 1, cols_of(half)], (16, lanes)).astype(BF16)
            for part in range(SLOT // 16):
                at = SLOT * b + 16 * part
                b_ref[g, at : at + 16, cols_of(half)] = lax.clamp(
                    BF16(-1), digit + BF16(16 * part) - lo, BF16(1)
                )

    h_refs = (h0_ref, h1_ref, h2_ref, h3_ref)

    def tabulate(g, half=1 - me):
        got = lax.dot_general(
            a_ref[g, :, cols_of(half)], b_ref[g, :, cols_of(half)], NT, preferred_element_type=F32
        )
        for k in range(2):
            rows, piece = slice(GROUP * HI * k, GROUP * HI * (k + 1)), got[:, 128 * k : 128 * (k + 1)]
            h_refs[g][rows, :] = piece if half is me else piece + h_refs[g][rows, :]

    place(me, reach_ref[rows_of(me), :])
    to_cards(me, False)
    loads[3].wait()
    groups = boards // GROUP
    for d in range(CARDS):
        hot_rows(1 - me, d)
    for g in range(groups):
        low_factor(me, g)
        low_factor(1 - me, g)
    pl.semaphore_wait(barrier, len(plane + line + cross))
    swap = to_partner(reach_ref.at[rows_of(1 - me), :], swap_ref, swap_sem)
    for g in range(groups):
        high_factor(me, g)
        tabulate(g, me)
    swap.wait()
    place(1 - me, swap_ref[...])
    to_cards(1 - me, True)

    part_of = iota((ROWS, block), 1) // boards

    def pack(d, carry):
        for ref, at in ((w_ref, 0), (g_ref, block)):
            got = o_ref[d, 0, :, at : at + block]
            for q in range(1, PARTS):
                got = jnp.where(part_of == q, o_ref[d, q, :, at : at + block], got)
            ref[d] = got
        return carry

    lax.fori_loop(0, CARDS, pack, 0, unroll=4)

    def pairs(i, carry):
        mine = [g_ref[DBLOCK * i + k].astype(BF16) for k in range(DBLOCK)]
        sums = [None] * DBLOCK
        for e in range(CARDS):
            ge, we = g_ref[e].astype(BF16), w_ref[e].astype(BF16)
            for k in range(DBLOCK):
                sign = lax.clamp(BF16(-1), mine[k] - ge, BF16(1))
                term = sign.astype(F32) * we.astype(F32)
                sums[k] = term if sums[k] is None else sums[k] + term
        for k in range(DBLOCK):
            q_ref[DBLOCK * i + k] = sums[k]
        return carry

    lax.fori_loop(0, CARDS // DBLOCK, pairs, 0)
    card = iota((64, lanes), 0).astype(F32)
    card_totals = jnp.zeros((boards, 64), F32)
    for half in (1 - me, me):
        hold = ((card == c_ref[0:1, cols_of(half)]) | (card == c_ref[1:2, cols_of(half)])).astype(F32).astype(BF16)
        card_totals = card_totals + lax.dot_general(
            x_ref[0:boards, cols_of(half)], hold, NT, preferred_element_type=F32
        )
    tabulate(0)
    tabulate(1)
    wide = jnp.concatenate([card_totals, jnp.zeros((boards, 64), F32)], axis=1)
    pair_lanes = PARTS * CARDS * ROWS
    turned = jnp.transpose(q_ref[...].reshape(CARDS * ROWS, block))
    for k, piece in enumerate(split2(turned)):
        for q in range(PARTS):
            l_ref[0, boards * k : boards * (k + 1), CARDS * ROWS * q : CARDS * ROWS * (q + 1)] = piece[
                boards * q : boards * (q + 1)
            ]
    for k, piece in enumerate(split2(wide)):
        l_ref[0, boards * k : boards * (k + 1), pair_lanes:] = piece
    pair_copy = to_partner(l_ref.at[0], l_ref.at[1], pair_sem)

    row_slot = iota((GROUP, 128), 0) % 4
    upper = iota((GROUP, 128), 0) < 4
    shift = (iota((GROUP, 128), 1) // SLOT - row_slot) % 4
    tiles = HI // 4
    t_refs = (t0_ref, t1_ref, t2_ref, t3_ref)

    def lay_out(g):
        for t in range(tiles):
            parts = [
                jnp.where(
                    upper,
                    h_refs[g][pl.ds(4 * t + k, GROUP, stride=HI), :],
                    h_refs[g][pl.ds(4 * t + k + GROUP * HI, GROUP, stride=HI), :],
                )
                for k in range(4)
            ]
            row = None
            for k in range(4):
                moved = parts[(3 + k) % 4]
                for p in range(3):
                    moved = jnp.where(row_slot == p, parts[(p + k) % 4], moved)
                row = moved if row is None else jnp.where(shift == k, pltpu.roll(moved, SLOT * k, 1), row)
            t_refs[g][t] = row

    src, dst = iota((256, 128), 0), iota((256, 128), 1)
    within = (dst // SLOT > (src - 128) // SLOT).astype(F32) - (dst // SLOT < (src - 128) // SLOT).astype(F32)
    spread = jnp.where(src % SLOT == LO, jnp.where(src < 128, 1.0, within), 0.0).astype(BF16)
    spot = iota((GROUP, 128), 1) % SLOT == LO

    def add_rows(g):
        run = jnp.zeros((GROUP, 128), F32)
        below, whole = [], []
        for t in range(tiles):
            mark = jnp.where(spot, t_refs[g][t], 0.0)
            whole.append(mark)
            below.append(run)
            run = run + mark
        both = jnp.concatenate(
            [jnp.concatenate([below[t] - (run - below[t] - whole[t]), whole[t]], axis=1) for t in range(tiles)],
            axis=0,
        )
        got = jnp.dot(jnp.concatenate(split2(both), axis=0), spread, preferred_element_type=F32)
        got = got[: GROUP * tiles] + got[GROUP * tiles :]
        for t in range(tiles):
            t_refs[g][t] = t_refs[g][t] + got[GROUP * t : GROUP * (t + 1)]

    def look_up(g, half=1 - me):
        rows = slice(GROUP * g, GROUP * (g + 1))
        for k in range(lanes // 128):
            hi = f_ref[0, rows, cols_of(half, 128 * k, 128)].astype(jnp.int32)
            lo = f_ref[1, rows, cols_of(half, 128 * k, 128)].astype(jnp.int32)
            tile = hi >> 2
            at = ((hi & 3) << 5) + lo
            found = jnp.zeros((GROUP, 128), F32)
            for t in range(tiles):
                got = jnp.take_along_axis(t_refs[g][t], at, axis=1, mode="promise_in_bounds")
                found = jnp.where(tile == t, got, found)
            s_ref[half, rows, 128 * k : 128 * k + 128] = found

    stages = (tabulate, lay_out, add_rows, look_up)
    for step in range(groups + len(stages) - 1):
        for k, stage in enumerate(stages):
            if 0 <= step - k < groups and (k or step > 1):
                stage(step - k)
    sum_copy = to_partner(s_ref.at[1 - me], s_ref.at[2], sum_sem)

    pair_copy.wait()
    for g in range(groups):
        look_up(g, me)
    back = [p_ref[:, q, :, cols_of(me)].reshape(CARDS * ROWS, lanes) for q in range(PARTS)]
    shared = jnp.dot(
        l_ref[:, :, 0:pair_lanes].reshape(4 * boards, pair_lanes),
        jnp.concatenate(back, axis=0),
        preferred_element_type=F32,
    )
    held = jnp.dot(
        l_ref[:, :, pair_lanes:].reshape(4 * boards, 128)[:, 0:64], hold, preferred_element_type=F32
    )
    sum_copy.wait()
    for load in loads[4:]:
        load.wait()
    part = mass = None
    for k, core in ((0, me), (1, 1 - me)):
        at = 2 * boards * k
        live = (
            0.5 * jnp.sum(l_ref[k, :, pair_lanes:].astype(F32).reshape(2, boards, 128).sum(0), axis=1, keepdims=True)
            - (held[at : at + boards] + held[at + boards : at + 2 * boards])
        )[:, 0:own_count] + reach_ref[rows_of(core), :].astype(F32)
        sums = s_ref[me] if k == 0 else s_ref[2]
        margin = (sums - (shared[at : at + boards] + shared[at + boards : at + 2 * boards]))[:, 0:own_count]
        pot = column(pot_ref[...], core * boards, boards)
        bet = column(bet_ref[...], core * boards, boards)
        half_pot = 0.5 * pot
        half_pot, bet = half_pot / hand_count, bet / hand_count
        stake = half_pot * live
        values = jnp.maximum((half_pot + bet * pot) * margin, -stake)
        values_ref[rows_of(core), :] = values
        values, stake = (jnp.sum(v, axis=0, keepdims=True) for v in (values, stake))
        part = values if part is None else part + values
        mass = stake if mass is None else mass + stake
    part, mass = part / total_boards, mass / total_boards
    trav = trav_ref[...].reshape(1, own_count)
    numerator = jnp.sum(part * trav, axis=1, keepdims=True)
    denominator = jnp.sum(mass * trav, axis=1, keepdims=True)

    spot = XS * y + x
    last = lanes // 128 - 1
    for k in range(last):
        mine_ref[0, k : k + 1, :] = part[:, 128 * k : 128 * (k + 1)]
    fill = jnp.concatenate([part[:, 128 * last :], jnp.zeros((1, lanes - own_count), F32)], axis=1)
    lane = iota((1, 128), 1)
    mine_ref[0, last : last + 1, :] = jnp.where(lane == 126, numerator, jnp.where(lane == 127, denominator, fill))

    rows, ends_row = slice(0, lanes // 128), slice(last, last + 1)

    def exchange(source, groups):
        sent = []
        for peers, here, these, slots, sems in groups:
            for k, peer in enumerate(peers):
                copy = pltpu.make_async_remote_copy(
                    source.at[these, :], slots.at[here, these, :], sems.at[0, k], sems.at[1, here],
                    device_id=peer, device_id_type=MESH,
                )
                copy.start()
                sent.append(copy)
        return sent

    def arrived(source, where, these, slots, sems):
        pltpu.make_async_remote_copy(
            source.at[these, :], slots.at[where, these, :], sems.at[0, 0], sems.at[1, where],
            device_id=plane[0], device_id_type=MESH,
        ).wait_recv()

    sent = exchange(mine_ref.at[0], [(plane, spot, rows, plane_ref, plane_sem)])
    plane_ref[spot, rows, :] = mine_ref[0, rows, :]
    for peer in plane:
        arrived(mine_ref.at[0], XS * peer["board_0"] + peer["board_1"], rows, plane_ref, plane_sem)
    mine_ref[1, rows, :] = functools.reduce(jnp.add, [plane_ref[k, rows, :] for k in range(YS * XS)])
    sent += exchange(
        mine_ref.at[1], [(line, z, rows, line_ref, line_sem), (cross, z, ends_row, cross_ref, cross_sem)]
    )
    line_ref[z, rows, :] = mine_ref[1, rows, :]
    for peer in line:
        arrived(mine_ref.at[1], peer["board_2"], rows, line_ref, line_sem)
    for peer in cross:
        arrived(mine_ref.at[1], peer["board_2"], ends_row, cross_ref, cross_sem)
    total = functools.reduce(jnp.add, [line_ref[k, rows, :] for k in range(ZS)])
    rest = functools.reduce(jnp.add, [cross_ref[k, ends_row, :] for k in range(ZS)])
    hand_ref[rows, :] = total
    hand_ref[lanes // 128 :, :] = jnp.zeros((8 - lanes // 128, 128), F32)
    ends = total[ends_row] + rest
    ratio_ref[...] = ends[:, 126:127] / ends[:, 127:128]
    for copy in sent:
        copy.wait_send()


def write_kernel(*refs):
    count = (len(refs) - 1) // 2
    pieces = []
    for source, target in zip(refs[:count], refs[count:-1]):
        step = max(source.shape[0] // WRITES // 8 * 8, min(source.shape[0], 8))
        for start in range(0, source.shape[0], step):
            pieces.append((source.at[start : start + step, :], target.at[start : start + step, :]))
    copies = [pltpu.make_async_copy(*piece, refs[-1].at[k]) for k, piece in enumerate(pieces)]
    for copy in copies:
        copy.start()
    for copy in copies:
        copy.wait()


def write_out(*arrays):
    return pl.pallas_call(
        write_kernel,
        out_shape=tuple(jax.ShapeDtypeStruct(a.shape, a.dtype) for a in arrays),
        in_specs=[pl.BlockSpec(memory_space=pltpu.VMEM)] * len(arrays),
        out_specs=(pl.BlockSpec(memory_space=pl.ANY),) * len(arrays),
        scratch_shapes=[pltpu.SemaphoreType.DMA((WRITES + len(arrays),))],
        cost_estimate=pl.CostEstimate(flops=10**6, bytes_accessed=10**6, transcendentals=0),
    )(*(pltpu.with_memory_space_constraint(a, pltpu.VMEM) for a in arrays))


def local(opp_reach, hand_rank, hand_cards, pot, bet_frac, trav_reach):
    boards, hand_count = hand_rank.shape
    own_count = opp_reach.shape[1]
    lanes = -(-own_count // 128) * 128
    width = 2 * lanes
    half = boards // 2
    total_boards = boards * lax.axis_size(BOARD)
    whole = pl.BlockSpec(memory_space=pltpu.VMEM)
    board_values, hand_rows, ratio = pl.pallas_call(
        functools.partial(fused_kernel, total_boards, hand_count),
        out_shape=(
            pltpu.VMEM((boards, own_count), F32),
            pltpu.VMEM((8, 128), F32),
            pltpu.VMEM((1, 1), F32),
        ),
        in_specs=[pl.BlockSpec(memory_space=pl.ANY)] * 6,
        out_specs=(whole, whole, whole),
        scratch_shapes=[
            pltpu.VMEM((boards, own_count), BF16),
            pltpu.VMEM((half, hand_count), jnp.int32),
            pltpu.VMEM((2, hand_count), jnp.int32),
            pltpu.VMEM((1, boards), F32),
            pltpu.VMEM((1, boards), F32),
            pltpu.VMEM((own_count,), F32),
            pltpu.SemaphoreType.DMA((6,)),
            pltpu.VMEM((8 * half, width), BF16),
            pltpu.VMEM((CARDS, PARTS, ROWS, width), BF16),
            pltpu.VMEM((CARDS, PARTS, ROWS, 8 * half), F32),
            pltpu.VMEM((CARDS, ROWS, 4 * half), F32),
            pltpu.VMEM((CARDS, ROWS, 4 * half), F32),
            pltpu.VMEM((CARDS, ROWS, 4 * half), F32),
            pltpu.VMEM((2, 2 * half, PARTS * CARDS * ROWS + 128), BF16),
            pltpu.VMEM((3, half, width), F32),
            pltpu.VMEM((half // GROUP, GROUP * HI, width), BF16),
            pltpu.VMEM((half // GROUP, GROUP * SLOT, width), BF16),
            *[pltpu.VMEM((2 * GROUP * HI, 128), F32)] * 4,
            *[pltpu.VMEM((HI // 4, GROUP, 128), F32)] * 4,
            pltpu.VMEM((3, half, lanes), F32),
            pltpu.VMEM((2, width), F32),
            pltpu.VMEM((half, own_count), BF16),
            pltpu.VMEM((2, 8, 128), F32),
            pltpu.VMEM((YS * XS, 8, 128), F32),
            pltpu.VMEM((ZS, 8, 128), F32),
            pltpu.VMEM((ZS, 8, 128), F32),
            pltpu.SemaphoreType.DMA((2,)),
            pltpu.SemaphoreType.DMA((2,)),
            pltpu.SemaphoreType.DMA((2,)),
            pltpu.SemaphoreType.DMA((2, YS * XS)),
            pltpu.SemaphoreType.DMA((2, ZS)),
            pltpu.SemaphoreType.DMA((2, ZS)),
        ],
        compiler_params=pltpu.CompilerParams(
            vmem_limit_bytes=56 * 1024 * 1024, collective_id=0, has_side_effects=True
        ),
        cost_estimate=pl.CostEstimate(flops=10**9, bytes_accessed=10**6, transcendentals=0),
    )(opp_reach, hand_rank, hand_cards.T, pot[None, :], bet_frac[None, :], trav_reach)
    board_values, hand_rows, ratio = write_out(board_values, hand_rows, ratio)
    return board_values, hand_rows.reshape(-1)[:own_count], ratio[0, 0]


def solution(mesh):
    torus = Mesh(
        mesh.devices.reshape(YS, XS, ZS, mesh.shape["hand"]), ("board_0", "board_1", "board_2", "hand")
    )
    placed = (P(BOARD, "hand"), P(BOARD, None), P(), P(BOARD), P(BOARD), P("hand"))
    return jax.shard_map(
        local,
        mesh=torus,
        in_specs=placed,
        out_specs=(P(BOARD, "hand"), P("hand"), P()),
        check_vma=False,
    )
```

```python
import functools

import jax
import jax.numpy as jnp
from jax import lax
from jax.experimental import pallas as pl
from jax.experimental.pallas import tpu as pltpu
from jax.sharding import Mesh
from jax.sharding import PartitionSpec as P

CARDS = 52
BOARD = ("board_0", "board_1", "board_2")
BF16 = jnp.bfloat16
F32 = jnp.float32

PARTS = 4
SHARE = CARDS // PARTS
ROWS = 16
HI, LO = 48, 28
SLOT = 32
GROUP = 8
DBLOCK = 4
WRITES = 4
YS, XS, ZS = 4, 4, 8
MESH = pl.DeviceIdType.MESH
NT = (((1,), (1,)), ((), ()))


def iota(shape, axis):
    return lax.broadcasted_iota(jnp.int32, shape, axis)


def split2(x):
    high = x.astype(BF16)
    return high, (x - high.astype(F32)).astype(BF16)


def rank_code(rank):
    return (((rank & 127) | 128) << (rank >> 7)).astype(F32).astype(BF16)


def every_peer(places):
    y, x, z, h = places
    plane = [
        {"board_0": lax.rem(y + i, YS), "board_1": lax.rem(x + j, XS)}
        for i in (2, 1, 3, 0)
        for j in (2, 1, 3, 0)
        if i or j
    ]
    line = [{"board_2": lax.rem(z + i, ZS)} for i in (4, 3, 5, 2, 6, 1, 7)]
    cross = [{"board_2": lax.rem(z + i, ZS), "hand": 1 - h} for i in (4, 3, 5, 2, 6, 1, 7, 0)]
    return plane, line, cross


def column(row, start, size):
    n = row.shape[1]
    hit = iota((size, n), 1) == iota((size, n), 0) + start
    return jnp.sum(jnp.where(hit, row, 0.0), axis=1, keepdims=True)


def fused_kernel(
    total_boards, hand_count,
    reach_hbm, rank_hbm, cards_hbm, pot_hbm, bet_hbm, trav_hbm,
    values_ref, hand_ref, ratio_ref,
    reach_ref, rank_ref, cards_ref, pot_ref, bet_ref, trav_ref, io_sem,
    x_ref, p_ref, o_ref, w_ref, g_ref, q_ref, l_ref, f_ref, a_ref, b_ref, h0_ref, h1_ref, h2_ref, h3_ref, t0_ref, t1_ref, t2_ref, t3_ref, s_ref, c_ref,
    swap_ref, mine_ref, plane_ref, line_ref, cross_ref,
    swap_sem, pair_sem, sum_sem, plane_sem, line_sem, cross_sem,
):
    all_boards, own_count = reach_ref.shape
    boards = all_boards // 2
    block = 4 * boards
    lanes = x_ref.shape[1] // 2
    width = 2 * lanes
    places = tuple(lax.axis_index(name) for name in BOARD) + (lax.axis_index("hand"),)
    y, x, z, me = places
    plane, line, cross = every_peer(places)
    barrier = pltpu.get_barrier_semaphore()

    def cols_of(half, start=0, size=lanes):
        return pl.ds(pl.multiple_of(half * lanes + start, 128), size)

    def rows_of(core):
        return pl.ds(pl.multiple_of(core * boards, boards), boards)

    def to_partner(source, target, sems):
        copy = pltpu.make_async_remote_copy(
            source, target, sems.at[0], sems.at[1], device_id={"hand": 1 - me}, device_id_type=MESH
        )
        copy.start()
        return copy

    loads = [
        pltpu.make_async_copy(source, target, io_sem.at[k])
        for k, (source, target) in enumerate(
            (
                (cards_hbm, cards_ref),
                (rank_hbm.at[rows_of(me), :], rank_ref),
                (reach_hbm, reach_ref),
                (pot_hbm, pot_ref),
                (bet_hbm, bet_ref),
                (trav_hbm, trav_ref),
            )
        )
    ]
    for load in loads:
        load.start()
    for peer in plane + line + cross:
        pl.semaphore_signal(barrier, inc=1, device_id=peer, device_id_type=MESH)

    loads[0].wait()
    for half in range(2):
        start = half * lanes
        c_ref[:, start + lanes - 128 : start + lanes] = jnp.full((2, 128), -1.0, F32)
        c_ref[:, start : start + own_count] = cards_ref[:, half * own_count : (half + 1) * own_count].astype(F32)

    row16 = iota((16, lanes), 0)
    own_row = [
        jnp.where(row16 < SHARE, row16 + SHARE * q, -5).astype(F32).astype(BF16) for q in range(PARTS)
    ]

    def hot_rows(half, d):
        low, high = c_ref[0:1, cols_of(half)], c_ref[1:2, cols_of(half)]
        partner = jnp.where(low == float(d), high, jnp.where(high == float(d), low, -1.0))
        wide = jnp.broadcast_to(partner, (16, lanes)).astype(BF16)
        for q in range(PARTS):
            p_ref[d, q, :, cols_of(half)] = jnp.where(wide == own_row[q], BF16(1), BF16(0))

    loads[1].wait()
    loads[2].wait()
    for half in range(2):
        start = half * lanes
        f_ref[0:2, :, start + lanes - 128 : start + lanes] = jnp.zeros((2, boards, 128), F32)
        x_ref[:, start + lanes - 128 : start + lanes] = jnp.zeros((8 * boards, 128), BF16)
        rank = rank_ref[:, half * own_count : (half + 1) * own_count]
        x_ref[block : block + boards, start : start + own_count] = rank_code(rank)
        hi = (rank * 2341) >> 16
        f_ref[0, :, start : start + own_count] = hi.astype(F32)
        f_ref[1, :, start : start + own_count] = (rank - LO * hi).astype(F32)
    for k in range(1, PARTS):
        x_ref[block + k * boards : block + (k + 1) * boards, :] = x_ref[block : block + boards, :]

    def place(half, reach):
        x_ref[0:boards, pl.ds(pl.multiple_of(half * lanes, 128), own_count)] = reach
        f_ref[2, :, cols_of(half)] = x_ref[0:boards, cols_of(half)].astype(F32)
        for k in range(1, PARTS):
            x_ref[k * boards : (k + 1) * boards, cols_of(half)] = x_ref[0:boards, cols_of(half)]

    chunk = CARDS // PARTS

    def to_cards(half, more):
        for i in range(PARTS):
            these = slice(chunk * i, chunk * (i + 1))
            if not more:
                for d in range(chunk * i, chunk * (i + 1)):
                    hot_rows(half, d)
            if more:
                high_factor(half, i)
            rows = p_ref[these, :, :, cols_of(half)].reshape(chunk * PARTS * ROWS, lanes)
            got = lax.dot_general(rows, x_ref[:, cols_of(half)], NT, preferred_element_type=F32)
            got = got.reshape(chunk, PARTS, ROWS, 2 * block)
            o_ref[these] = got + o_ref[these] if more else got

    digit = iota((16, lanes), 0).astype(F32).astype(BF16)

    pair = (iota((16, lanes), 0) // GROUP).astype(F32).astype(BF16)

    def high_factor(half, g):
        boards_here = slice(GROUP * g, GROUP * (g + 1))
        hi, reach = (
            jnp.concatenate([f_ref[k, boards_here, cols_of(half)]] * 2, axis=0).astype(BF16) for k in (0, 2)
        )
        for two in range(HI // 2):
            hit = hi == pair + BF16(2 * two)
            a_ref[g, 16 * two : 16 * two + 16, cols_of(half)] = jnp.where(hit, reach, BF16(0))

    def low_factor(half, g):
        for b in range(GROUP):
            at = GROUP * g + b
            lo = jnp.broadcast_to(f_ref[1, at : at + 1, cols_of(half)], (16, lanes)).astype(BF16)
            for part in range(SLOT // 16):
                at = SLOT * b + 16 * part
                b_ref[g, at : at + 16, cols_of(half)] = lax.clamp(
                    BF16(-1), digit + BF16(16 * part) - lo, BF16(1)
                )

    h_refs = (h0_ref, h1_ref, h2_ref, h3_ref)

    def tabulate(g, half=1 - me):
        got = lax.dot_general(
            a_ref[g, :, cols_of(half)], b_ref[g, :, cols_of(half)], NT, preferred_element_type=F32
        )
        for k in range(2):
            rows, piece = slice(GROUP * HI * k, GROUP * HI * (k + 1)), got[:, 128 * k : 128 * (k + 1)]
            h_refs[g][rows, :] = piece if half is me else piece + h_refs[g][rows, :]

    place(me, reach_ref[rows_of(me), :])
    to_cards(me, False)
    loads[3].wait()
    groups = boards // GROUP
    for d in range(CARDS):
        hot_rows(1 - me, d)
    for g in range(groups):
        low_factor(me, g)
        low_factor(1 - me, g)
    pl.semaphore_wait(barrier, len(plane + line + cross))
    swap = to_partner(reach_ref.at[rows_of(1 - me), :], swap_ref, swap_sem)
    for g in range(groups):
        high_factor(me, g)
        tabulate(g, me)
    swap.wait()
    place(1 - me, swap_ref[...])
    to_cards(1 - me, True)

    part_of = iota((ROWS, block), 1) // boards

    def pack(d, carry):
        for ref, at in ((w_ref, 0), (g_ref, block)):
            got = o_ref[d, 0, :, at : at + block]
            for q in range(1, PARTS):
                got = jnp.where(part_of == q, o_ref[d, q, :, at : at + block], got)
            ref[d] = got
        return carry

    lax.fori_loop(0, CARDS, pack, 0, unroll=4)

    def pairs(i, carry):
        mine = [g_ref[DBLOCK * i + k].astype(BF16) for k in range(DBLOCK)]
        sums = [None] * DBLOCK
        for e in range(CARDS):
            ge, we = g_ref[e].astype(BF16), w_ref[e].astype(BF16)
            for k in range(DBLOCK):
                sign = lax.clamp(BF16(-1), mine[k] - ge, BF16(1))
                term = sign.astype(F32) * we.astype(F32)
                sums[k] = term if sums[k] is None else sums[k] + term
        for k in range(DBLOCK):
            q_ref[DBLOCK * i + k] = sums[k]
        return carry

    lax.fori_loop(0, CARDS // DBLOCK, pairs, 0)
    card = iota((64, lanes), 0).astype(F32)
    card_totals = jnp.zeros((boards, 64), F32)
    for half in (1 - me, me):
        hold = ((card == c_ref[0:1, cols_of(half)]) | (card == c_ref[1:2, cols_of(half)])).astype(F32).astype(BF16)
        card_totals = card_totals + lax.dot_general(
            x_ref[0:boards, cols_of(half)], hold, NT, preferred_element_type=F32
        )
    wide = jnp.concatenate([card_totals, jnp.zeros((boards, 64), F32)], axis=1)
    pair_lanes = PARTS * CARDS * ROWS
    turned = jnp.transpose(q_ref[...].reshape(CARDS * ROWS, block))
    for k, piece in enumerate(split2(turned)):
        for q in range(PARTS):
            l_ref[0, boards * k : boards * (k + 1), CARDS * ROWS * q : CARDS * ROWS * (q + 1)] = piece[
                boards * q : boards * (q + 1)
            ]
    for k, piece in enumerate(split2(wide)):
        l_ref[0, boards * k : boards * (k + 1), pair_lanes:] = piece
    pair_copy = to_partner(l_ref.at[0], l_ref.at[1], pair_sem)

    row_slot = iota((GROUP, 128), 0) % 4
    upper = iota((GROUP, 128), 0) < 4
    shift = (iota((GROUP, 128), 1) // SLOT - row_slot) % 4
    tiles = HI // 4
    t_refs = (t0_ref, t1_ref, t2_ref, t3_ref)

    def lay_out(g):
        for t in range(tiles):
            parts = []
            for k in range(4):
                at = GROUP * (4 * t + k)
                parts.append(
                    jnp.where(
                        upper,
                        h_refs[g][at : at + GROUP, :],
                        h_refs[g][GROUP * HI + at : GROUP * HI + at + GROUP, :],
                    )
                )
            row = None
            for k in range(4):
                moved = parts[(3 + k) % 4]
                for p in range(3):
                    moved = jnp.where(row_slot == p, parts[(p + k) % 4], moved)
                row = moved if row is None else jnp.where(shift == k, pltpu.roll(moved, SLOT * k, 1), row)
            t_refs[g][t] = row

    src, dst = iota((256, 128), 0), iota((256, 128), 1)
    within = (dst // SLOT > (src - 128) // SLOT).astype(F32) - (dst // SLOT < (src - 128) // SLOT).astype(F32)
    spread = jnp.where(src % SLOT == LO, jnp.where(src < 128, 1.0, within), 0.0).astype(BF16)
    spot = iota((GROUP, 128), 1) % SLOT == LO

    def add_rows(g):
        run = jnp.zeros((GROUP, 128), F32)
        below, whole = [], []
        for t in range(tiles):
            mark = jnp.where(spot, t_refs[g][t], 0.0)
            whole.append(mark)
            below.append(run)
            run = run + mark
        both = jnp.concatenate(
            [jnp.concatenate([below[t] - (run - below[t] - whole[t]), whole[t]], axis=1) for t in range(tiles)],
            axis=0,
        )
        got = jnp.dot(jnp.concatenate(split2(both), axis=0), spread, preferred_element_type=F32)
        got = got[: GROUP * tiles] + got[GROUP * tiles :]
        for t in range(tiles):
            t_refs[g][t] = t_refs[g][t] + got[GROUP * t : GROUP * (t + 1)]

    def look_up(g, half=1 - me):
        rows = slice(GROUP * g, GROUP * (g + 1))
        for k in range(lanes // 128):
            hi = f_ref[0, rows, cols_of(half, 128 * k, 128)].astype(jnp.int32)
            lo = f_ref[1, rows, cols_of(half, 128 * k, 128)].astype(jnp.int32)
            tile = hi >> 2
            at = ((hi & 3) << 5) + lo
            found = jnp.zeros((GROUP, 128), F32)
            for t in range(tiles):
                got = jnp.take_along_axis(t_refs[g][t], at, axis=1, mode="promise_in_bounds")
                found = jnp.where(tile == t, got, found)
            s_ref[half, rows, 128 * k : 128 * k + 128] = found

    stages = (tabulate, lay_out, add_rows, look_up)
    for step in range(groups + len(stages) - 1):
        for k, stage in enumerate(stages):
            if 0 <= step - k < groups:
                stage(step - k)
    sum_copy = to_partner(s_ref.at[1 - me], s_ref.at[2], sum_sem)

    pair_copy.wait()
    for g in range(groups):
        look_up(g, me)
    back = [p_ref[:, q, :, cols_of(me)].reshape(CARDS * ROWS, lanes) for q in range(PARTS)]
    shared = jnp.dot(
        l_ref[:, :, 0:pair_lanes].reshape(4 * boards, pair_lanes),
        jnp.concatenate(back, axis=0),
        preferred_element_type=F32,
    )
    held = jnp.dot(
        l_ref[:, :, pair_lanes:].reshape(4 * boards, 128)[:, 0:64], hold, preferred_element_type=F32
    )
    sum_copy.wait()
    for load in loads[4:]:
        load.wait()
    part = mass = None
    for k, core in ((0, me), (1, 1 - me)):
        at = 2 * boards * k
        live = (
            0.5 * jnp.sum(l_ref[k, :, pair_lanes:].astype(F32).reshape(2, boards, 128).sum(0), axis=1, keepdims=True)
            - (held[at : at + boards] + held[at + boards : at + 2 * boards])
        )[:, 0:own_count] + reach_ref[rows_of(core), :].astype(F32)
        sums = s_ref[me] if k == 0 else s_ref[2]
        margin = (sums - (shared[at : at + boards] + shared[at + boards : at + 2 * boards]))[:, 0:own_count]
        pot = column(pot_ref[...], core * boards, boards)
        bet = column(bet_ref[...], core * boards, boards)
        half_pot = 0.5 * pot
        half_pot, bet = half_pot / hand_count, bet / hand_count
        stake = half_pot * live
        values = jnp.maximum((half_pot + bet * pot) * margin, -stake)
        values_ref[rows_of(core), :] = values
        values, stake = (jnp.sum(v, axis=0, keepdims=True) for v in (values, stake))
        part = values if part is None else part + values
        mass = stake if mass is None else mass + stake
    part, mass = part / total_boards, mass / total_boards
    trav = trav_ref[...].reshape(1, own_count)
    numerator = jnp.sum(part * trav, axis=1, keepdims=True)
    denominator = jnp.sum(mass * trav, axis=1, keepdims=True)

    spot = XS * y + x
    last = lanes // 128 - 1
    for k in range(last):
        mine_ref[0, k : k + 1, :] = part[:, 128 * k : 128 * (k + 1)]
    fill = jnp.concatenate([part[:, 128 * last :], jnp.zeros((1, lanes - own_count), F32)], axis=1)
    lane = iota((1, 128), 1)
    mine_ref[0, last : last + 1, :] = jnp.where(lane == 126, numerator, jnp.where(lane == 127, denominator, fill))

    rows, ends_row = slice(0, lanes // 128), slice(last, last + 1)

    def exchange(source, groups):
        sent = []
        for peers, here, these, slots, sems in groups:
            for k, peer in enumerate(peers):
                copy = pltpu.make_async_remote_copy(
                    source.at[these, :], slots.at[here, these, :], sems.at[0, k], sems.at[1, here],
                    device_id=peer, device_id_type=MESH,
                )
                copy.start()
                sent.append(copy)
        return sent

    def arrived(source, where, these, slots, sems):
        pltpu.make_async_remote_copy(
            source.at[these, :], slots.at[where, these, :], sems.at[0, 0], sems.at[1, where],
            device_id=plane[0], device_id_type=MESH,
        ).wait_recv()

    sent = exchange(mine_ref.at[0], [(plane, spot, rows, plane_ref, plane_sem)])
    plane_ref[spot, rows, :] = mine_ref[0, rows, :]
    for peer in plane:
        arrived(mine_ref.at[0], XS * peer["board_0"] + peer["board_1"], rows, plane_ref, plane_sem)
    mine_ref[1, rows, :] = functools.reduce(jnp.add, [plane_ref[k, rows, :] for k in range(YS * XS)])
    sent += exchange(
        mine_ref.at[1], [(line, z, rows, line_ref, line_sem), (cross, z, ends_row, cross_ref, cross_sem)]
    )
    line_ref[z, rows, :] = mine_ref[1, rows, :]
    for peer in line:
        arrived(mine_ref.at[1], peer["board_2"], rows, line_ref, line_sem)
    for peer in cross:
        arrived(mine_ref.at[1], peer["board_2"], ends_row, cross_ref, cross_sem)
    total = functools.reduce(jnp.add, [line_ref[k, rows, :] for k in range(ZS)])
    rest = functools.reduce(jnp.add, [cross_ref[k, ends_row, :] for k in range(ZS)])
    hand_ref[rows, :] = total
    hand_ref[lanes // 128 :, :] = jnp.zeros((8 - lanes // 128, 128), F32)
    ends = total[ends_row] + rest
    ratio_ref[...] = ends[:, 126:127] / ends[:, 127:128]
    for copy in sent:
        copy.wait_send()


def write_kernel(*refs):
    count = (len(refs) - 1) // 2
    pieces = []
    for source, target in zip(refs[:count], refs[count:-1]):
        step = max(source.shape[0] // WRITES // 8 * 8, min(source.shape[0], 8))
        for start in range(0, source.shape[0], step):
            pieces.append((source.at[start : start + step, :], target.at[start : start + step, :]))
    copies = [pltpu.make_async_copy(*piece, refs[-1].at[k]) for k, piece in enumerate(pieces)]
    for copy in copies:
        copy.start()
    for copy in copies:
        copy.wait()


def write_out(*arrays):
    return pl.pallas_call(
        write_kernel,
        out_shape=tuple(jax.ShapeDtypeStruct(a.shape, a.dtype) for a in arrays),
        in_specs=[pl.BlockSpec(memory_space=pltpu.VMEM)] * len(arrays),
        out_specs=(pl.BlockSpec(memory_space=pl.ANY),) * len(arrays),
        scratch_shapes=[pltpu.SemaphoreType.DMA((WRITES + len(arrays),))],
        cost_estimate=pl.CostEstimate(flops=10**6, bytes_accessed=10**6, transcendentals=0),
    )(*(pltpu.with_memory_space_constraint(a, pltpu.VMEM) for a in arrays))


def local(opp_reach, hand_rank, hand_cards, pot, bet_frac, trav_reach):
    boards, hand_count = hand_rank.shape
    own_count = opp_reach.shape[1]
    lanes = -(-own_count // 128) * 128
    width = 2 * lanes
    half = boards // 2
    total_boards = boards * lax.axis_size(BOARD)
    whole = pl.BlockSpec(memory_space=pltpu.VMEM)
    board_values, hand_rows, ratio = pl.pallas_call(
        functools.partial(fused_kernel, total_boards, hand_count),
        out_shape=(
            pltpu.VMEM((boards, own_count), F32),
            pltpu.VMEM((8, 128), F32),
            pltpu.VMEM((1, 1), F32),
        ),
        in_specs=[pl.BlockSpec(memory_space=pl.ANY)] * 6,
        out_specs=(whole, whole, whole),
        scratch_shapes=[
            pltpu.VMEM((boards, own_count), BF16),
            pltpu.VMEM((half, hand_count), jnp.int32),
            pltpu.VMEM((2, hand_count), jnp.int32),
            pltpu.VMEM((1, boards), F32),
            pltpu.VMEM((1, boards), F32),
            pltpu.VMEM((own_count,), F32),
            pltpu.SemaphoreType.DMA((6,)),
            pltpu.VMEM((8 * half, width), BF16),
            pltpu.VMEM((CARDS, PARTS, ROWS, width), BF16),
            pltpu.VMEM((CARDS, PARTS, ROWS, 8 * half), F32),
            pltpu.VMEM((CARDS, ROWS, 4 * half), F32),
            pltpu.VMEM((CARDS, ROWS, 4 * half), F32),
            pltpu.VMEM((CARDS, ROWS, 4 * half), F32),
            pltpu.VMEM((2, 2 * half, PARTS * CARDS * ROWS + 128), BF16),
            pltpu.VMEM((3, half, width), F32),
            pltpu.VMEM((half // GROUP, GROUP * HI, width), BF16),
            pltpu.VMEM((half // GROUP, GROUP * SLOT, width), BF16),
            *[pltpu.VMEM((2 * GROUP * HI, 128), F32)] * 4,
            *[pltpu.VMEM((HI // 4, GROUP, 128), F32)] * 4,
            pltpu.VMEM((3, half, lanes), F32),
            pltpu.VMEM((2, width), F32),
            pltpu.VMEM((half, own_count), BF16),
            pltpu.VMEM((2, 8, 128), F32),
            pltpu.VMEM((YS * XS, 8, 128), F32),
            pltpu.VMEM((ZS, 8, 128), F32),
            pltpu.VMEM((ZS, 8, 128), F32),
            pltpu.SemaphoreType.DMA((2,)),
            pltpu.SemaphoreType.DMA((2,)),
            pltpu.SemaphoreType.DMA((2,)),
            pltpu.SemaphoreType.DMA((2, YS * XS)),
            pltpu.SemaphoreType.DMA((2, ZS)),
            pltpu.SemaphoreType.DMA((2, ZS)),
        ],
        compiler_params=pltpu.CompilerParams(
            vmem_limit_bytes=56 * 1024 * 1024, collective_id=0, has_side_effects=True
        ),
        cost_estimate=pl.CostEstimate(flops=10**9, bytes_accessed=10**6, transcendentals=0),
    )(opp_reach, hand_rank, hand_cards.T, pot[None, :], bet_frac[None, :], trav_reach)
    board_values, hand_rows, ratio = write_out(board_values, hand_rows, ratio)
    return board_values, hand_rows.reshape(-1)[:own_count], ratio[0, 0]


def solution(mesh):
    torus = Mesh(
        mesh.devices.reshape(YS, XS, ZS, mesh.shape["hand"]), ("board_0", "board_1", "board_2", "hand")
    )
    placed = (P(BOARD, "hand"), P(BOARD, None), P(), P(BOARD), P(BOARD), P("hand"))
    return jax.shard_map(
        local,
        mesh=torus,
        in_specs=placed,
        out_specs=(P(BOARD, "hand"), P("hand"), P()),
        check_vma=False,
    )
```

```python
import functools

import jax
import jax.numpy as jnp
from jax import lax
from jax.experimental import pallas as pl
from jax.experimental.pallas import tpu as pltpu
from jax.sharding import Mesh
from jax.sharding import PartitionSpec as P

CARDS = 52
BOARD = ("board_0", "board_1", "board_2")
BF16 = jnp.bfloat16
F32 = jnp.float32

PARTS = 4
SHARE = CARDS // PARTS
ROWS = 16
HI, LO = 48, 28
SLOT = 32
GROUP = 8
DBLOCK = 4
YS, XS, ZS = 4, 4, 8
MESH = pl.DeviceIdType.MESH
NT = (((1,), (1,)), ((), ()))


def iota(shape, axis):
    return lax.broadcasted_iota(jnp.int32, shape, axis)


def split2(x):
    high = x.astype(BF16)
    return high, (x - high.astype(F32)).astype(BF16)


def rank_code(rank):
    return (((rank & 127) | 128) << (rank >> 7)).astype(F32).astype(BF16)


def every_peer(places):
    y, x, z, h = places
    plane = [
        {"board_0": lax.rem(y + i, YS), "board_1": lax.rem(x + j, XS)}
        for i in (2, 1, 3, 0)
        for j in (2, 1, 3, 0)
        if i or j
    ]
    line = [{"board_2": lax.rem(z + i, ZS)} for i in (4, 3, 5, 2, 6, 1, 7)]
    cross = [{"board_2": lax.rem(z + i, ZS), "hand": 1 - h} for i in (4, 3, 5, 2, 6, 1, 7, 0)]
    return plane, line, cross


def column(row, start, size):
    n = row.shape[1]
    hit = iota((size, n), 1) == iota((size, n), 0) + start
    return jnp.sum(jnp.where(hit, row, 0.0), axis=1, keepdims=True)


def fused_kernel(
    total_boards, hand_count,
    reach_hbm, rank_hbm, cards_hbm, pot_hbm, bet_hbm, trav_hbm,
    values_ref, hand_ref,
    reach_ref, rank_ref, cards_ref, pot_ref, bet_ref, trav_ref, io_sem,
    x_ref, p_ref, o_ref, w_ref, g_ref, q_ref, l_ref, f_ref, a_ref, b_ref, h0_ref, h1_ref, h2_ref, h3_ref, t0_ref, t1_ref, t2_ref, t3_ref, s_ref, c_ref,
    swap_ref, mine_ref, plane_ref, line_ref, cross_ref,
    swap_sem, pair_sem, sum_sem, plane_sem, line_sem, cross_sem,
):
    all_boards, own_count = reach_ref.shape
    boards = all_boards // 2
    block = 4 * boards
    lanes = x_ref.shape[1] // 2
    width = 2 * lanes
    places = tuple(lax.axis_index(name) for name in BOARD) + (lax.axis_index("hand"),)
    y, x, z, me = places
    plane, line, cross = every_peer(places)
    barrier = pltpu.get_barrier_semaphore()

    def cols_of(half, start=0, size=lanes):
        return pl.ds(pl.multiple_of(half * lanes + start, 128), size)

    def rows_of(core):
        return pl.ds(pl.multiple_of(core * boards, boards), boards)

    def to_partner(source, target, sems):
        copy = pltpu.make_async_remote_copy(
            source, target, sems.at[0], sems.at[1], device_id={"hand": 1 - me}, device_id_type=MESH
        )
        copy.start()
        return copy

    loads = [
        pltpu.make_async_copy(source, target, io_sem.at[k])
        for k, (source, target) in enumerate(
            (
                (cards_hbm, cards_ref),
                (rank_hbm.at[rows_of(me), :], rank_ref),
                (reach_hbm, reach_ref),
                (pot_hbm, pot_ref),
                (bet_hbm, bet_ref),
                (trav_hbm, trav_ref),
            )
        )
    ]
    for load in loads:
        load.start()
    for peer in plane + line + cross:
        pl.semaphore_signal(barrier, inc=1, device_id=peer, device_id_type=MESH)

    loads[0].wait()
    for half in range(2):
        start = half * lanes
        c_ref[:, start + lanes - 128 : start + lanes] = jnp.full((2, 128), -1.0, F32)
        c_ref[:, start : start + own_count] = cards_ref[:, half * own_count : (half + 1) * own_count].astype(F32)

    row16 = iota((16, lanes), 0)
    own_row = [
        jnp.where(row16 < SHARE, row16 + SHARE * q, -5).astype(F32).astype(BF16) for q in range(PARTS)
    ]

    def hot_rows(half, d):
        low, high = c_ref[0:1, cols_of(half)], c_ref[1:2, cols_of(half)]
        partner = jnp.where(low == float(d), high, jnp.where(high == float(d), low, -1.0))
        wide = jnp.broadcast_to(partner, (16, lanes)).astype(BF16)
        for q in range(PARTS):
            p_ref[d, q, :, cols_of(half)] = jnp.where(wide == own_row[q], BF16(1), BF16(0))

    loads[1].wait()
    loads[2].wait()
    for half in range(2):
        start = half * lanes
        f_ref[0:2, :, start + lanes - 128 : start + lanes] = jnp.zeros((2, boards, 128), F32)
        x_ref[:, start + lanes - 128 : start + lanes] = jnp.zeros((8 * boards, 128), BF16)
        rank = rank_ref[:, half * own_count : (half + 1) * own_count]
        x_ref[block : block + boards, start : start + own_count] = rank_code(rank)
        hi = (rank * 2341) >> 16
        f_ref[0, :, start : start + own_count] = hi.astype(F32)
        f_ref[1, :, start : start + own_count] = (rank - LO * hi).astype(F32)
    for k in range(1, PARTS):
        x_ref[block + k * boards : block + (k + 1) * boards, :] = x_ref[block : block + boards, :]

    def place(half, reach):
        x_ref[0:boards, pl.ds(pl.multiple_of(half * lanes, 128), own_count)] = reach
        f_ref[2, :, cols_of(half)] = x_ref[0:boards, cols_of(half)].astype(F32)
        for k in range(1, PARTS):
            x_ref[k * boards : (k + 1) * boards, cols_of(half)] = x_ref[0:boards, cols_of(half)]

    chunk = CARDS // PARTS

    def to_cards(half, more):
        for i in range(PARTS):
            these = slice(chunk * i, chunk * (i + 1))
            if not more:
                for d in range(chunk * i, chunk * (i + 1)):
                    hot_rows(half, d)
            if more:
                high_factor(half, i)
            rows = p_ref[these, :, :, cols_of(half)].reshape(chunk * PARTS * ROWS, lanes)
            got = lax.dot_general(rows, x_ref[:, cols_of(half)], NT, preferred_element_type=F32)
            got = got.reshape(chunk, PARTS, ROWS, 2 * block)
            o_ref[these] = got + o_ref[these] if more else got

    digit = iota((16, lanes), 0).astype(F32).astype(BF16)

    pair = (iota((16, lanes), 0) // GROUP).astype(F32).astype(BF16)

    def high_factor(half, g):
        boards_here = slice(GROUP * g, GROUP * (g + 1))
        hi, reach = (
            jnp.concatenate([f_ref[k, boards_here, cols_of(half)]] * 2, axis=0).astype(BF16) for k in (0, 2)
        )
        for two in range(HI // 2):
            hit = hi == pair + BF16(2 * two)
            a_ref[g, 16 * two : 16 * two + 16, cols_of(half)] = jnp.where(hit, reach, BF16(0))

    def low_factor(half, g):
        for b in range(GROUP):
            at = GROUP * g + b
            lo = jnp.broadcast_to(f_ref[1, at : at + 1, cols_of(half)], (16, lanes)).astype(BF16)
            for part in range(SLOT // 16):
                at = SLOT * b + 16 * part
                b_ref[g, at : at + 16, cols_of(half)] = lax.clamp(
                    BF16(-1), digit + BF16(16 * part) - lo, BF16(1)
                )

    h_refs = (h0_ref, h1_ref, h2_ref, h3_ref)

    def tabulate(g, half=1 - me):
        got = lax.dot_general(
            a_ref[g, :, cols_of(half)], b_ref[g, :, cols_of(half)], NT, preferred_element_type=F32
        )
        for k in range(2):
            rows, piece = slice(GROUP * HI * k, GROUP * HI * (k + 1)), got[:, 128 * k : 128 * (k + 1)]
            h_refs[g][rows, :] = piece if half is me else piece + h_refs[g][rows, :]

    place(me, reach_ref[rows_of(me), :])
    to_cards(me, False)
    loads[3].wait()
    groups = boards // GROUP
    for d in range(CARDS):
        hot_rows(1 - me, d)
    for g in range(groups):
        low_factor(me, g)
        low_factor(1 - me, g)
    pl.semaphore_wait(barrier, len(plane + line + cross))
    swap = to_partner(reach_ref.at[rows_of(1 - me), :], swap_ref, swap_sem)
    for g in range(groups):
        high_factor(me, g)
        tabulate(g, me)
    swap.wait()
    place(1 - me, swap_ref[...])
    to_cards(1 - me, True)

    part_of = iota((ROWS, block), 1) // boards

    def pack(d, carry):
        for ref, at in ((w_ref, 0), (g_ref, block)):
            got = o_ref[d, 0, :, at : at + block]
            for q in range(1, PARTS):
                got = jnp.where(part_of == q, o_ref[d, q, :, at : at + block], got)
            ref[d] = got
        return carry

    lax.fori_loop(0, CARDS, pack, 0, unroll=4)

    def pairs(i, carry):
        mine = [g_ref[DBLOCK * i + k].astype(BF16) for k in range(DBLOCK)]
        sums = [None] * DBLOCK
        for e in range(CARDS):
            ge, we = g_ref[e].astype(BF16), w_ref[e].astype(BF16)
            for k in range(DBLOCK):
                sign = lax.clamp(BF16(-1), mine[k] - ge, BF16(1))
                term = sign.astype(F32) * we.astype(F32)
                sums[k] = term if sums[k] is None else sums[k] + term
        for k in range(DBLOCK):
            q_ref[DBLOCK * i + k] = sums[k]
        return carry

    lax.fori_loop(0, CARDS // DBLOCK, pairs, 0)
    card = iota((64, lanes), 0).astype(F32)
    card_totals = jnp.zeros((boards, 64), F32)
    for half in (1 - me, me):
        hold = ((card == c_ref[0:1, cols_of(half)]) | (card == c_ref[1:2, cols_of(half)])).astype(F32).astype(BF16)
        card_totals = card_totals + lax.dot_general(
            x_ref[0:boards, cols_of(half)], hold, NT, preferred_element_type=F32
        )
    wide = jnp.concatenate([card_totals, jnp.zeros((boards, 64), F32)], axis=1)
    pair_lanes = PARTS * CARDS * ROWS
    turned = jnp.transpose(q_ref[...].reshape(CARDS * ROWS, block))
    for k, piece in enumerate(split2(turned)):
        for q in range(PARTS):
            l_ref[0, boards * k : boards * (k + 1), CARDS * ROWS * q : CARDS * ROWS * (q + 1)] = piece[
                boards * q : boards * (q + 1)
            ]
    for k, piece in enumerate(split2(wide)):
        l_ref[0, boards * k : boards * (k + 1), pair_lanes:] = piece
    pair_copy = to_partner(l_ref.at[0], l_ref.at[1], pair_sem)

    row_slot = iota((GROUP, 128), 0) % 4
    upper = iota((GROUP, 128), 0) < 4
    shift = (iota((GROUP, 128), 1) // SLOT - row_slot) % 4
    tiles = HI // 4
    t_refs = (t0_ref, t1_ref, t2_ref, t3_ref)

    def lay_out(g):
        for t in range(tiles):
            parts = []
            for k in range(4):
                at = GROUP * (4 * t + k)
                parts.append(
                    jnp.where(
                        upper,
                        h_refs[g][at : at + GROUP, :],
                        h_refs[g][GROUP * HI + at : GROUP * HI + at + GROUP, :],
                    )
                )
            row = None
            for k in range(4):
                moved = parts[(3 + k) % 4]
                for p in range(3):
                    moved = jnp.where(row_slot == p, parts[(p + k) % 4], moved)
                row = moved if row is None else jnp.where(shift == k, pltpu.roll(moved, SLOT * k, 1), row)
            t_refs[g][t] = row

    src, dst = iota((256, 128), 0), iota((256, 128), 1)
    within = (dst // SLOT > (src - 128) // SLOT).astype(F32) - (dst // SLOT < (src - 128) // SLOT).astype(F32)
    spread = jnp.where(src % SLOT == LO, jnp.where(src < 128, 1.0, within), 0.0).astype(BF16)
    spot = iota((GROUP, 128), 1) % SLOT == LO

    def add_rows(g):
        run = jnp.zeros((GROUP, 128), F32)
        below, whole = [], []
        for t in range(tiles):
            mark = jnp.where(spot, t_refs[g][t], 0.0)
            whole.append(mark)
            below.append(run)
            run = run + mark
        both = jnp.concatenate(
            [jnp.concatenate([below[t] - (run - below[t] - whole[t]), whole[t]], axis=1) for t in range(tiles)],
            axis=0,
        )
        got = jnp.dot(jnp.concatenate(split2(both), axis=0), spread, preferred_element_type=F32)
        got = got[: GROUP * tiles] + got[GROUP * tiles :]
        for t in range(tiles):
            t_refs[g][t] = t_refs[g][t] + got[GROUP * t : GROUP * (t + 1)]

    def look_up(g, half=1 - me):
        rows = slice(GROUP * g, GROUP * (g + 1))
        for k in range(lanes // 128):
            hi = f_ref[0, rows, cols_of(half, 128 * k, 128)].astype(jnp.int32)
            lo = f_ref[1, rows, cols_of(half, 128 * k, 128)].astype(jnp.int32)
            tile = hi >> 2
            at = ((hi & 3) << 5) + lo
            found = jnp.zeros((GROUP, 128), F32)
            for t in range(tiles):
                got = jnp.take_along_axis(t_refs[g][t], at, axis=1, mode="promise_in_bounds")
                found = jnp.where(tile == t, got, found)
            s_ref[half, rows, 128 * k : 128 * k + 128] = found

    stages = (tabulate, lay_out, add_rows, look_up)
    for step in range(groups + len(stages) - 1):
        for k, stage in enumerate(stages):
            if 0 <= step - k < groups:
                stage(step - k)
    sum_copy = to_partner(s_ref.at[1 - me], s_ref.at[2], sum_sem)

    pair_copy.wait()
    for g in range(groups):
        look_up(g, me)
    back = [p_ref[:, q, :, cols_of(me)].reshape(CARDS * ROWS, lanes) for q in range(PARTS)]
    shared = jnp.dot(
        l_ref[:, :, 0:pair_lanes].reshape(4 * boards, pair_lanes),
        jnp.concatenate(back, axis=0),
        preferred_element_type=F32,
    )
    held = jnp.dot(
        l_ref[:, :, pair_lanes:].reshape(4 * boards, 128)[:, 0:64], hold, preferred_element_type=F32
    )
    sum_copy.wait()
    for load in loads[4:]:
        load.wait()
    part = mass = None
    for k, core in ((0, me), (1, 1 - me)):
        at = 2 * boards * k
        live = (
            0.5 * jnp.sum(l_ref[k, :, pair_lanes:].astype(F32).reshape(2, boards, 128).sum(0), axis=1, keepdims=True)
            - (held[at : at + boards] + held[at + boards : at + 2 * boards])
        )[:, 0:own_count] + reach_ref[rows_of(core), :].astype(F32)
        sums = s_ref[me] if k == 0 else s_ref[2]
        margin = (sums - (shared[at : at + boards] + shared[at + boards : at + 2 * boards]))[:, 0:own_count]
        pot = column(pot_ref[...], core * boards, boards)
        bet = column(bet_ref[...], core * boards, boards)
        half_pot = 0.5 * pot
        half_pot, bet = half_pot / hand_count, bet / hand_count
        stake = half_pot * live
        values = jnp.maximum((half_pot + bet * pot) * margin, -stake)
        values_ref[rows_of(core), :] = values
        values, stake = (jnp.sum(v, axis=0, keepdims=True) for v in (values, stake))
        part = values if part is None else part + values
        mass = stake if mass is None else mass + stake
    part, mass = part / total_boards, mass / total_boards
    trav = trav_ref[...].reshape(1, own_count)
    numerator = jnp.sum(part * trav, axis=1, keepdims=True)
    denominator = jnp.sum(mass * trav, axis=1, keepdims=True)

    spot = XS * y + x
    last = lanes // 128 - 1
    for k in range(last):
        mine_ref[0, k : k + 1, :] = part[:, 128 * k : 128 * (k + 1)]
    fill = jnp.concatenate([part[:, 128 * last :], jnp.zeros((1, lanes - own_count), F32)], axis=1)
    lane = iota((1, 128), 1)
    mine_ref[0, last : last + 1, :] = jnp.where(lane == 126, numerator, jnp.where(lane == 127, denominator, fill))

    rows, ends_row = slice(0, lanes // 128), slice(last, last + 1)

    def exchange(source, groups):
        sent = []
        for peers, here, these, slots, sems in groups:
            for k, peer in enumerate(peers):
                copy = pltpu.make_async_remote_copy(
                    source.at[these, :], slots.at[here, these, :], sems.at[0, k], sems.at[1, here],
                    device_id=peer, device_id_type=MESH,
                )
                copy.start()
                sent.append(copy)
        return sent

    def arrived(source, where, these, slots, sems):
        pltpu.make_async_remote_copy(
            source.at[these, :], slots.at[where, these, :], sems.at[0, 0], sems.at[1, where],
            device_id=plane[0], device_id_type=MESH,
        ).wait_recv()

    sent = exchange(mine_ref.at[0], [(plane, spot, rows, plane_ref, plane_sem)])
    plane_ref[spot, rows, :] = mine_ref[0, rows, :]
    for peer in plane:
        arrived(mine_ref.at[0], XS * peer["board_0"] + peer["board_1"], rows, plane_ref, plane_sem)
    mine_ref[1, rows, :] = functools.reduce(jnp.add, [plane_ref[k, rows, :] for k in range(YS * XS)])
    sent += exchange(
        mine_ref.at[1], [(line, z, rows, line_ref, line_sem), (cross, z, ends_row, cross_ref, cross_sem)]
    )
    line_ref[z, rows, :] = mine_ref[1, rows, :]
    for peer in line:
        arrived(mine_ref.at[1], peer["board_2"], rows, line_ref, line_sem)
    for peer in cross:
        arrived(mine_ref.at[1], peer["board_2"], ends_row, cross_ref, cross_sem)
    total = functools.reduce(jnp.add, [line_ref[k, rows, :] for k in range(ZS)])
    rest = functools.reduce(jnp.add, [cross_ref[k, ends_row, :] for k in range(ZS)])
    hand_ref[rows, :] = total
    ends = total[ends_row] + rest
    hand_ref[lanes // 128 :, :] = jnp.broadcast_to(ends / pltpu.roll(ends, 127, 1), (8 - lanes // 128, 128))
    for copy in sent:
        copy.wait_send()


def write_kernel(values_ref, hand_ref, values_out, hand_out, ratio_out, ratio_ref, sems):
    ratio_ref[...] = hand_ref[7:8, 126:127]
    moves = ((values_ref, values_out), (hand_ref, hand_out), (ratio_ref, ratio_out))
    copies = [pltpu.make_async_copy(source, target, sems.at[k]) for k, (source, target) in enumerate(moves)]
    for copy in copies:
        copy.start()
    for copy in copies:
        copy.wait()


def write_out(*arrays):
    shapes = [a.shape for a in arrays] + [(1, 1)]
    return pl.pallas_call(
        write_kernel,
        out_shape=tuple(jax.ShapeDtypeStruct(shape, F32) for shape in shapes),
        in_specs=[pl.BlockSpec(memory_space=pltpu.VMEM)] * len(arrays),
        out_specs=(pl.BlockSpec(memory_space=pl.ANY),) * len(shapes),
        scratch_shapes=[pltpu.VMEM((1, 1), F32), pltpu.SemaphoreType.DMA((len(shapes),))],
        cost_estimate=pl.CostEstimate(flops=10**6, bytes_accessed=10**6, transcendentals=0),
    )(*(pltpu.with_memory_space_constraint(a, pltpu.VMEM) for a in arrays))


def local(opp_reach, hand_rank, hand_cards, pot, bet_frac, trav_reach):
    boards, hand_count = hand_rank.shape
    own_count = opp_reach.shape[1]
    lanes = -(-own_count // 128) * 128
    width = 2 * lanes
    half = boards // 2
    total_boards = boards * lax.axis_size(BOARD)
    whole = pl.BlockSpec(memory_space=pltpu.VMEM)
    board_values, hand_rows = pl.pallas_call(
        functools.partial(fused_kernel, total_boards, hand_count),
        out_shape=(
            pltpu.VMEM((boards, own_count), F32),
            pltpu.VMEM((8, 128), F32),
        ),
        in_specs=[pl.BlockSpec(memory_space=pl.ANY)] * 6,
        out_specs=(whole, whole),
        scratch_shapes=[
            pltpu.VMEM((boards, own_count), BF16),
            pltpu.VMEM((half, hand_count), jnp.int32),
            pltpu.VMEM((2, hand_count), jnp.int32),
            pltpu.VMEM((1, boards), F32),
            pltpu.VMEM((1, boards), F32),
            pltpu.VMEM((own_count,), F32),
            pltpu.SemaphoreType.DMA((6,)),
            pltpu.VMEM((8 * half, width), BF16),
            pltpu.VMEM((CARDS, PARTS, ROWS, width), BF16),
            pltpu.VMEM((CARDS, PARTS, ROWS, 8 * half), F32),
            pltpu.VMEM((CARDS, ROWS, 4 * half), F32),
            pltpu.VMEM((CARDS, ROWS, 4 * half), F32),
            pltpu.VMEM((CARDS, ROWS, 4 * half), F32),
            pltpu.VMEM((2, 2 * half, PARTS * CARDS * ROWS + 128), BF16),
            pltpu.VMEM((3, half, width), F32),
            pltpu.VMEM((half // GROUP, GROUP * HI, width), BF16),
            pltpu.VMEM((half // GROUP, GROUP * SLOT, width), BF16),
            *[pltpu.VMEM((2 * GROUP * HI, 128), F32)] * 4,
            *[pltpu.VMEM((HI // 4, GROUP, 128), F32)] * 4,
            pltpu.VMEM((3, half, lanes), F32),
            pltpu.VMEM((2, width), F32),
            pltpu.VMEM((half, own_count), BF16),
            pltpu.VMEM((2, 8, 128), F32),
            pltpu.VMEM((YS * XS, 8, 128), F32),
            pltpu.VMEM((ZS, 8, 128), F32),
            pltpu.VMEM((ZS, 8, 128), F32),
            pltpu.SemaphoreType.DMA((2,)),
            pltpu.SemaphoreType.DMA((2,)),
            pltpu.SemaphoreType.DMA((2,)),
            pltpu.SemaphoreType.DMA((2, YS * XS)),
            pltpu.SemaphoreType.DMA((2, ZS)),
            pltpu.SemaphoreType.DMA((2, ZS)),
        ],
        compiler_params=pltpu.CompilerParams(
            vmem_limit_bytes=56 * 1024 * 1024, collective_id=0, has_side_effects=True
        ),
        cost_estimate=pl.CostEstimate(flops=10**9, bytes_accessed=10**6, transcendentals=0),
    )(opp_reach, hand_rank, hand_cards.T, pot[None, :], bet_frac[None, :], trav_reach)
    board_values, hand_rows, ratio = write_out(board_values, hand_rows)
    return board_values, hand_rows.reshape(-1)[:own_count], ratio[0, 0]


def solution(mesh):
    torus = Mesh(
        mesh.devices.reshape(YS, XS, ZS, mesh.shape["hand"]), ("board_0", "board_1", "board_2", "hand")
    )
    placed = (P(BOARD, "hand"), P(BOARD, None), P(), P(BOARD), P(BOARD), P("hand"))
    return jax.shard_map(
        local,
        mesh=torus,
        in_specs=placed,
        out_specs=(P(BOARD, "hand"), P("hand"), P()),
        check_vma=False,
    )
```

```python
import functools

import jax
import jax.numpy as jnp
from jax import lax
from jax.experimental import pallas as pl
from jax.experimental.pallas import tpu as pltpu
from jax.sharding import Mesh
from jax.sharding import PartitionSpec as P

CARDS = 52
BOARD = ("board_0", "board_1", "board_2")
BF16 = jnp.bfloat16
F32 = jnp.float32

PARTS = 4
SHARE = CARDS // PARTS
ROWS = 16
HI, LO = 48, 28
SLOT = 32
GROUP = 8
DBLOCK = 4
YS, XS, ZS = 4, 4, 8
MESH = pl.DeviceIdType.MESH
NT = (((1,), (1,)), ((), ()))


def iota(shape, axis):
    return lax.broadcasted_iota(jnp.int32, shape, axis)


def split2(x):
    high = x.astype(BF16)
    return high, (x - high.astype(F32)).astype(BF16)


def rank_code(rank):
    return (((rank & 127) | 128) << (rank >> 7)).astype(F32).astype(BF16)


def every_peer(places):
    y, x, z, h = places
    plane = [
        {"board_0": lax.rem(y + i, YS), "board_1": lax.rem(x + j, XS)}
        for i in (2, 1, 3, 0)
        for j in (2, 1, 3, 0)
        if i or j
    ]
    line = [{"board_2": lax.rem(z + i, ZS)} for i in (4, 3, 5, 2, 6, 1, 7)]
    cross = [{"board_2": lax.rem(z + i, ZS), "hand": 1 - h} for i in (4, 3, 5, 2, 6, 1, 7, 0)]
    return plane, line, cross


def column(row, start, size):
    n = row.shape[1]
    hit = iota((size, n), 1) == iota((size, n), 0) + start
    return jnp.sum(jnp.where(hit, row, 0.0), axis=1, keepdims=True)


def fused_kernel(
    total_boards, hand_count,
    reach_hbm, rank_hbm, cards_hbm, pot_hbm, bet_hbm, trav_hbm,
    values_ref, hand_ref,
    reach_ref, rank_ref, cards_ref, pot_ref, bet_ref, trav_ref, io_sem,
    x_ref, p_ref, o_ref, w_ref, g_ref, q_ref, l_ref, f_ref, a_ref, b_ref, h0_ref, h1_ref, h2_ref, h3_ref, t0_ref, t1_ref, t2_ref, t3_ref, s_ref, c_ref,
    swap_ref, mine_ref, plane_ref, line_ref, cross_ref,
    swap_sem, pair_sem, sum_sem, plane_sem, line_sem, cross_sem,
):
    all_boards, own_count = reach_ref.shape
    boards = all_boards // 2
    block = 4 * boards
    lanes = x_ref.shape[1] // 2
    width = 2 * lanes
    places = tuple(lax.axis_index(name) for name in BOARD) + (lax.axis_index("hand"),)
    y, x, z, me = places
    plane, line, cross = every_peer(places)
    barrier = pltpu.get_barrier_semaphore()

    def cols_of(half, start=0, size=lanes):
        return pl.ds(pl.multiple_of(half * lanes + start, 128), size)

    def rows_of(core):
        return pl.ds(pl.multiple_of(core * boards, boards), boards)

    def to_partner(source, target, sems):
        copy = pltpu.make_async_remote_copy(
            source, target, sems.at[0], sems.at[1], device_id={"hand": 1 - me}, device_id_type=MESH
        )
        copy.start()
        return copy

    loads = [
        pltpu.make_async_copy(source, target, io_sem.at[k])
        for k, (source, target) in enumerate(
            (
                (cards_hbm, cards_ref),
                (rank_hbm.at[rows_of(me), :], rank_ref),
                (reach_hbm, reach_ref),
                (pot_hbm, pot_ref),
                (bet_hbm, bet_ref),
                (trav_hbm, trav_ref),
            )
        )
    ]
    for load in loads:
        load.start()
    for peer in plane + line + cross:
        pl.semaphore_signal(barrier, inc=1, device_id=peer, device_id_type=MESH)

    loads[0].wait()
    for half in range(2):
        start = half * lanes
        c_ref[:, start + lanes - 128 : start + lanes] = jnp.full((2, 128), -1.0, F32)
        c_ref[:, start : start + own_count] = cards_ref[:, half * own_count : (half + 1) * own_count].astype(F32)

    row16 = iota((16, lanes), 0)
    own_row = [
        jnp.where(row16 < SHARE, row16 + SHARE * q, -5).astype(F32).astype(BF16) for q in range(PARTS)
    ]

    def hot_rows(half, d):
        low, high = c_ref[0:1, cols_of(half)], c_ref[1:2, cols_of(half)]
        partner = jnp.where(low == float(d), high, jnp.where(high == float(d), low, -1.0))
        wide = jnp.broadcast_to(partner, (16, lanes)).astype(BF16)
        for q in range(PARTS):
            p_ref[d, q, :, cols_of(half)] = jnp.where(wide == own_row[q], BF16(1), BF16(0))

    loads[1].wait()
    loads[2].wait()
    for half in range(2):
        start = half * lanes
        f_ref[0:2, :, start + lanes - 128 : start + lanes] = jnp.zeros((2, boards, 128), F32)
        x_ref[:, start + lanes - 128 : start + lanes] = jnp.zeros((8 * boards, 128), BF16)
        rank = rank_ref[:, half * own_count : (half + 1) * own_count]
        x_ref[block : block + boards, start : start + own_count] = rank_code(rank)
        hi = (rank * 2341) >> 16
        f_ref[0, :, start : start + own_count] = hi.astype(F32)
        f_ref[1, :, start : start + own_count] = (rank - LO * hi).astype(F32)
    for k in range(1, PARTS):
        x_ref[block + k * boards : block + (k + 1) * boards, :] = x_ref[block : block + boards, :]

    def place(half, reach):
        x_ref[0:boards, pl.ds(pl.multiple_of(half * lanes, 128), own_count)] = reach
        f_ref[2, :, cols_of(half)] = x_ref[0:boards, cols_of(half)].astype(F32)
        for k in range(1, PARTS):
            x_ref[k * boards : (k + 1) * boards, cols_of(half)] = x_ref[0:boards, cols_of(half)]

    chunk = CARDS // PARTS

    def to_cards(half, more):
        for i in range(PARTS):
            these = slice(chunk * i, chunk * (i + 1))
            if not more:
                for d in range(chunk * i, chunk * (i + 1)):
                    hot_rows(half, d)
            if more:
                high_factor(half, i)
            rows = p_ref[these, :, :, cols_of(half)].reshape(chunk * PARTS * ROWS, lanes)
            got = lax.dot_general(rows, x_ref[:, cols_of(half)], NT, preferred_element_type=F32)
            got = got.reshape(chunk, PARTS, ROWS, 2 * block)
            o_ref[these] = got + o_ref[these] if more else got

    digit = iota((16, lanes), 0).astype(F32).astype(BF16)

    pair = (iota((16, lanes), 0) // GROUP).astype(F32).astype(BF16)

    def high_factor(half, g):
        boards_here = slice(GROUP * g, GROUP * (g + 1))
        hi, reach = (
            jnp.concatenate([f_ref[k, boards_here, cols_of(half)]] * 2, axis=0).astype(BF16) for k in (0, 2)
        )
        for two in range(HI // 2):
            hit = hi == pair + BF16(2 * two)
            a_ref[g, 16 * two : 16 * two + 16, cols_of(half)] = jnp.where(hit, reach, BF16(0))

    def low_factor(half, g):
        for b in range(GROUP):
            at = GROUP * g + b
            lo = jnp.broadcast_to(f_ref[1, at : at + 1, cols_of(half)], (16, lanes)).astype(BF16)
            for part in range(SLOT // 16):
                at = SLOT * b + 16 * part
                b_ref[g, at : at + 16, cols_of(half)] = lax.clamp(
                    BF16(-1), digit + BF16(16 * part) - lo, BF16(1)
                )

    h_refs = (h0_ref, h1_ref, h2_ref, h3_ref)

    def tabulate(g, half=1 - me):
        got = lax.dot_general(
            a_ref[g, :, cols_of(half)], b_ref[g, :, cols_of(half)], NT, preferred_element_type=F32
        )
        for k in range(2):
            rows, piece = slice(GROUP * HI * k, GROUP * HI * (k + 1)), got[:, 128 * k : 128 * (k + 1)]
            h_refs[g][rows, :] = piece if half is me else piece + h_refs[g][rows, :]

    place(me, reach_ref[rows_of(me), :])
    to_cards(me, False)
    loads[3].wait()
    groups = boards // GROUP
    for d in range(CARDS):
        hot_rows(1 - me, d)
    for g in range(groups):
        low_factor(me, g)
        low_factor(1 - me, g)
    pl.semaphore_wait(barrier, len(plane + line + cross))
    swap = to_partner(reach_ref.at[rows_of(1 - me), :], swap_ref, swap_sem)
    for g in range(groups):
        high_factor(me, g)
        tabulate(g, me)
    swap.wait()
    place(1 - me, swap_ref[...])
    to_cards(1 - me, True)

    part_of = iota((ROWS, block), 1) // boards

    def pack(d, carry):
        for ref, at in ((w_ref, 0), (g_ref, block)):
            got = o_ref[d, 0, :, at : at + block]
            for q in range(1, PARTS):
                got = jnp.where(part_of == q, o_ref[d, q, :, at : at + block], got)
            ref[d] = got
        return carry

    lax.fori_loop(0, CARDS, pack, 0, unroll=4)

    def pairs(i, carry):
        mine = [g_ref[DBLOCK * i + k].astype(BF16) for k in range(DBLOCK)]
        sums = [None] * DBLOCK
        for e in range(CARDS):
            ge, we = g_ref[e].astype(BF16), w_ref[e].astype(BF16)
            for k in range(DBLOCK):
                sign = lax.clamp(BF16(-1), mine[k] - ge, BF16(1))
                term = sign.astype(F32) * we.astype(F32)
                sums[k] = term if sums[k] is None else sums[k] + term
        for k in range(DBLOCK):
            q_ref[DBLOCK * i + k] = sums[k]
        return carry

    lax.fori_loop(0, CARDS // DBLOCK, pairs, 0)
    card = iota((64, lanes), 0).astype(F32)
    card_totals = jnp.zeros((boards, 64), F32)
    for half in (1 - me, me):
        hold = ((card == c_ref[0:1, cols_of(half)]) | (card == c_ref[1:2, cols_of(half)])).astype(F32).astype(BF16)
        card_totals = card_totals + lax.dot_general(
            x_ref[0:boards, cols_of(half)], hold, NT, preferred_element_type=F32
        )
    wide = jnp.concatenate([card_totals, jnp.zeros((boards, 64), F32)], axis=1)
    pair_lanes = PARTS * CARDS * ROWS
    turned = jnp.transpose(q_ref[...].reshape(CARDS * ROWS, block))
    for k, piece in enumerate(split2(turned)):
        for q in range(PARTS):
            l_ref[0, boards * k : boards * (k + 1), CARDS * ROWS * q : CARDS * ROWS * (q + 1)] = piece[
                boards * q : boards * (q + 1)
            ]
    for k, piece in enumerate(split2(wide)):
        l_ref[0, boards * k : boards * (k + 1), pair_lanes:] = piece
    pair_copy = to_partner(l_ref.at[0], l_ref.at[1], pair_sem)

    row_slot = iota((GROUP, 128), 0) % 4
    upper = iota((GROUP, 128), 0) < 4
    shift = (iota((GROUP, 128), 1) // SLOT - row_slot) % 4
    tiles = HI // 4
    t_refs = (t0_ref, t1_ref, t2_ref, t3_ref)

    def lay_out(g):
        for t in range(tiles):
            parts = []
            for k in range(4):
                at = GROUP * (4 * t + k)
                parts.append(
                    jnp.where(
                        upper,
                        h_refs[g][at : at + GROUP, :],
                        h_refs[g][GROUP * HI + at : GROUP * HI + at + GROUP, :],
                    )
                )
            row = None
            for k in range(4):
                moved = parts[(3 + k) % 4]
                for p in range(3):
                    moved = jnp.where(row_slot == p, parts[(p + k) % 4], moved)
                row = moved if row is None else jnp.where(shift == k, pltpu.roll(moved, SLOT * k, 1), row)
            t_refs[g][t] = row

    src, dst = iota((256, 128), 0), iota((256, 128), 1)
    within = (dst // SLOT > (src - 128) // SLOT).astype(F32) - (dst // SLOT < (src - 128) // SLOT).astype(F32)
    spread = jnp.where(src % SLOT == LO, jnp.where(src < 128, 1.0, within), 0.0).astype(BF16)
    spot = iota((GROUP, 128), 1) % SLOT == LO

    def add_rows(g):
        run = jnp.zeros((GROUP, 128), F32)
        below, whole = [], []
        for t in range(tiles):
            mark = jnp.where(spot, t_refs[g][t], 0.0)
            whole.append(mark)
            below.append(run)
            run = run + mark
        both = jnp.concatenate(
            [jnp.concatenate([below[t] - (run - below[t] - whole[t]), whole[t]], axis=1) for t in range(tiles)],
            axis=0,
        )
        got = jnp.dot(jnp.concatenate(split2(both), axis=0), spread, preferred_element_type=F32)
        got = got[: GROUP * tiles] + got[GROUP * tiles :]
        for t in range(tiles):
            t_refs[g][t] = t_refs[g][t] + got[GROUP * t : GROUP * (t + 1)]

    def look_up(g, half=1 - me):
        rows = slice(GROUP * g, GROUP * (g + 1))
        for k in range(lanes // 128):
            hi = f_ref[0, rows, cols_of(half, 128 * k, 128)].astype(jnp.int32)
            lo = f_ref[1, rows, cols_of(half, 128 * k, 128)].astype(jnp.int32)
            tile = hi >> 2
            at = ((hi & 3) << 5) + lo
            found = jnp.zeros((GROUP, 128), F32)
            for t in range(tiles):
                got = jnp.take_along_axis(t_refs[g][t], at, axis=1, mode="promise_in_bounds")
                found = jnp.where(tile == t, got, found)
            s_ref[half, rows, 128 * k : 128 * k + 128] = found

    stages = (tabulate, lay_out, add_rows, look_up)
    for step in range(groups + len(stages) - 1):
        for k, stage in enumerate(stages):
            if 0 <= step - k < groups:
                stage(step - k)
    sum_copy = to_partner(s_ref.at[1 - me], s_ref.at[2], sum_sem)

    pair_copy.wait()
    for load in loads[4:]:
        load.wait()
    for g in range(groups):
        look_up(g, me)
    back = [p_ref[:, q, :, cols_of(me)].reshape(CARDS * ROWS, lanes) for q in range(PARTS)]
    shared = jnp.dot(
        l_ref[:, :, 0:pair_lanes].reshape(4 * boards, pair_lanes),
        jnp.concatenate(back, axis=0),
        preferred_element_type=F32,
    )
    held = jnp.dot(
        l_ref[:, :, pair_lanes:].reshape(4 * boards, 128)[:, 0:64], hold, preferred_element_type=F32
    )
    trav = trav_ref[...].reshape(1, own_count)

    def ready(k, core):
        at = 2 * boards * k
        live = (
            0.5 * jnp.sum(l_ref[k, :, pair_lanes:].astype(F32).reshape(2, boards, 128).sum(0), axis=1, keepdims=True)
            - (held[at : at + boards] + held[at + boards : at + 2 * boards])
        )[:, 0:own_count] + reach_ref[rows_of(core), :].astype(F32)
        pot = column(pot_ref[...], core * boards, boards)
        bet = column(bet_ref[...], core * boards, boards) / hand_count
        half_pot = 0.5 * pot / hand_count
        return half_pot + bet * pot, shared[at : at + boards] + shared[at + boards : at + 2 * boards], half_pot * live

    def settle(core, sums, rate, taken, stake):
        values = jnp.maximum(rate * (sums - taken)[:, 0:own_count], -stake)
        values_ref[rows_of(core), :] = values
        return jnp.sum(values, axis=0, keepdims=True)

    here, there = ready(0, me), ready(1, 1 - me)
    mass = (jnp.sum(here[2], axis=0, keepdims=True) + jnp.sum(there[2], axis=0, keepdims=True)) / total_boards
    denominator = jnp.sum(mass * trav, axis=1, keepdims=True)
    part = settle(me, s_ref[me], *here)
    sum_copy.wait()
    part = (part + settle(1 - me, s_ref[2], *there)) / total_boards
    numerator = jnp.sum(part * trav, axis=1, keepdims=True)

    spot = XS * y + x
    last = lanes // 128 - 1
    for k in range(last):
        mine_ref[0, k : k + 1, :] = part[:, 128 * k : 128 * (k + 1)]
    fill = jnp.concatenate([part[:, 128 * last :], jnp.zeros((1, lanes - own_count), F32)], axis=1)
    lane = iota((1, 128), 1)
    mine_ref[0, last : last + 1, :] = jnp.where(lane == 126, numerator, jnp.where(lane == 127, denominator, fill))

    rows, ends_row = slice(0, lanes // 128), slice(last, last + 1)

    def exchange(source, groups):
        sent = []
        for peers, here, these, slots, sems in groups:
            for k, peer in enumerate(peers):
                copy = pltpu.make_async_remote_copy(
                    source.at[these, :], slots.at[here, these, :], sems.at[0, k], sems.at[1, here],
                    device_id=peer, device_id_type=MESH,
                )
                copy.start()
                sent.append(copy)
        return sent

    def arrived(source, where, these, slots, sems):
        pltpu.make_async_remote_copy(
            source.at[these, :], slots.at[where, these, :], sems.at[0, 0], sems.at[1, where],
            device_id=plane[0], device_id_type=MESH,
        ).wait_recv()

    sent = exchange(mine_ref.at[0], [(plane, spot, rows, plane_ref, plane_sem)])
    plane_ref[spot, rows, :] = mine_ref[0, rows, :]
    for peer in plane:
        arrived(mine_ref.at[0], XS * peer["board_0"] + peer["board_1"], rows, plane_ref, plane_sem)
    mine_ref[1, rows, :] = functools.reduce(jnp.add, [plane_ref[k, rows, :] for k in range(YS * XS)])
    sent += exchange(
        mine_ref.at[1], [(line, z, rows, line_ref, line_sem), (cross, z, ends_row, cross_ref, cross_sem)]
    )
    line_ref[z, rows, :] = mine_ref[1, rows, :]
    for peer in line:
        arrived(mine_ref.at[1], peer["board_2"], rows, line_ref, line_sem)
    for peer in cross:
        arrived(mine_ref.at[1], peer["board_2"], ends_row, cross_ref, cross_sem)
    total = functools.reduce(jnp.add, [line_ref[k, rows, :] for k in range(ZS)])
    rest = functools.reduce(jnp.add, [cross_ref[k, ends_row, :] for k in range(ZS)])
    hand_ref[rows, :] = total
    ends = total[ends_row] + rest
    hand_ref[lanes // 128 :, :] = jnp.broadcast_to(ends / pltpu.roll(ends, 127, 1), (8 - lanes // 128, 128))
    for copy in sent:
        copy.wait_send()


def write_kernel(values_ref, hand_ref, values_out, hand_out, ratio_out, ratio_ref, sems):
    ratio_ref[...] = hand_ref[7:8, 126:127]
    moves = ((values_ref, values_out), (hand_ref, hand_out), (ratio_ref, ratio_out))
    copies = [pltpu.make_async_copy(source, target, sems.at[k]) for k, (source, target) in enumerate(moves)]
    for copy in copies:
        copy.start()
    for copy in copies:
        copy.wait()


def write_out(*arrays):
    shapes = [a.shape for a in arrays] + [(1, 1)]
    return pl.pallas_call(
        write_kernel,
        out_shape=tuple(jax.ShapeDtypeStruct(shape, F32) for shape in shapes),
        in_specs=[pl.BlockSpec(memory_space=pltpu.VMEM)] * len(arrays),
        out_specs=(pl.BlockSpec(memory_space=pl.ANY),) * len(shapes),
        scratch_shapes=[pltpu.VMEM((1, 1), F32), pltpu.SemaphoreType.DMA((len(shapes),))],
        cost_estimate=pl.CostEstimate(flops=10**6, bytes_accessed=10**6, transcendentals=0),
    )(*(pltpu.with_memory_space_constraint(a, pltpu.VMEM) for a in arrays))


def local(opp_reach, hand_rank, hand_cards, pot, bet_frac, trav_reach):
    boards, hand_count = hand_rank.shape
    own_count = opp_reach.shape[1]
    lanes = -(-own_count // 128) * 128
    width = 2 * lanes
    half = boards // 2
    total_boards = boards * lax.axis_size(BOARD)
    whole = pl.BlockSpec(memory_space=pltpu.VMEM)
    board_values, hand_rows = pl.pallas_call(
        functools.partial(fused_kernel, total_boards, hand_count),
        out_shape=(
            pltpu.VMEM((boards, own_count), F32),
            pltpu.VMEM((8, 128), F32),
        ),
        in_specs=[pl.BlockSpec(memory_space=pl.ANY)] * 6,
        out_specs=(whole, whole),
        scratch_shapes=[
            pltpu.VMEM((boards, own_count), BF16),
            pltpu.VMEM((half, hand_count), jnp.int32),
            pltpu.VMEM((2, hand_count), jnp.int32),
            pltpu.VMEM((1, boards), F32),
            pltpu.VMEM((1, boards), F32),
            pltpu.VMEM((own_count,), F32),
            pltpu.SemaphoreType.DMA((6,)),
            pltpu.VMEM((8 * half, width), BF16),
            pltpu.VMEM((CARDS, PARTS, ROWS, width), BF16),
            pltpu.VMEM((CARDS, PARTS, ROWS, 8 * half), F32),
            pltpu.VMEM((CARDS, ROWS, 4 * half), F32),
            pltpu.VMEM((CARDS, ROWS, 4 * half), F32),
            pltpu.VMEM((CARDS, ROWS, 4 * half), F32),
            pltpu.VMEM((2, 2 * half, PARTS * CARDS * ROWS + 128), BF16),
            pltpu.VMEM((3, half, width), F32),
            pltpu.VMEM((half // GROUP, GROUP * HI, width), BF16),
            pltpu.VMEM((half // GROUP, GROUP * SLOT, width), BF16),
            *[pltpu.VMEM((2 * GROUP * HI, 128), F32)] * 4,
            *[pltpu.VMEM((HI // 4, GROUP, 128), F32)] * 4,
            pltpu.VMEM((3, half, lanes), F32),
            pltpu.VMEM((2, width), F32),
            pltpu.VMEM((half, own_count), BF16),
            pltpu.VMEM((2, 8, 128), F32),
            pltpu.VMEM((YS * XS, 8, 128), F32),
            pltpu.VMEM((ZS, 8, 128), F32),
            pltpu.VMEM((ZS, 8, 128), F32),
            pltpu.SemaphoreType.DMA((2,)),
            pltpu.SemaphoreType.DMA((2,)),
            pltpu.SemaphoreType.DMA((2,)),
            pltpu.SemaphoreType.DMA((2, YS * XS)),
            pltpu.SemaphoreType.DMA((2, ZS)),
            pltpu.SemaphoreType.DMA((2, ZS)),
        ],
        compiler_params=pltpu.CompilerParams(
            vmem_limit_bytes=56 * 1024 * 1024, collective_id=0, has_side_effects=True
        ),
        cost_estimate=pl.CostEstimate(flops=10**9, bytes_accessed=10**6, transcendentals=0),
    )(opp_reach, hand_rank, hand_cards.T, pot[None, :], bet_frac[None, :], trav_reach)
    board_values, hand_rows, ratio = write_out(board_values, hand_rows)
    return board_values, hand_rows.reshape(-1)[:own_count], ratio[0, 0]


def solution(mesh):
    torus = Mesh(
        mesh.devices.reshape(YS, XS, ZS, mesh.shape["hand"]), ("board_0", "board_1", "board_2", "hand")
    )
    placed = (P(BOARD, "hand"), P(BOARD, None), P(), P(BOARD), P(BOARD), P("hand"))
    return jax.shard_map(
        local,
        mesh=torus,
        in_specs=placed,
        out_specs=(P(BOARD, "hand"), P("hand"), P()),
        check_vma=False,
    )
```

```python
import functools

import jax
import jax.numpy as jnp
from jax import lax
from jax.experimental import pallas as pl
from jax.experimental.pallas import tpu as pltpu
from jax.sharding import Mesh
from jax.sharding import PartitionSpec as P

CARDS = 52
BOARD = ("board_0", "board_1", "board_2")
BF16 = jnp.bfloat16
F32 = jnp.float32

PARTS = 4
SHARE = CARDS // PARTS
ROWS = 16
HI, LO = 48, 28
SLOT = 32
GROUP = 8
DBLOCK = 4
YS, XS, ZS = 4, 4, 8
MESH = pl.DeviceIdType.MESH
NT = (((1,), (1,)), ((), ()))


def iota(shape, axis):
    return lax.broadcasted_iota(jnp.int32, shape, axis)


def split2(x):
    high = x.astype(BF16)
    return high, (x - high.astype(F32)).astype(BF16)


def rank_code(rank):
    return (((rank & 127) | 128) << (rank >> 7)).astype(F32).astype(BF16)


def every_peer(places):
    y, x, z, h = places
    plane = [
        {"board_0": lax.rem(y + i, YS), "board_1": lax.rem(x + j, XS)}
        for i in (2, 1, 3, 0)
        for j in (2, 1, 3, 0)
        if i or j
    ]
    line = [{"board_2": lax.rem(z + i, ZS)} for i in (4, 3, 5, 2, 6, 1, 7)]
    cross = [{"board_2": lax.rem(z + i, ZS), "hand": 1 - h} for i in (4, 3, 5, 2, 6, 1, 7, 0)]
    return plane, line, cross


def column(row, start, size):
    n = row.shape[1]
    hit = iota((size, n), 1) == iota((size, n), 0) + start
    return jnp.sum(jnp.where(hit, row, 0.0), axis=1, keepdims=True)


def fused_kernel(
    total_boards, hand_count,
    reach_hbm, rank_hbm, cards_hbm, pot_hbm, bet_hbm, trav_hbm,
    values_ref, hand_ref,
    reach_ref, rank_ref, cards_ref, pot_ref, bet_ref, trav_ref, io_sem,
    x_ref, p_ref, o_ref, w_ref, g_ref, q_ref, l_ref, f_ref, a_ref, b_ref, h0_ref, h1_ref, h2_ref, h3_ref, t0_ref, t1_ref, t2_ref, t3_ref, s_ref, c_ref,
    swap_ref, mine_ref, plane_ref, line_ref, cross_ref,
    swap_sem, pair_sem, sum_sem, plane_sem, line_sem, cross_sem,
):
    all_boards, own_count = reach_ref.shape
    boards = all_boards // 2
    block = 4 * boards
    lanes = x_ref.shape[1] // 2
    width = 2 * lanes
    places = tuple(lax.axis_index(name) for name in BOARD) + (lax.axis_index("hand"),)
    y, x, z, me = places
    plane, line, cross = every_peer(places)
    barrier = pltpu.get_barrier_semaphore()

    def cols_of(half, start=0, size=lanes):
        return pl.ds(pl.multiple_of(half * lanes + start, 128), size)

    def rows_of(core):
        return pl.ds(pl.multiple_of(core * boards, boards), boards)

    def to_partner(source, target, sems):
        copy = pltpu.make_async_remote_copy(
            source, target, sems.at[0], sems.at[1], device_id={"hand": 1 - me}, device_id_type=MESH
        )
        copy.start()
        return copy

    loads = [
        pltpu.make_async_copy(source, target, io_sem.at[k])
        for k, (source, target) in enumerate(
            (
                (cards_hbm, cards_ref),
                (rank_hbm.at[rows_of(me), :], rank_ref),
                (reach_hbm, reach_ref),
                (pot_hbm, pot_ref),
                (bet_hbm, bet_ref),
                (trav_hbm, trav_ref),
            )
        )
    ]
    for load in loads:
        load.start()
    for peer in plane + line + cross:
        pl.semaphore_signal(barrier, inc=1, device_id=peer, device_id_type=MESH)

    loads[0].wait()
    for half in range(2):
        start = half * lanes
        c_ref[:, start + lanes - 128 : start + lanes] = jnp.full((2, 128), -1.0, F32)
        c_ref[:, start : start + own_count] = cards_ref[:, half * own_count : (half + 1) * own_count].astype(F32)

    row16 = iota((16, lanes), 0)
    own_row = [
        jnp.where(row16 < SHARE, row16 + SHARE * q, -5).astype(F32).astype(BF16) for q in range(PARTS)
    ]

    def hot_rows(half, d):
        low, high = c_ref[0:1, cols_of(half)], c_ref[1:2, cols_of(half)]
        partner = jnp.where(low == float(d), high, jnp.where(high == float(d), low, -1.0))
        wide = jnp.broadcast_to(partner, (16, lanes)).astype(BF16)
        for q in range(PARTS):
            p_ref[d, q, :, cols_of(half)] = jnp.where(wide == own_row[q], BF16(1), BF16(0))

    loads[1].wait()
    loads[2].wait()
    for half in range(2):
        start = half * lanes
        f_ref[0:2, :, start + lanes - 128 : start + lanes] = jnp.zeros((2, boards, 128), F32)
        x_ref[:, start + lanes - 128 : start + lanes] = jnp.zeros((8 * boards, 128), BF16)
        rank = rank_ref[:, half * own_count : (half + 1) * own_count]
        x_ref[block : block + boards, start : start + own_count] = rank_code(rank)
        hi = (rank * 2341) >> 16
        f_ref[0, :, start : start + own_count] = hi.astype(F32)
        f_ref[1, :, start : start + own_count] = (rank - LO * hi).astype(F32)
    for k in range(1, PARTS):
        x_ref[block + k * boards : block + (k + 1) * boards, :] = x_ref[block : block + boards, :]

    def place(half, reach):
        x_ref[0:boards, pl.ds(pl.multiple_of(half * lanes, 128), own_count)] = reach
        f_ref[2, :, cols_of(half)] = x_ref[0:boards, cols_of(half)].astype(F32)
        for k in range(1, PARTS):
            x_ref[k * boards : (k + 1) * boards, cols_of(half)] = x_ref[0:boards, cols_of(half)]

    chunk = CARDS // PARTS

    def to_cards(half, more):
        for i in range(PARTS):
            these = slice(chunk * i, chunk * (i + 1))
            if not more:
                for d in range(chunk * i, chunk * (i + 1)):
                    hot_rows(half, d)
            if more:
                high_factor(half, i)
            rows = p_ref[these, :, :, cols_of(half)].reshape(chunk * PARTS * ROWS, lanes)
            got = lax.dot_general(rows, x_ref[:, cols_of(half)], NT, preferred_element_type=F32)
            got = got.reshape(chunk, PARTS, ROWS, 2 * block)
            o_ref[these] = got + o_ref[these] if more else got

    digit = iota((16, lanes), 0).astype(F32).astype(BF16)

    pair = (iota((16, lanes), 0) // GROUP).astype(F32).astype(BF16)

    def high_factor(half, g):
        boards_here = slice(GROUP * g, GROUP * (g + 1))
        hi, reach = (
            jnp.concatenate([f_ref[k, boards_here, cols_of(half)]] * 2, axis=0).astype(BF16) for k in (0, 2)
        )
        for two in range(HI // 2):
            hit = hi == pair + BF16(2 * two)
            a_ref[g, 16 * two : 16 * two + 16, cols_of(half)] = jnp.where(hit, reach, BF16(0))

    def low_factor(half, g):
        for b in range(GROUP):
            at = GROUP * g + b
            lo = jnp.broadcast_to(f_ref[1, at : at + 1, cols_of(half)], (16, lanes)).astype(BF16)
            for part in range(SLOT // 16):
                at = SLOT * b + 16 * part
                b_ref[g, at : at + 16, cols_of(half)] = lax.clamp(
                    BF16(-1), digit + BF16(16 * part) - lo, BF16(1)
                )

    h_refs = (h0_ref, h1_ref, h2_ref, h3_ref)

    def tabulate(g, half=1 - me):
        got = lax.dot_general(
            a_ref[g, :, cols_of(half)], b_ref[g, :, cols_of(half)], NT, preferred_element_type=F32
        )
        for k in range(2):
            rows, piece = slice(GROUP * HI * k, GROUP * HI * (k + 1)), got[:, 128 * k : 128 * (k + 1)]
            h_refs[g][rows, :] = piece if half is me else piece + h_refs[g][rows, :]

    place(me, reach_ref[rows_of(me), :])
    to_cards(me, False)
    loads[3].wait()
    groups = boards // GROUP
    for d in range(CARDS):
        hot_rows(1 - me, d)
    for g in range(groups):
        low_factor(me, g)
        low_factor(1 - me, g)
    pl.semaphore_wait(barrier, len(plane + line + cross))
    swap = to_partner(reach_ref.at[rows_of(1 - me), :], swap_ref, swap_sem)
    for g in range(groups):
        high_factor(me, g)
        tabulate(g, me)
    swap.wait()
    place(1 - me, swap_ref[...])
    to_cards(1 - me, True)

    part_of = iota((ROWS, block), 1) // boards

    def pack(d, carry):
        for ref, at in ((w_ref, 0), (g_ref, block)):
            got = o_ref[d, 0, :, at : at + block]
            for q in range(1, PARTS):
                got = jnp.where(part_of == q, o_ref[d, q, :, at : at + block], got)
            ref[d] = got
        return carry

    lax.fori_loop(0, CARDS, pack, 0, unroll=4)

    def pairs(i, carry):
        mine = [g_ref[DBLOCK * i + k].astype(BF16) for k in range(DBLOCK)]
        sums = [None] * DBLOCK
        for e in range(CARDS):
            ge, we = g_ref[e].astype(BF16), w_ref[e].astype(BF16)
            for k in range(DBLOCK):
                sign = lax.clamp(BF16(-1), mine[k] - ge, BF16(1))
                term = sign.astype(F32) * we.astype(F32)
                sums[k] = term if sums[k] is None else sums[k] + term
        for k in range(DBLOCK):
            q_ref[DBLOCK * i + k] = sums[k]
        return carry

    lax.fori_loop(0, CARDS // DBLOCK, pairs, 0)
    card = iota((64, lanes), 0).astype(F32)
    card_totals = jnp.zeros((boards, 64), F32)
    for half in (1 - me, me):
        hold = ((card == c_ref[0:1, cols_of(half)]) | (card == c_ref[1:2, cols_of(half)])).astype(F32).astype(BF16)
        card_totals = card_totals + lax.dot_general(
            x_ref[0:boards, cols_of(half)], hold, NT, preferred_element_type=F32
        )
    wide = jnp.concatenate([card_totals, jnp.zeros((boards, 64), F32)], axis=1)
    pair_lanes = PARTS * CARDS * ROWS
    turned = jnp.transpose(q_ref[...].reshape(CARDS * ROWS, block))
    for k, piece in enumerate(split2(turned)):
        for q in range(PARTS):
            l_ref[0, boards * k : boards * (k + 1), CARDS * ROWS * q : CARDS * ROWS * (q + 1)] = piece[
                boards * q : boards * (q + 1)
            ]
    for k, piece in enumerate(split2(wide)):
        l_ref[0, boards * k : boards * (k + 1), pair_lanes:] = piece
    pair_copy = to_partner(l_ref.at[0], l_ref.at[1], pair_sem)

    row_slot = iota((GROUP, 128), 0) % 4
    upper = iota((GROUP, 128), 0) < 4
    shift = (iota((GROUP, 128), 1) // SLOT - row_slot) % 4
    tiles = HI // 4
    t_refs = (t0_ref, t1_ref, t2_ref, t3_ref)

    def lay_out(g):
        for t in range(tiles):
            parts = []
            for k in range(4):
                at = GROUP * (4 * t + k)
                parts.append(
                    jnp.where(
                        upper,
                        h_refs[g][at : at + GROUP, :],
                        h_refs[g][GROUP * HI + at : GROUP * HI + at + GROUP, :],
                    )
                )
            row = None
            for k in range(4):
                moved = parts[(3 + k) % 4]
                for p in range(3):
                    moved = jnp.where(row_slot == p, parts[(p + k) % 4], moved)
                row = moved if row is None else jnp.where(shift == k, pltpu.roll(moved, SLOT * k, 1), row)
            t_refs[g][t] = row

    src, dst = iota((256, 128), 0), iota((256, 128), 1)
    within = (dst // SLOT > (src - 128) // SLOT).astype(F32) - (dst // SLOT < (src - 128) // SLOT).astype(F32)
    spread = jnp.where(src % SLOT == LO, jnp.where(src < 128, 1.0, within), 0.0).astype(BF16)
    spot = iota((GROUP, 128), 1) % SLOT == LO

    def add_rows(g):
        run = jnp.zeros((GROUP, 128), F32)
        below, whole = [], []
        for t in range(tiles):
            mark = jnp.where(spot, t_refs[g][t], 0.0)
            whole.append(mark)
            below.append(run)
            run = run + mark
        both = jnp.concatenate(
            [jnp.concatenate([below[t] - (run - below[t] - whole[t]), whole[t]], axis=1) for t in range(tiles)],
            axis=0,
        )
        got = jnp.dot(jnp.concatenate(split2(both), axis=0), spread, preferred_element_type=F32)
        got = got[: GROUP * tiles] + got[GROUP * tiles :]
        for t in range(tiles):
            t_refs[g][t] = t_refs[g][t] + got[GROUP * t : GROUP * (t + 1)]

    def look_up(g, half=1 - me):
        rows = slice(GROUP * g, GROUP * (g + 1))
        for k in range(lanes // 128):
            hi = f_ref[0, rows, cols_of(half, 128 * k, 128)].astype(jnp.int32)
            lo = f_ref[1, rows, cols_of(half, 128 * k, 128)].astype(jnp.int32)
            tile = hi >> 2
            at = ((hi & 3) << 5) + lo
            found = jnp.zeros((GROUP, 128), F32)
            for t in range(tiles):
                got = jnp.take_along_axis(t_refs[g][t], at, axis=1, mode="promise_in_bounds")
                found = jnp.where(tile == t, got, found)
            s_ref[half, rows, 128 * k : 128 * k + 128] = found

    stages = (tabulate, lay_out, add_rows, look_up)
    for step in range(groups + len(stages) - 1):
        for k, stage in enumerate(stages):
            if 0 <= step - k < groups:
                stage(step - k)
    sum_copy = to_partner(s_ref.at[1 - me], s_ref.at[2], sum_sem)

    pair_copy.wait()
    for load in loads[4:]:
        load.wait()
    for g in range(groups):
        look_up(g, me)
    back = [p_ref[:, q, :, cols_of(me)].reshape(CARDS * ROWS, lanes) for q in range(PARTS)]
    shared = jnp.dot(
        l_ref[:, :, 0:pair_lanes].reshape(4 * boards, pair_lanes),
        jnp.concatenate(back, axis=0),
        preferred_element_type=F32,
    )
    held = jnp.dot(
        l_ref[:, :, pair_lanes:].reshape(4 * boards, 128)[:, 0:64], hold, preferred_element_type=F32
    )
    trav = trav_ref[...].reshape(1, own_count)

    def ready(k, core):
        at = 2 * boards * k
        live = (
            0.5 * jnp.sum(l_ref[k, :, pair_lanes:].astype(F32).reshape(2, boards, 128).sum(0), axis=1, keepdims=True)
            - (held[at : at + boards] + held[at + boards : at + 2 * boards])
        )[:, 0:own_count] + reach_ref[rows_of(core), :].astype(F32)
        pot = column(pot_ref[...], core * boards, boards)
        bet = column(bet_ref[...], core * boards, boards) / hand_count
        half_pot = 0.5 * pot / hand_count
        return half_pot + bet * pot, shared[at : at + boards] + shared[at + boards : at + 2 * boards], half_pot * live

    def settle(core, sums, rate, taken, stake):
        values = jnp.maximum(rate * (sums - taken)[:, 0:own_count], -stake)
        values_ref[rows_of(core), :] = values
        return jnp.sum(values, axis=0, keepdims=True)

    here, there = ready(0, me), ready(1, 1 - me)
    mass = (jnp.sum(here[2], axis=0, keepdims=True) + jnp.sum(there[2], axis=0, keepdims=True)) / total_boards
    denominator = jnp.sum(mass * trav, axis=1, keepdims=True)
    part = settle(me, s_ref[me], *here)
    sum_copy.wait()
    part = (part + settle(1 - me, s_ref[2], *there)) / total_boards
    numerator = jnp.sum(part * trav, axis=1, keepdims=True)

    spot = XS * y + x
    for k in range(lanes // 128):
        size = min(128, own_count - 128 * k)
        mine_ref[0, k : k + 1, 0:size] = part[:, 128 * k : 128 * k + size]
        if size < 128:
            mine_ref[0, k : k + 1, size:] = jnp.zeros((1, 128 - size), F32)
    mine_ref[0, 6:7, :] = jnp.broadcast_to(numerator, (1, 128))
    mine_ref[0, 7:8, :] = jnp.broadcast_to(denominator, (1, 128))
    rows, ends_row = slice(0, 8), slice(6, 8)

    def exchange(source, groups):
        sent = []
        for peers, here, these, slots, sems in groups:
            for k, peer in enumerate(peers):
                copy = pltpu.make_async_remote_copy(
                    source.at[these, :], slots.at[here, these, :], sems.at[0, k], sems.at[1, here],
                    device_id=peer, device_id_type=MESH,
                )
                copy.start()
                sent.append(copy)
        return sent

    def arrived(source, where, these, slots, sems):
        pltpu.make_async_remote_copy(
            source.at[these, :], slots.at[where, these, :], sems.at[0, 0], sems.at[1, where],
            device_id=plane[0], device_id_type=MESH,
        ).wait_recv()

    sent = exchange(mine_ref.at[0], [(plane, spot, rows, plane_ref, plane_sem)])
    plane_ref[spot, rows, :] = mine_ref[0, rows, :]
    for peer in plane:
        arrived(mine_ref.at[0], XS * peer["board_0"] + peer["board_1"], rows, plane_ref, plane_sem)
    mine_ref[1, rows, :] = functools.reduce(jnp.add, [plane_ref[k, rows, :] for k in range(YS * XS)])
    sent += exchange(
        mine_ref.at[1], [(line, z, rows, line_ref, line_sem), (cross, z, ends_row, cross_ref, cross_sem)]
    )
    line_ref[z, rows, :] = mine_ref[1, rows, :]
    for peer in line:
        arrived(mine_ref.at[1], peer["board_2"], rows, line_ref, line_sem)
    for peer in cross:
        arrived(mine_ref.at[1], peer["board_2"], ends_row, cross_ref, cross_sem)
    total = functools.reduce(jnp.add, [line_ref[k, rows, :] for k in range(ZS)])
    rest = functools.reduce(jnp.add, [cross_ref[k, ends_row, :] for k in range(ZS)])
    hand_ref[0:7, :] = total[0:7]
    ends = total[6:8] + rest
    hand_ref[7:8, :] = ends[0:1] / ends[1:2]
    for copy in sent:
        copy.wait_send()


def write_kernel(values_ref, hand_ref, values_out, hand_out, ratio_out, ratio_ref, sems):
    ratio_ref[...] = hand_ref[7:8, 0:1]
    moves = ((values_ref, values_out), (hand_ref, hand_out), (ratio_ref, ratio_out))
    copies = [pltpu.make_async_copy(source, target, sems.at[k]) for k, (source, target) in enumerate(moves)]
    for copy in copies:
        copy.start()
    for copy in copies:
        copy.wait()


def write_out(*arrays):
    shapes = [a.shape for a in arrays] + [(1, 1)]
    return pl.pallas_call(
        write_kernel,
        out_shape=tuple(jax.ShapeDtypeStruct(shape, F32) for shape in shapes),
        in_specs=[pl.BlockSpec(memory_space=pltpu.VMEM)] * len(arrays),
        out_specs=(pl.BlockSpec(memory_space=pl.ANY),) * len(shapes),
        scratch_shapes=[pltpu.VMEM((1, 1), F32), pltpu.SemaphoreType.DMA((len(shapes),))],
        cost_estimate=pl.CostEstimate(flops=10**6, bytes_accessed=10**6, transcendentals=0),
    )(*(pltpu.with_memory_space_constraint(a, pltpu.VMEM) for a in arrays))


def local(opp_reach, hand_rank, hand_cards, pot, bet_frac, trav_reach):
    boards, hand_count = hand_rank.shape
    own_count = opp_reach.shape[1]
    lanes = -(-own_count // 128) * 128
    width = 2 * lanes
    half = boards // 2
    total_boards = boards * lax.axis_size(BOARD)
    whole = pl.BlockSpec(memory_space=pltpu.VMEM)
    board_values, hand_rows = pl.pallas_call(
        functools.partial(fused_kernel, total_boards, hand_count),
        out_shape=(
            pltpu.VMEM((boards, own_count), F32),
            pltpu.VMEM((8, 128), F32),
        ),
        in_specs=[pl.BlockSpec(memory_space=pl.ANY)] * 6,
        out_specs=(whole, whole),
        scratch_shapes=[
            pltpu.VMEM((boards, own_count), BF16),
            pltpu.VMEM((half, hand_count), jnp.int32),
            pltpu.VMEM((2, hand_count), jnp.int32),
            pltpu.VMEM((1, boards), F32),
            pltpu.VMEM((1, boards), F32),
            pltpu.VMEM((own_count,), F32),
            pltpu.SemaphoreType.DMA((6,)),
            pltpu.VMEM((8 * half, width), BF16),
            pltpu.VMEM((CARDS, PARTS, ROWS, width), BF16),
            pltpu.VMEM((CARDS, PARTS, ROWS, 8 * half), F32),
            pltpu.VMEM((CARDS, ROWS, 4 * half), F32),
            pltpu.VMEM((CARDS, ROWS, 4 * half), F32),
            pltpu.VMEM((CARDS, ROWS, 4 * half), F32),
            pltpu.VMEM((2, 2 * half, PARTS * CARDS * ROWS + 128), BF16),
            pltpu.VMEM((3, half, width), F32),
            pltpu.VMEM((half // GROUP, GROUP * HI, width), BF16),
            pltpu.VMEM((half // GROUP, GROUP * SLOT, width), BF16),
            *[pltpu.VMEM((2 * GROUP * HI, 128), F32)] * 4,
            *[pltpu.VMEM((HI // 4, GROUP, 128), F32)] * 4,
            pltpu.VMEM((3, half, lanes), F32),
            pltpu.VMEM((2, width), F32),
            pltpu.VMEM((half, own_count), BF16),
            pltpu.VMEM((2, 8, 128), F32),
            pltpu.VMEM((YS * XS, 8, 128), F32),
            pltpu.VMEM((ZS, 8, 128), F32),
            pltpu.VMEM((ZS, 8, 128), F32),
            pltpu.SemaphoreType.DMA((2,)),
            pltpu.SemaphoreType.DMA((2,)),
            pltpu.SemaphoreType.DMA((2,)),
            pltpu.SemaphoreType.DMA((2, YS * XS)),
            pltpu.SemaphoreType.DMA((2, ZS)),
            pltpu.SemaphoreType.DMA((2, ZS)),
        ],
        compiler_params=pltpu.CompilerParams(
            vmem_limit_bytes=56 * 1024 * 1024, collective_id=0, has_side_effects=True
        ),
        cost_estimate=pl.CostEstimate(flops=10**9, bytes_accessed=10**6, transcendentals=0),
    )(opp_reach, hand_rank, hand_cards.T, pot[None, :], bet_frac[None, :], trav_reach)
    board_values, hand_rows, ratio = write_out(board_values, hand_rows)
    return board_values, hand_rows.reshape(-1)[:own_count], ratio[0, 0]


def solution(mesh):
    torus = Mesh(
        mesh.devices.reshape(YS, XS, ZS, mesh.shape["hand"]), ("board_0", "board_1", "board_2", "hand")
    )
    placed = (P(BOARD, "hand"), P(BOARD, None), P(), P(BOARD), P(BOARD), P("hand"))
    return jax.shard_map(
        local,
        mesh=torus,
        in_specs=placed,
        out_specs=(P(BOARD, "hand"), P("hand"), P()),
        check_vma=False,
    )
```

```python
import functools

import jax
import jax.numpy as jnp
from jax import lax
from jax.experimental import pallas as pl
from jax.experimental.pallas import tpu as pltpu
from jax.sharding import Mesh
from jax.sharding import PartitionSpec as P

CARDS = 52
BOARD = ("board_0", "board_1", "board_2")
BF16 = jnp.bfloat16
F32 = jnp.float32

PARTS = 4
SHARE = CARDS // PARTS
ROWS = 16
HI, LO = 48, 28
SLOT = 32
GROUP = 8
DBLOCK = 4
YS, XS, ZS = 4, 4, 8
MESH = pl.DeviceIdType.MESH
NT = (((1,), (1,)), ((), ()))


def iota(shape, axis):
    return lax.broadcasted_iota(jnp.int32, shape, axis)


def split2(x):
    high = x.astype(BF16)
    return high, (x - high.astype(F32)).astype(BF16)


def rank_code(rank):
    return (((rank & 127) | 128) << (rank >> 7)).astype(F32).astype(BF16)


def every_peer(places):
    y, x, z, h = places
    plane = [
        {"board_0": lax.rem(y + i, YS), "board_1": lax.rem(x + j, XS)}
        for i in (2, 1, 3, 0)
        for j in (2, 1, 3, 0)
        if i or j
    ]
    line = [{"board_2": lax.rem(z + i, ZS)} for i in (4, 3, 5, 2, 6, 1, 7)]
    cross = [{"board_2": lax.rem(z + i, ZS), "hand": 1 - h} for i in (4, 3, 5, 2, 6, 1, 7, 0)]
    return plane, line, cross


def column(row, start, size):
    n = row.shape[1]
    hit = iota((size, n), 1) == iota((size, n), 0) + start
    return jnp.sum(jnp.where(hit, row, 0.0), axis=1, keepdims=True)


def fused_kernel(
    total_boards, hand_count,
    reach_hbm, rank_hbm, cards_hbm, pot_hbm, bet_hbm, trav_hbm,
    values_ref, hand_ref,
    reach_ref, rank_ref, cards_ref, pot_ref, bet_ref, trav_ref, io_sem,
    x_ref, p_ref, o_ref, w_ref, g_ref, q_ref, l_ref, f_ref, a_ref, b_ref, h0_ref, h1_ref, h2_ref, h3_ref, t0_ref, t1_ref, t2_ref, t3_ref, s_ref, c_ref,
    swap_ref, mine_ref, plane_ref, line_ref, cross_ref,
    swap_sem, pair_sem, sum_sem, plane_sem, line_sem, cross_sem,
):
    all_boards, own_count = reach_ref.shape
    boards = all_boards // 2
    block = 4 * boards
    lanes = x_ref.shape[1] // 2
    width = 2 * lanes
    places = tuple(lax.axis_index(name) for name in BOARD) + (lax.axis_index("hand"),)
    y, x, z, me = places
    plane, line, cross = every_peer(places)
    barrier = pltpu.get_barrier_semaphore()

    def cols_of(half, start=0, size=lanes):
        return pl.ds(pl.multiple_of(half * lanes + start, 128), size)

    def rows_of(core):
        return pl.ds(pl.multiple_of(core * boards, boards), boards)

    def to_partner(source, target, sems):
        copy = pltpu.make_async_remote_copy(
            source, target, sems.at[0], sems.at[1], device_id={"hand": 1 - me}, device_id_type=MESH
        )
        copy.start()
        return copy

    loads = [
        pltpu.make_async_copy(source, target, io_sem.at[k])
        for k, (source, target) in enumerate(
            (
                (cards_hbm, cards_ref),
                (rank_hbm.at[rows_of(me), :], rank_ref),
                (reach_hbm, reach_ref),
                (pot_hbm, pot_ref),
                (bet_hbm, bet_ref),
                (trav_hbm, trav_ref),
            )
        )
    ]
    for load in loads:
        load.start()
    for peer in plane + line + cross:
        pl.semaphore_signal(barrier, inc=1, device_id=peer, device_id_type=MESH)

    loads[0].wait()
    for half in range(2):
        start = half * lanes
        c_ref[:, start + lanes - 128 : start + lanes] = jnp.full((2, 128), -1.0, F32)
        c_ref[:, start : start + own_count] = cards_ref[:, half * own_count : (half + 1) * own_count].astype(F32)

    row16 = iota((16, lanes), 0)
    own_row = [
        jnp.where(row16 < SHARE, row16 + SHARE * q, -5).astype(F32).astype(BF16) for q in range(PARTS)
    ]

    def hot_rows(half, d):
        low, high = c_ref[0:1, cols_of(half)], c_ref[1:2, cols_of(half)]
        partner = jnp.where(low == float(d), high, jnp.where(high == float(d), low, -1.0))
        wide = jnp.broadcast_to(partner, (16, lanes)).astype(BF16)
        for q in range(PARTS):
            p_ref[d, q, :, cols_of(half)] = jnp.where(wide == own_row[q], BF16(1), BF16(0))

    loads[1].wait()
    loads[2].wait()
    for half in range(2):
        start = half * lanes
        f_ref[0:2, :, start + lanes - 128 : start + lanes] = jnp.zeros((2, boards, 128), F32)
        x_ref[:, start + lanes - 128 : start + lanes] = jnp.zeros((8 * boards, 128), BF16)
        rank = rank_ref[:, half * own_count : (half + 1) * own_count]
        x_ref[block : block + boards, start : start + own_count] = rank_code(rank)
        hi = (rank * 2341) >> 16
        f_ref[0, :, start : start + own_count] = hi.astype(F32)
        f_ref[1, :, start : start + own_count] = (rank - LO * hi).astype(F32)
    for k in range(1, PARTS):
        x_ref[block + k * boards : block + (k + 1) * boards, :] = x_ref[block : block + boards, :]

    def place(half, reach):
        x_ref[0:boards, pl.ds(pl.multiple_of(half * lanes, 128), own_count)] = reach
        f_ref[2, :, cols_of(half)] = x_ref[0:boards, cols_of(half)].astype(F32)
        for k in range(1, PARTS):
            x_ref[k * boards : (k + 1) * boards, cols_of(half)] = x_ref[0:boards, cols_of(half)]

    chunk = CARDS // PARTS

    def to_cards(half, more):
        for i in range(PARTS):
            these = slice(chunk * i, chunk * (i + 1))
            if not more:
                for d in range(chunk * i, chunk * (i + 1)):
                    hot_rows(half, d)
            if more:
                high_factor(half, i)
            rows = p_ref[these, :, :, cols_of(half)].reshape(chunk * PARTS * ROWS, lanes)
            got = lax.dot_general(rows, x_ref[:, cols_of(half)], NT, preferred_element_type=F32)
            got = got.reshape(chunk, PARTS, ROWS, 2 * block)
            o_ref[these] = got + o_ref[these] if more else got

    digit = iota((16, lanes), 0).astype(F32).astype(BF16)

    pair = (iota((16, lanes), 0) // GROUP).astype(F32).astype(BF16)

    def high_factor(half, g):
        boards_here = slice(GROUP * g, GROUP * (g + 1))
        hi, reach = (
            jnp.concatenate([f_ref[k, boards_here, cols_of(half)]] * 2, axis=0).astype(BF16) for k in (0, 2)
        )
        for two in range(HI // 2):
            hit = hi == pair + BF16(2 * two)
            a_ref[g, 16 * two : 16 * two + 16, cols_of(half)] = jnp.where(hit, reach, BF16(0))

    def low_factor(half, g):
        for b in range(GROUP):
            at = GROUP * g + b
            lo = jnp.broadcast_to(f_ref[1, at : at + 1, cols_of(half)], (16, lanes)).astype(BF16)
            for part in range(SLOT // 16):
                at = SLOT * b + 16 * part
                b_ref[g, at : at + 16, cols_of(half)] = lax.clamp(
                    BF16(-1), digit + BF16(16 * part) - lo, BF16(1)
                )

    h_refs = (h0_ref, h1_ref, h2_ref, h3_ref)

    def tabulate(g, half=1 - me):
        got = lax.dot_general(
            a_ref[g, :, cols_of(half)], b_ref[g, :, cols_of(half)], NT, preferred_element_type=F32
        )
        for k in range(2):
            rows, piece = slice(GROUP * HI * k, GROUP * HI * (k + 1)), got[:, 128 * k : 128 * (k + 1)]
            h_refs[g][rows, :] = piece if half is me else piece + h_refs[g][rows, :]

    place(me, reach_ref[rows_of(me), :])
    to_cards(me, False)
    loads[3].wait()
    groups = boards // GROUP
    for d in range(CARDS):
        hot_rows(1 - me, d)
    for g in range(groups):
        low_factor(me, g)
        low_factor(1 - me, g)
    pl.semaphore_wait(barrier, len(plane + line + cross))
    swap = to_partner(reach_ref.at[rows_of(1 - me), :], swap_ref, swap_sem)
    for g in range(groups):
        high_factor(me, g)
        tabulate(g, me)
    swap.wait()
    place(1 - me, swap_ref[...])
    card = iota((64, lanes), 0).astype(F32)
    card_totals = jnp.zeros((boards, 64), F32)
    for half in (1 - me, me):
        hold = ((card == c_ref[0:1, cols_of(half)]) | (card == c_ref[1:2, cols_of(half)])).astype(F32).astype(BF16)
        card_totals = card_totals + lax.dot_general(
            x_ref[0:boards, cols_of(half)], hold, NT, preferred_element_type=F32
        )
    to_cards(1 - me, True)

    part_of = iota((ROWS, block), 1) // boards

    def pack(d, carry):
        for ref, at in ((w_ref, 0), (g_ref, block)):
            got = o_ref[d, 0, :, at : at + block]
            for q in range(1, PARTS):
                got = jnp.where(part_of == q, o_ref[d, q, :, at : at + block], got)
            ref[d] = got
        return carry

    lax.fori_loop(0, CARDS, pack, 0, unroll=4)

    def pairs(i, carry):
        mine = [g_ref[DBLOCK * i + k].astype(BF16) for k in range(DBLOCK)]
        sums = [None] * DBLOCK
        for e in range(CARDS):
            ge, we = g_ref[e].astype(BF16), w_ref[e].astype(BF16)
            for k in range(DBLOCK):
                sign = lax.clamp(BF16(-1), mine[k] - ge, BF16(1))
                term = sign.astype(F32) * we.astype(F32)
                sums[k] = term if sums[k] is None else sums[k] + term
        for k in range(DBLOCK):
            q_ref[DBLOCK * i + k] = sums[k]
        return carry

    lax.fori_loop(0, CARDS // DBLOCK, pairs, 0)
    wide = jnp.concatenate([card_totals, jnp.zeros((boards, 64), F32)], axis=1)
    pair_lanes = PARTS * CARDS * ROWS
    turned = jnp.transpose(q_ref[...].reshape(CARDS * ROWS, block))
    for k, piece in enumerate(split2(turned)):
        for q in range(PARTS):
            l_ref[0, boards * k : boards * (k + 1), CARDS * ROWS * q : CARDS * ROWS * (q + 1)] = piece[
                boards * q : boards * (q + 1)
            ]
    for k, piece in enumerate(split2(wide)):
        l_ref[0, boards * k : boards * (k + 1), pair_lanes:] = piece
    pair_copy = to_partner(l_ref.at[0], l_ref.at[1], pair_sem)

    row_slot = iota((GROUP, 128), 0) % 4
    upper = iota((GROUP, 128), 0) < 4
    shift = (iota((GROUP, 128), 1) // SLOT - row_slot) % 4
    tiles = HI // 4
    t_refs = (t0_ref, t1_ref, t2_ref, t3_ref)

    def lay_out(g):
        for t in range(tiles):
            parts = []
            for k in range(4):
                at = GROUP * (4 * t + k)
                parts.append(
                    jnp.where(
                        upper,
                        h_refs[g][at : at + GROUP, :],
                        h_refs[g][GROUP * HI + at : GROUP * HI + at + GROUP, :],
                    )
                )
            row = None
            for k in range(4):
                moved = parts[(3 + k) % 4]
                for p in range(3):
                    moved = jnp.where(row_slot == p, parts[(p + k) % 4], moved)
                row = moved if row is None else jnp.where(shift == k, pltpu.roll(moved, SLOT * k, 1), row)
            t_refs[g][t] = row

    src, dst = iota((256, 128), 0), iota((256, 128), 1)
    within = (dst // SLOT > (src - 128) // SLOT).astype(F32) - (dst // SLOT < (src - 128) // SLOT).astype(F32)
    spread = jnp.where(src % SLOT == LO, jnp.where(src < 128, 1.0, within), 0.0).astype(BF16)
    spot = iota((GROUP, 128), 1) % SLOT == LO

    def add_rows(g):
        run = jnp.zeros((GROUP, 128), F32)
        below, whole = [], []
        for t in range(tiles):
            mark = jnp.where(spot, t_refs[g][t], 0.0)
            whole.append(mark)
            below.append(run)
            run = run + mark
        both = jnp.concatenate(
            [jnp.concatenate([below[t] - (run - below[t] - whole[t]), whole[t]], axis=1) for t in range(tiles)],
            axis=0,
        )
        got = jnp.dot(jnp.concatenate(split2(both), axis=0), spread, preferred_element_type=F32)
        got = got[: GROUP * tiles] + got[GROUP * tiles :]
        for t in range(tiles):
            t_refs[g][t] = t_refs[g][t] + got[GROUP * t : GROUP * (t + 1)]

    def look_up(g, half=1 - me):
        rows = slice(GROUP * g, GROUP * (g + 1))
        for k in range(lanes // 128):
            hi = f_ref[0, rows, cols_of(half, 128 * k, 128)].astype(jnp.int32)
            lo = f_ref[1, rows, cols_of(half, 128 * k, 128)].astype(jnp.int32)
            tile = hi >> 2
            at = ((hi & 3) << 5) + lo
            found = jnp.zeros((GROUP, 128), F32)
            for t in range(tiles):
                got = jnp.take_along_axis(t_refs[g][t], at, axis=1, mode="promise_in_bounds")
                found = jnp.where(tile == t, got, found)
            s_ref[half, rows, 128 * k : 128 * k + 128] = found

    stages = (tabulate, lay_out, add_rows, look_up)
    for step in range(groups + len(stages) - 1):
        for k, stage in enumerate(stages):
            if 0 <= step - k < groups:
                stage(step - k)
    sum_copy = to_partner(s_ref.at[1 - me], s_ref.at[2], sum_sem)

    pair_copy.wait()
    for load in loads[4:]:
        load.wait()
    for g in range(groups):
        look_up(g, me)
    back = [p_ref[:, q, :, cols_of(me)].reshape(CARDS * ROWS, lanes) for q in range(PARTS)]
    shared = jnp.dot(
        l_ref[:, :, 0:pair_lanes].reshape(4 * boards, pair_lanes),
        jnp.concatenate(back, axis=0),
        preferred_element_type=F32,
    )
    held = jnp.dot(
        l_ref[:, :, pair_lanes:].reshape(4 * boards, 128)[:, 0:64], hold, preferred_element_type=F32
    )
    trav = trav_ref[...].reshape(1, own_count)

    def ready(k, core):
        at = 2 * boards * k
        live = (
            0.5 * jnp.sum(l_ref[k, :, pair_lanes:].astype(F32).reshape(2, boards, 128).sum(0), axis=1, keepdims=True)
            - (held[at : at + boards] + held[at + boards : at + 2 * boards])
        )[:, 0:own_count] + reach_ref[rows_of(core), :].astype(F32)
        pot = column(pot_ref[...], core * boards, boards)
        bet = column(bet_ref[...], core * boards, boards) / hand_count
        half_pot = 0.5 * pot / hand_count
        return half_pot + bet * pot, shared[at : at + boards] + shared[at + boards : at + 2 * boards], half_pot * live

    def settle(core, sums, rate, taken, stake):
        values = jnp.maximum(rate * (sums - taken)[:, 0:own_count], -stake)
        values_ref[rows_of(core), :] = values
        return jnp.sum(values, axis=0, keepdims=True)

    here, there = ready(0, me), ready(1, 1 - me)
    mass = (jnp.sum(here[2], axis=0, keepdims=True) + jnp.sum(there[2], axis=0, keepdims=True)) / total_boards
    denominator = jnp.sum(mass * trav, axis=1, keepdims=True)
    part = settle(me, s_ref[me], *here)
    sum_copy.wait()
    part = (part + settle(1 - me, s_ref[2], *there)) / total_boards
    numerator = jnp.sum(part * trav, axis=1, keepdims=True)

    spot = XS * y + x
    for k in range(lanes // 128):
        size = min(128, own_count - 128 * k)
        mine_ref[0, k : k + 1, 0:size] = part[:, 128 * k : 128 * k + size]
        if size < 128:
            mine_ref[0, k : k + 1, size:] = jnp.zeros((1, 128 - size), F32)
    mine_ref[0, 6:7, :] = jnp.broadcast_to(numerator, (1, 128))
    mine_ref[0, 7:8, :] = jnp.broadcast_to(denominator, (1, 128))
    rows, ends_row = slice(0, 8), slice(6, 8)

    def exchange(source, groups):
        sent = []
        for peers, here, these, slots, sems in groups:
            for k, peer in enumerate(peers):
                copy = pltpu.make_async_remote_copy(
                    source.at[these, :], slots.at[here, these, :], sems.at[0, k], sems.at[1, here],
                    device_id=peer, device_id_type=MESH,
                )
                copy.start()
                sent.append(copy)
        return sent

    def arrived(source, where, these, slots, sems):
        pltpu.make_async_remote_copy(
            source.at[these, :], slots.at[where, these, :], sems.at[0, 0], sems.at[1, where],
            device_id=plane[0], device_id_type=MESH,
        ).wait_recv()

    sent = exchange(mine_ref.at[0], [(plane, spot, rows, plane_ref, plane_sem)])
    plane_ref[spot, rows, :] = mine_ref[0, rows, :]
    for peer in plane:
        arrived(mine_ref.at[0], XS * peer["board_0"] + peer["board_1"], rows, plane_ref, plane_sem)
    mine_ref[1, rows, :] = functools.reduce(jnp.add, [plane_ref[k, rows, :] for k in range(YS * XS)])
    sent += exchange(
        mine_ref.at[1], [(line, z, rows, line_ref, line_sem), (cross, z, ends_row, cross_ref, cross_sem)]
    )
    line_ref[z, rows, :] = mine_ref[1, rows, :]
    for peer in line:
        arrived(mine_ref.at[1], peer["board_2"], rows, line_ref, line_sem)
    for peer in cross:
        arrived(mine_ref.at[1], peer["board_2"], ends_row, cross_ref, cross_sem)
    total = functools.reduce(jnp.add, [line_ref[k, rows, :] for k in range(ZS)])
    rest = functools.reduce(jnp.add, [cross_ref[k, ends_row, :] for k in range(ZS)])
    hand_ref[0:7, :] = total[0:7]
    ends = total[6:8] + rest
    hand_ref[7:8, :] = ends[0:1] / ends[1:2]
    for copy in sent:
        copy.wait_send()


def write_kernel(values_ref, hand_ref, values_out, hand_out, ratio_out, ratio_ref, sems):
    ratio_ref[...] = hand_ref[7:8, 0:1]
    moves = ((values_ref, values_out), (hand_ref, hand_out), (ratio_ref, ratio_out))
    copies = [pltpu.make_async_copy(source, target, sems.at[k]) for k, (source, target) in enumerate(moves)]
    for copy in copies:
        copy.start()
    for copy in copies:
        copy.wait()


def write_out(*arrays):
    shapes = [a.shape for a in arrays] + [(1, 1)]
    return pl.pallas_call(
        write_kernel,
        out_shape=tuple(jax.ShapeDtypeStruct(shape, F32) for shape in shapes),
        in_specs=[pl.BlockSpec(memory_space=pltpu.VMEM)] * len(arrays),
        out_specs=(pl.BlockSpec(memory_space=pl.ANY),) * len(shapes),
        scratch_shapes=[pltpu.VMEM((1, 1), F32), pltpu.SemaphoreType.DMA((len(shapes),))],
        cost_estimate=pl.CostEstimate(flops=10**6, bytes_accessed=10**6, transcendentals=0),
    )(*(pltpu.with_memory_space_constraint(a, pltpu.VMEM) for a in arrays))


def local(opp_reach, hand_rank, hand_cards, pot, bet_frac, trav_reach):
    boards, hand_count = hand_rank.shape
    own_count = opp_reach.shape[1]
    lanes = -(-own_count // 128) * 128
    width = 2 * lanes
    half = boards // 2
    total_boards = boards * lax.axis_size(BOARD)
    whole = pl.BlockSpec(memory_space=pltpu.VMEM)
    board_values, hand_rows = pl.pallas_call(
        functools.partial(fused_kernel, total_boards, hand_count),
        out_shape=(
            pltpu.VMEM((boards, own_count), F32),
            pltpu.VMEM((8, 128), F32),
        ),
        in_specs=[pl.BlockSpec(memory_space=pl.ANY)] * 6,
        out_specs=(whole, whole),
        scratch_shapes=[
            pltpu.VMEM((boards, own_count), BF16),
            pltpu.VMEM((half, hand_count), jnp.int32),
            pltpu.VMEM((2, hand_count), jnp.int32),
            pltpu.VMEM((1, boards), F32),
            pltpu.VMEM((1, boards), F32),
            pltpu.VMEM((own_count,), F32),
            pltpu.SemaphoreType.DMA((6,)),
            pltpu.VMEM((8 * half, width), BF16),
            pltpu.VMEM((CARDS, PARTS, ROWS, width), BF16),
            pltpu.VMEM((CARDS, PARTS, ROWS, 8 * half), F32),
            pltpu.VMEM((CARDS, ROWS, 4 * half), F32),
            pltpu.VMEM((CARDS, ROWS, 4 * half), F32),
            pltpu.VMEM((CARDS, ROWS, 4 * half), F32),
            pltpu.VMEM((2, 2 * half, PARTS * CARDS * ROWS + 128), BF16),
            pltpu.VMEM((3, half, width), F32),
            pltpu.VMEM((half // GROUP, GROUP * HI, width), BF16),
            pltpu.VMEM((half // GROUP, GROUP * SLOT, width), BF16),
            *[pltpu.VMEM((2 * GROUP * HI, 128), F32)] * 4,
            *[pltpu.VMEM((HI // 4, GROUP, 128), F32)] * 4,
            pltpu.VMEM((3, half, lanes), F32),
            pltpu.VMEM((2, width), F32),
            pltpu.VMEM((half, own_count), BF16),
            pltpu.VMEM((2, 8, 128), F32),
            pltpu.VMEM((YS * XS, 8, 128), F32),
            pltpu.VMEM((ZS, 8, 128), F32),
            pltpu.VMEM((ZS, 8, 128), F32),
            pltpu.SemaphoreType.DMA((2,)),
            pltpu.SemaphoreType.DMA((2,)),
            pltpu.SemaphoreType.DMA((2,)),
            pltpu.SemaphoreType.DMA((2, YS * XS)),
            pltpu.SemaphoreType.DMA((2, ZS)),
            pltpu.SemaphoreType.DMA((2, ZS)),
        ],
        compiler_params=pltpu.CompilerParams(
            vmem_limit_bytes=56 * 1024 * 1024, collective_id=0, has_side_effects=True
        ),
        cost_estimate=pl.CostEstimate(flops=10**9, bytes_accessed=10**6, transcendentals=0),
    )(opp_reach, hand_rank, hand_cards.T, pot[None, :], bet_frac[None, :], trav_reach)
    board_values, hand_rows, ratio = write_out(board_values, hand_rows)
    return board_values, hand_rows.reshape(-1)[:own_count], ratio[0, 0]


def solution(mesh):
    torus = Mesh(
        mesh.devices.reshape(YS, XS, ZS, mesh.shape["hand"]), ("board_0", "board_1", "board_2", "hand")
    )
    placed = (P(BOARD, "hand"), P(BOARD, None), P(), P(BOARD), P(BOARD), P("hand"))
    return jax.shard_map(
        local,
        mesh=torus,
        in_specs=placed,
        out_specs=(P(BOARD, "hand"), P("hand"), P()),
        check_vma=False,
    )
```
